128 devices in a mesh: fsdp: 32 (over z, y, x_hi), sp: 4 (over x_lo, core).
Axes of the slice: x: 4 (x_hi: 2, x_lo: 2; x = x_hi * 2 + x_lo), y: 4, z: 4, core: 2. Of those that a mesh axis runs over, the one named last changes fastest.
Arguments:
- tokens: bfloat16 [32, 512, 1536], P('fsdp', 'sp'), may hold values from -6 to 6
- modulation: float32 [32, 1, 6, 1536], P('fsdp'), may hold values from -4 to 4
- w_qkv: bfloat16 [1, 1536, 3, 1536], P(None, 'fsdp', None, 'sp'), may hold values from -0.15625 to 0.15625
- w_out: bfloat16 [1, 1536, 1536], P(None, 'sp', 'fsdp'), may hold values from -0.15625 to 0.15625
- w_in: bfloat16 [1, 1536, 6144], P(None, 'fsdp', 'sp'), may hold values from -0.15625 to 0.15625
- w_back: bfloat16 [1, 6144, 1536], P(None, 'sp', 'fsdp'), may hold values from -0.078125 to 0.078125
- out_grad: bfloat16 [32, 512, 1536], P('fsdp', 'sp'), may hold values from -6 to 6
Outputs:
- final_out: bfloat16 [32, 512, 1536], P('fsdp', 'sp')
- input_grad: float32 [32, 512, 1536], P('fsdp', 'sp')
- grad_qkv: float32 [1, 1536, 3, 1536], P(None, 'fsdp', None, 'sp')
- grad_out: float32 [1, 1536, 1536], P(None, 'sp', 'fsdp')
- grad_in: float32 [1, 1536, 6144], P(None, 'fsdp', 'sp')
- grad_back: float32 [1, 6144, 1536], P(None, 'sp', 'fsdp')
The draws below stay inside these ranges and needn't reach their ends.
All inputs are finite; a program needn't handle non-finite values.
Results may differ from the reference program's by a relative error of at most 0.03.
Values may be sent and summed in bfloat16 or wider, within the bound.
A program may use at most 128 MiB of HBM per device.

```python
import math
import jax
import jax.numpy as jnp
from jax import lax

D = 1536
HEAD_DIM = 128
FF = 6144
LAYERS = 1
SEQ = 512
BATCH = 32
N_FSDP = 32


def block_scale(rng, dims, shards, smallest, top_value):
    def one(axis_at, parts):
        heights = jax.random.uniform(jax.random.fold_in(jax.random.fold_in(rng, 6), axis_at), (parts,), jnp.float32, smallest / len(shards), top_value / len(shards))
        return jnp.repeat(jnp.exp(heights), dims[axis_at] // parts).reshape((-1,) + (1,) * (len(dims) - axis_at - 1))

    gain = one(*shards[0])
    for cut in shards[1:]:
        gain = gain * one(*cut)
    return gain


def bell_draw(stream_key, shape, spread, limit, cuts=(), dtype=jnp.bfloat16):
    drawn = spread * jax.random.normal(stream_key, shape, jnp.float32)
    if cuts:
        drawn = drawn * block_scale(stream_key, shape, cuts, -0.22, 0.18)
    return jnp.clip(drawn, -limit, limit).astype(dtype)


def setup_inputs(seed: int = 0) -> dict:
    keys = jax.random.split(jax.random.key(seed), 8)
    tokens = bell_draw(keys[0], (BATCH, SEQ, D), 1.0, 6.0, ((0, 32), (1, 4)))
    modulation = bell_draw(keys[1], (BATCH, LAYERS, 6, D), 1.0, 4.0, ((0, 32),), jnp.float32)
    w_qkv = bell_draw(keys[2], (LAYERS, D, 3, D), D ** -0.5, 0.15625, ((1, 32), (3, 4)))
    w_out = bell_draw(keys[3], (LAYERS, D, D), D ** -0.5, 0.15625, ((1, 4), (2, 32)))
    w_in = bell_draw(keys[4], (LAYERS, D, FF), D ** -0.5, 0.15625, ((1, 32), (2, 4)))
    w_back = bell_draw(keys[5], (LAYERS, FF, D), FF ** -0.5, 0.078125, ((1, 4), (2, 32)))
    out_grad = bell_draw(keys[6], (BATCH, SEQ, D), 1.0, 6.0, ((0, 32), (1, 4)))
    return dict(tokens=tokens, modulation=modulation, w_qkv=w_qkv, w_out=w_out, w_in=w_in, w_back=w_back, out_grad=out_grad)


ln_eps = 1e-06
temper = 2.5
block_limit = 512

def normalize(stream):
    mean_part = lax.optimization_barrier(jnp.mean(stream, axis=-1, keepdims=True))
    centred = stream - mean_part
    rstd = lax.rsqrt(lax.optimization_barrier(jnp.mean(centred * centred, axis=-1, keepdims=True)) + ln_eps)
    return (centred * rstd, rstd)

def norm_back(normed, rstd, incoming):
    first = lax.optimization_barrier(jnp.mean(incoming, axis=-1, keepdims=True))
    second = lax.optimization_barrier(jnp.mean(incoming * normed, axis=-1, keepdims=True))
    return rstd * (incoming - first - normed * second)

def gelu_tanh(hidden):
    return jax.nn.gelu(hidden, approximate=True)

def project(left, weight):
    flat_rows = left.reshape(-1, left.shape[-1])
    result = jnp.dot(flat_rows, weight, preferred_element_type=jnp.float32)
    return result.reshape(left.shape[:-1] + (weight.shape[1],))

def project_back(left, weight):
    flat_rows = left.reshape(-1, left.shape[-1])
    result = lax.dot_general(flat_rows, weight, (((1,), (1,)), ((), ())), preferred_element_type=jnp.float32)
    return result.reshape(left.shape[:-1] + (weight.shape[0],))

def group_grad(left, right, grad_scale):
    width_left = left.shape[-1]
    width_right = right.shape[-1]
    left_groups = left.reshape(N_FSDP, -1, width_left)
    right_groups = right.reshape(N_FSDP, -1, width_right)

    def add_group(total, pair):
        left_part, right_part = pair
        term = lax.dot_general(left_part, right_part, (((0,), (0,)), ((), ())), preferred_element_type=jnp.float32) * grad_scale
        rounded = lax.optimization_barrier(term.astype(jnp.bfloat16))
        return (total + rounded.astype(jnp.float32), None)
    total, unused = lax.scan(add_group, jnp.zeros((width_left, width_right), jnp.float32), (left_groups, right_groups))
    return total

def split_heads(packed, head_count):
    return packed.reshape(packed.shape[:-1] + (head_count, packed.shape[-1] // head_count))

def heads_major(tensor):
    videos, seq_len, head_count, head_width = tensor.shape
    return tensor.transpose(0, 2, 1, 3).reshape(videos * head_count, seq_len, head_width)

def heads_minor(tensor, videos):
    merged, seq_len, head_width = tensor.shape
    return tensor.reshape(videos, merged // videos, seq_len, head_width).transpose(0, 2, 1, 3)

def attend_head(triple):
    queries, key_rows, values = triple
    seq_len, head_width = queries.shape
    block_size = min(block_limit, seq_len)
    score_factor = temper / math.sqrt(head_width)
    values_wide = values.astype(jnp.float32)

    def one_block(query_rows):
        scores = jnp.dot(query_rows, key_rows.T, preferred_element_type=jnp.float32) * score_factor
        softmaxed = jax.nn.softmax(scores, axis=-1)
        return jnp.dot(softmaxed, values_wide, precision=lax.Precision.HIGHEST).astype(jnp.bfloat16)
    attended = lax.map(one_block, queries.reshape(seq_len // block_size, block_size, head_width))
    return attended.reshape(seq_len, head_width)

def attend_back(quadruple):
    queries, key_rows, values, upstream = quadruple
    seq_len, head_width = queries.shape
    block_size = min(block_limit, seq_len)
    score_factor = temper / math.sqrt(head_width)
    keys_wide = key_rows.astype(jnp.float32)

    def one_block(running, block_pair):
        query_rows, grad_rows = block_pair
        scores = jnp.dot(query_rows, key_rows.T, preferred_element_type=jnp.float32) * score_factor
        softmaxed = jax.nn.softmax(scores, axis=-1)
        dprobs = jnp.dot(grad_rows, values.T, preferred_element_type=jnp.float32)
        dscores = softmaxed * (dprobs - lax.optimization_barrier(jnp.sum(softmaxed * dprobs, axis=-1, keepdims=True))) * score_factor
        dquery = jnp.dot(dscores, keys_wide, precision=lax.Precision.HIGHEST)
        grad_keys = running[0] + jnp.dot(dscores.T, query_rows.astype(jnp.float32), precision=lax.Precision.HIGHEST)
        dvalues = running[1] + jnp.dot(softmaxed.T, grad_rows.astype(jnp.float32), precision=lax.Precision.HIGHEST)
        return ((grad_keys, dvalues), dquery)
    zero_rows = jnp.zeros((seq_len, head_width), jnp.float32)
    count = seq_len // block_size
    blocks = (queries.reshape(count, block_size, head_width), upstream.reshape(count, block_size, head_width))
    (grad_keys, dvalues), dquery = lax.scan(one_block, (zero_rows, zero_rows), blocks)
    return (dquery.reshape(seq_len, head_width).astype(jnp.bfloat16), grad_keys.astype(jnp.bfloat16), dvalues.astype(jnp.bfloat16))

def attend_all(queries, key_rows, values):
    attended = lax.map(attend_head, (heads_major(queries), heads_major(key_rows), heads_major(values)))
    return heads_minor(attended, queries.shape[0])

def attend_all_back(queries, key_rows, values, upstream):
    grad_heads = lax.map(attend_back, (heads_major(queries), heads_major(key_rows), heads_major(values), heads_major(upstream)))
    return tuple((heads_minor(grad_piece, queries.shape[0]) for grad_piece in grad_heads))

def reference(tokens, modulation, w_qkv, w_out, w_in, w_back, out_grad):
    videos, seq_len, model_width = tokens.shape
    layers = w_qkv.shape[0]
    head_count = model_width // HEAD_DIM
    grad_scale = 1.0 / math.sqrt(videos * seq_len)
    stream = tokens.astype(jnp.float32)
    stored = []
    for layer_index in range(layers):
        layer_mod = modulation[:, layer_index][:, :, None, :]
        joint = w_qkv[layer_index].reshape(model_width, 3 * model_width)
        normed_first, rstd_first = normalize(stream)
        input_first = (normed_first * (1.0 + layer_mod[:, 1]) + layer_mod[:, 0]).astype(jnp.bfloat16)
        packed = project(input_first, joint).astype(jnp.bfloat16)
        queries = split_heads(packed[..., :model_width], head_count)
        key_rows = split_heads(packed[..., model_width:2 * model_width], head_count)
        values = split_heads(packed[..., 2 * model_width:], head_count)
        attended = attend_all(queries, key_rows, values).reshape(videos, seq_len, model_width)
        middle = stream + layer_mod[:, 2] * project(attended, w_out[layer_index])
        normed_second, rstd_second = normalize(middle)
        input_second = (normed_second * (1.0 + layer_mod[:, 4]) + layer_mod[:, 3]).astype(jnp.bfloat16)
        hidden = project(input_second, w_in[layer_index])
        activated = gelu_tanh(hidden).astype(jnp.bfloat16)
        stream = middle + layer_mod[:, 5] * project(activated, w_back[layer_index])
        stored.append((normed_first, rstd_first, input_first, queries, key_rows, values, attended, normed_second, rstd_second, input_second, hidden, activated))
    final_out = stream.astype(jnp.bfloat16)
    stream_grad = out_grad.astype(jnp.float32)
    results = [None] * layers
    for layer_index in range(layers - 1, -1, -1):
        normed_first, rstd_first, input_first, queries, key_rows, values, attended, normed_second, rstd_second, input_second, hidden, activated = stored[layer_index]
        layer_mod = modulation[:, layer_index][:, :, None, :]
        joint = w_qkv[layer_index].reshape(model_width, 3 * model_width)
        down_grad = (layer_mod[:, 5] * stream_grad).astype(jnp.bfloat16)
        back_hidden = project_back(down_grad, w_back[layer_index])
        unused, pullback = jax.vjp(gelu_tanh, hidden)
        up_grad = pullback(back_hidden)[0].astype(jnp.bfloat16)
        back_second = project_back(up_grad, w_in[layer_index])
        stream_grad = stream_grad + norm_back(normed_second, rstd_second, back_second * (1.0 + layer_mod[:, 4]))
        attn_grad = (layer_mod[:, 2] * stream_grad).astype(jnp.bfloat16)
        mixed_grad = split_heads(project_back(attn_grad, w_out[layer_index]).astype(jnp.bfloat16), head_count)
        grad_query, grad_keys, grad_values = attend_all_back(queries, key_rows, values, mixed_grad)
        packed_grad = jnp.concatenate([grad_query.reshape(videos, seq_len, model_width), grad_keys.reshape(videos, seq_len, model_width), grad_values.reshape(videos, seq_len, model_width)], axis=-1)
        back_first = project_back(packed_grad, joint)
        stream_grad = stream_grad + norm_back(normed_first, rstd_first, back_first * (1.0 + layer_mod[:, 1]))
        results[layer_index] = (group_grad(input_first, packed_grad, grad_scale).reshape(model_width, 3, model_width), group_grad(attended, attn_grad, grad_scale), group_grad(input_second, up_grad, grad_scale), group_grad(activated, down_grad, grad_scale))
    grad_qkv = jnp.stack([results[index][0] for index in range(layers)])
    grad_out = jnp.stack([results[index][1] for index in range(layers)])
    grad_in = jnp.stack([results[index][2] for index in range(layers)])
    grad_back = jnp.stack([results[index][3] for index in range(layers)])
    return (final_out, stream_grad, grad_qkv, grad_out, grad_in, grad_back)
```

```python
import functools
import math

import jax
import jax.numpy as jnp
from jax import lax
from jax.experimental import pallas as pl
from jax.experimental.pallas import tpu as pltpu
from jax.sharding import PartitionSpec as P

HEAD_DIM = 128
LN_EPS = 1e-06
TEMPER = 2.5
F32 = jnp.float32
BF16 = jnp.bfloat16
MESH = pl.DeviceIdType.MESH
GROUP = 1536
HALF = GROUP // 2
QUART = GROUP // 4
ROWS = 48


def rem(a, n):
    return lax.rem(a, n)


class Place:
    def __init__(self):
        f = lax.axis_index("fsdp")
        s = lax.axis_index("sp")
        self.z, self.y, self.xh = lax.div(f, 8), rem(lax.div(f, 2), 4), rem(f, 2)
        self.xl, self.c = lax.div(s, 2), rem(s, 2)
        self.s = s

    def dev(self, **kw):
        v = {k: kw.get(k, getattr(self, k)) for k in ("z", "y", "xh", "xl", "c")}
        return (v["z"] * 8 + v["y"] * 2 + v["xh"], v["xl"] * 2 + v["c"])

    def ring(self, axis, step):
        return rem(getattr(self, axis) + step + 4, 4)

    def near(self, axis, step):
        return self.dev(**{axis: self.ring(axis, step)})

    def across(self):
        return self.dev(xh=1 - self.xh)

    def chip(self):
        return self.dev(xl=1 - self.xl)

    def core(self):
        return self.dev(c=1 - self.c)


def greet(devices):
    barrier = pltpu.get_barrier_semaphore()
    for d in devices:
        pl.semaphore_signal(barrier, inc=1, device_id=d, device_id_type=MESH)
    pl.semaphore_wait(barrier, len(devices))


def torus_peers(me):
    return [me.near(a, s) for a in ("z", "y") for s in (1, -1)] + [me.across()]


class Sends:
    def __init__(self):
        self.open = []

    def start(self, src, dst, ssem, rsem, dev):
        copy = pltpu.make_async_remote_copy(
            src_ref=src, dst_ref=dst, send_sem=ssem, recv_sem=rsem, device_id=dev, device_id_type=MESH
        )
        copy.start()
        self.open.append(copy)

    def close(self):
        for copy in self.open:
            copy.wait_send()
        self.open = []


def arrive(ref, rsem, dev):
    pltpu.make_async_remote_copy(
        src_ref=ref, dst_ref=ref, send_sem=rsem, recv_sem=rsem, device_id=dev, device_id_type=MESH
    ).wait_recv()


class Gather:
    def __init__(self, me, w, half, col, xb, ssem, rsem, sends):
        self.me, self.w, self.xb, self.ssem, self.rsem, self.sends = me, w, xb, ssem, rsem, sends
        self.axes = ("y", "z") if half == 0 else ("z", "y")
        self.c0 = col + half * HALF

    def part(self, level, step, cols):
        axis = self.axes[level]
        at = {"z": self.me.z, "y": self.me.y}
        at[axis] = self.me.ring(axis, step)
        if level == 1:
            at[self.axes[0]] = slice(None)
        return self.w.at[at["z"], at["y"], self.xb, :, cols]

    def cols(self, which):
        return {
            "all": pl.ds(self.c0, HALF),
            "lo": pl.ds(self.c0, QUART),
            "hi": pl.ds(self.c0 + QUART, QUART),
        }[which]

    def go(self, level, step, which, to, i):
        ref = self.part(level, step, self.cols(which))
        i = level * 4 + i
        self.sends.start(ref, ref, self.ssem.at[i], self.rsem.at[i], self.me.near(self.axes[level], to))

    def got(self, level, step, which, i):
        arrive(self.part(level, step, self.cols(which)), self.rsem.at[level * 4 + i], self.me.near(self.axes[level], 1))

    def first(self, level):
        self.go(level, 0, "all", 1, 0)
        self.go(level, 0, "all", -1, 1)

    def second(self, level):
        self.got(level, -1, "all", 0)
        self.go(level, -1, "lo", 1, 2)
        self.got(level, 1, "all", 1)
        self.go(level, 1, "hi", -1, 3)

    def last(self, level):
        self.got(level, 2, "lo", 2)
        self.got(level, 2, "hi", 3)


def wider(ref_value):
    return ref_value.astype(F32)


class Scatter:
    def __init__(self, me, g, half, col, xb, bufs, ssem, rsem, sends):
        self.me, self.g, self.xb, self.ssem, self.rsem, self.sends = me, g, xb, ssem, rsem, sends
        self.axes = ("z", "y") if half == 0 else ("y", "z")
        self.c0 = col + half * HALF
        self.bufs = bufs

    def spot(self, level, step, which):
        axis = self.axes[level]
        at = {"z": self.me.z, "y": self.me.y}
        at[axis] = self.me.ring(axis, step)
        if level == 0:
            at[self.axes[1]] = slice(None)
        cols = {
            "all": pl.ds(self.c0, HALF),
            "lo": pl.ds(self.c0, QUART),
            "hi": pl.ds(self.c0 + QUART, QUART),
        }[which]
        return (at["z"], at["y"], self.xb, slice(None), cols)

    def far(self, level):
        for to, which, i in ((1, "lo", 0), (-1, "hi", 1)):
            j = level * 4 + i
            self.sends.start(
                self.g.at[self.spot(level, 2, which)], self.bufs[level][0].at[i],
                self.ssem.at[j], self.rsem.at[j], self.me.near(self.axes[level], to),
            )

    def relay(self, level):
        for to, which, i in ((1, "lo", 0), (-1, "hi", 1)):
            buf = self.bufs[level][0].at[i]
            arrive(buf, self.rsem.at[level * 4 + i], self.me.near(self.axes[level], -to))
            spot = self.spot(level, to, which)
            self.g[spot] = (wider(self.g[spot]) + wider(buf[...])).astype(BF16)
        for to, i in ((1, 0), (-1, 1)):
            j = level * 4 + 2 + i
            self.sends.start(
                self.g.at[self.spot(level, to, "all")], self.bufs[level][1].at[i],
                self.ssem.at[j], self.rsem.at[j], self.me.near(self.axes[level], to),
            )

    def total(self, level):
        near = self.bufs[level][1]
        for to, i in ((1, 0), (-1, 1)):
            arrive(near.at[i], self.rsem.at[level * 4 + 2 + i], self.me.near(self.axes[level], -to))
        spot = self.spot(level, 0, "all")
        return spot, wider(self.g[spot]) + wider(near[0]) + wider(near[1])

    def fold(self):
        spot, total = self.total(0)
        self.g[spot] = total.astype(BF16)


def gather_kernel(b_ref, w_ref, ssem, rsem, xs, xr, csem):
    me = Place()
    own = pltpu.make_async_copy(b_ref, w_ref.at[me.z, me.y, me.xh], csem)
    own.start()
    greet(torus_peers(me))
    own.wait()
    sends = Sends()
    pieces = []
    for group in range(3):
        for side in range(2):
            xb = me.xh if side == 0 else 1 - me.xh
            k = (group * 2 + side) * 2
            pieces.append(
                [Gather(me, w_ref, h, group * GROUP, xb, ssem.at[k + h], rsem.at[k + h], sends) for h in range(2)]
            )

    def each(k, what, *args):
        if 0 <= k < len(pieces):
            if what == "first" and args[0] == 0 and k % 2 == 1:
                cols = pl.ds(k // 2 * GROUP, GROUP)
                arrive(w_ref.at[me.z, me.y, 1 - me.xh, :, cols], xr.at[k // 2], me.across())
            for half in pieces[k]:
                getattr(half, what)(*args)

    for group in range(3):
        ref = w_ref.at[me.z, me.y, me.xh, :, pl.ds(group * GROUP, GROUP)]
        sends.start(ref, ref, xs.at[group], xr.at[group], me.across())
    each(0, "first", 0)
    each(0, "second", 0)
    each(1, "first", 0)
    each(0, "last", 0)
    for k in range(len(pieces) + 1):
        each(k, "first", 1)
        each(k + 2, "first", 0)
        each(k + 1, "second", 0)
        each(k - 1, "last", 1)
        each(k, "second", 1)
        each(k + 1, "last", 0)
    sends.close()


def scatter_kernel(g_ref, o_ref, r1, r2, p1, p2, xbuf, part, ssem, rsem, xs, xr):
    me = Place()
    greet(torus_peers(me))
    sends = Sends()
    pieces = []
    for n, group in enumerate((2, 1, 0)):
        for side in range(2):
            xb = 1 - me.xh if side == 0 else me.xh
            k = n * 2 + side
            halves = []
            for h in range(2):
                bufs = ((r1.at[k % 3, h], r2.at[k % 3, h]), (p1.at[k % 3, h], p2.at[k % 3, h]))
                halves.append(
                    Scatter(me, g_ref, h, group * GROUP, xb, bufs, ssem.at[k * 2 + h], rsem.at[k * 2 + h], sends)
                )
            pieces.append((group, side, halves))

    def each(k, what, *args):
        if 0 <= k < len(pieces):
            for half in pieces[k][2]:
                getattr(half, what)(*args)

    def finish(k):
        if not 0 <= k < len(pieces):
            return
        group, side, halves = pieces[k]
        for h, half in enumerate(halves):
            spot, total = half.total(1)
            cols = pl.ds(group * GROUP + h * HALF, HALF)
            if side == 0:
                part[:, cols] = total.astype(BF16)
            else:
                o_ref[:, cols] = total
        if side == 0:
            cols = pl.ds(group * GROUP, GROUP)
            sends.start(part.at[:, cols], xbuf.at[:, cols], xs.at[group], xr.at[group], me.across())
        else:
            cols = pl.ds(group * GROUP, GROUP)
            arrive(xbuf.at[:, cols], xr.at[group], me.across())
            o_ref[:, cols] += wider(xbuf[:, cols])

    each(0, "far", 0)
    for t in range(len(pieces) + 3):
        each(t + 1, "far", 0)
        each(t, "relay", 0)
        each(t - 1, "fold")
        each(t - 1, "far", 1)
        each(t - 2, "relay", 1)
        finish(t - 3)
    sends.close()


DMA = pltpu.SemaphoreType.DMA
VM = pl.BlockSpec(memory_space=pltpu.VMEM)


def params(cid):
    return pltpu.CompilerParams(collective_id=cid, has_side_effects=True, vmem_limit_bytes=60 * 2**20)


def torus_gather(block):
    return pl.pallas_call(
        gather_kernel,
        out_shape=jax.ShapeDtypeStruct((4, 4, 2, ROWS, 3 * GROUP), BF16),
        in_specs=[VM],
        out_specs=VM,
        scratch_shapes=[DMA((12, 8)), DMA((12, 8)), DMA((3,)), DMA((3,)), DMA],
        compiler_params=params(0),
        cost_estimate=pl.CostEstimate(flops=10**10, bytes_accessed=3 * 10**7, transcendentals=0),
    )(block)


def torus_scatter(grads):
    return pl.pallas_call(
        scatter_kernel,
        out_shape=jax.ShapeDtypeStruct((ROWS, 3 * GROUP), F32),
        in_specs=[VM],
        out_specs=VM,
        scratch_shapes=[
            pltpu.VMEM((3, 2, 2, 4, ROWS, QUART), BF16),
            pltpu.VMEM((3, 2, 2, 4, ROWS, HALF), BF16),
            pltpu.VMEM((3, 2, 2, ROWS, QUART), BF16),
            pltpu.VMEM((3, 2, 2, ROWS, HALF), BF16),
            pltpu.VMEM((ROWS, 3 * GROUP), BF16),
            pltpu.VMEM((ROWS, 3 * GROUP), BF16),
            DMA((12, 8)), DMA((12, 8)), DMA((3,)), DMA((3,)),
        ],
        compiler_params=params(1),
        cost_estimate=pl.CostEstimate(flops=10**10, bytes_accessed=3 * 10**7, transcendentals=0),
    )(grads)


def seq_gather_kernel(b_ref, o_ref, ss, rs, csem):
    me = Place()
    own = pltpu.make_async_copy(b_ref, o_ref.at[me.s], csem)
    own.start()
    greet([me.chip(), me.core()])
    own.wait()
    sends = Sends()
    sends.start(o_ref.at[me.s], o_ref.at[me.s], ss.at[0], rs.at[0], me.chip())
    sends.start(o_ref.at[me.s], o_ref.at[me.s], ss.at[1], rs.at[1], me.core())
    other = (1 - me.xl) * 2 + me.c
    arrive(o_ref.at[other], rs.at[0], me.chip())
    sends.start(o_ref.at[other], o_ref.at[other], ss.at[2], rs.at[2], me.core())
    arrive(o_ref.at[me.xl * 2 + 1 - me.c], rs.at[1], me.core())
    arrive(o_ref.at[(1 - me.xl) * 2 + 1 - me.c], rs.at[2], me.core())
    sends.close()


def seq_gather(block, cid):
    own, width = block.shape
    return pl.pallas_call(
        seq_gather_kernel,
        out_shape=jax.ShapeDtypeStruct((4, own, width), BF16),
        in_specs=[VM],
        out_specs=VM,
        scratch_shapes=[DMA((3,)), DMA((3,)), DMA],
        compiler_params=params(cid),
    )(block).reshape(4 * own, width)


def seq_scatter_kernel(p_ref, o_ref, swap, mine, theirs, ss, rs):
    me = Place()
    greet([me.chip(), me.core()])
    sends = Sends()
    for i, xl in enumerate((1 - me.xl, me.xl)):
        sends.start(p_ref.at[xl * 2 + 1 - me.c], swap.at[i], ss.at[i], rs.at[i], me.core())
    arrive(swap.at[0], rs.at[0], me.core())
    mine[...] = (wider(p_ref[(1 - me.xl) * 2 + me.c]) + wider(swap[0])).astype(BF16)
    sends.start(mine, theirs, ss.at[2], rs.at[2], me.chip())
    arrive(swap.at[1], rs.at[1], me.core())
    o_ref[...] = wider(p_ref[me.s]) + wider(swap[1])
    arrive(theirs, rs.at[2], me.chip())
    o_ref[...] += wider(theirs[...])
    sends.close()


def seq_scatter(whole, cid):
    rows, width = whole.shape
    own = rows // 4
    return pl.pallas_call(
        seq_scatter_kernel,
        out_shape=jax.ShapeDtypeStruct((own, width), F32),
        in_specs=[VM],
        out_specs=VM,
        scratch_shapes=[
            pltpu.VMEM((2, own, width), BF16), pltpu.VMEM((own, width), BF16), pltpu.VMEM((own, width), BF16),
            DMA((3,)), DMA((3,)),
        ],
        compiler_params=params(cid),
    )(whole.reshape(4, own, width))


def normalize(stream):
    centred = stream - jnp.mean(stream, axis=-1, keepdims=True)
    rstd = lax.rsqrt(jnp.mean(centred * centred, axis=-1, keepdims=True) + LN_EPS)
    return (centred * rstd, rstd)


def norm_back(normed, rstd, incoming):
    first = jnp.mean(incoming, axis=-1, keepdims=True)
    second = jnp.mean(incoming * normed, axis=-1, keepdims=True)
    return rstd * (incoming - first - normed * second)


def gelu_tanh(hidden):
    return jax.nn.gelu(hidden, approximate=True)


def contract(left, right, left_dim, right_dim):
    return lax.dot_general(
        left, right, (((left_dim,), (right_dim,)), ((), ())), preferred_element_type=F32
    )


def softmax_rows(queries, key_rows, factor):
    scores = contract(queries, key_rows, 1, 1) * factor
    scores = jnp.exp(scores - jnp.max(scores, axis=-1, keepdims=True))
    return scores * (1.0 / jnp.sum(scores, axis=-1, keepdims=True))


def attend_kernel(factor, q_ref, k_ref, v_ref, o_ref):
    probs = softmax_rows(q_ref[...], k_ref[...], factor)
    o_ref[...] = contract(probs.astype(BF16), v_ref[...], 1, 0).astype(BF16)


def attend_back_kernel(factor, heads, q_ref, k_ref, v_ref, do_ref, out_ref):
    head = pl.program_id(0)
    queries, key_rows, upstream = q_ref[...], k_ref[...], do_ref[...]
    probs = softmax_rows(queries, key_rows, factor)
    dprobs = contract(upstream, v_ref[...], 1, 1)
    dscores = probs * (dprobs - jnp.sum(probs * dprobs, axis=-1, keepdims=True)) * factor
    dscores = dscores.astype(BF16)
    parts = (
        contract(dscores, key_rows, 1, 0),
        contract(dscores, queries, 0, 0),
        contract(probs.astype(BF16), upstream, 0, 0),
    )
    for place, part in enumerate(parts):
        column = pl.multiple_of((place * heads + head) * HEAD_DIM, HEAD_DIM)
        out_ref[:, pl.ds(column, HEAD_DIM)] = part.astype(BF16)


def column_spec(seq, heads, place):
    return pl.BlockSpec((seq, HEAD_DIM), lambda head: (0, place * heads + head))


def attend(packed, heads, factor):
    seq = packed.shape[0]
    return pl.pallas_call(
        functools.partial(attend_kernel, factor),
        out_shape=jax.ShapeDtypeStruct((seq, heads * HEAD_DIM), BF16),
        grid=(heads,),
        in_specs=[column_spec(seq, heads, place) for place in range(3)],
        out_specs=column_spec(seq, heads, 0),
    )(packed, packed, packed)


def attend_back(packed, upstream, heads, factor):
    seq = packed.shape[0]
    return pl.pallas_call(
        functools.partial(attend_back_kernel, factor, heads),
        out_shape=jax.ShapeDtypeStruct(packed.shape, BF16),
        grid=(heads,),
        in_specs=[column_spec(seq, heads, place) for place in (0, 1, 2, 0)],
        out_specs=pl.BlockSpec((seq, packed.shape[1]), lambda head: (0, 0)),
    )(packed, packed, packed, upstream)


def local(tokens, modulation, w_qkv, w_out, w_in, w_back, out_grad):
    _, own, width = tokens.shape
    own_width = w_qkv.shape[3]
    heads = own_width // HEAD_DIM
    factor = TEMPER / math.sqrt(HEAD_DIM)
    grad_scale = 1.0 / math.sqrt(own * lax.axis_size("sp") * lax.axis_size("fsdp"))

    def grad_term(left, right):
        return (contract(left, right, 0, 0) * grad_scale).astype(BF16)

    stream = tokens[0].astype(F32)
    mod = modulation[0, 0][:, None, :]
    block = jnp.concatenate([w_qkv[0].reshape(ROWS, 3 * own_width), w_out[0].T, w_in[0], w_back[0].T], axis=1)
    whole = torus_gather(block).reshape(width, 3 * GROUP)
    joint, whole_out = whole[:, : 3 * own_width], whole[:, 3 * own_width : GROUP]
    whole_in, whole_back = whole[:, GROUP : 2 * GROUP], whole[:, 2 * GROUP :]

    n1, r1 = normalize(stream)
    a1 = seq_gather((n1 * (1.0 + mod[1]) + mod[0]).astype(BF16), 2)
    packed = contract(a1, joint, 1, 0).astype(BF16)
    attended = attend(packed, heads, factor)
    middle = stream + mod[2] * seq_scatter(contract(attended, whole_out, 1, 1).astype(BF16), 3)
    n2, r2 = normalize(middle)
    a2 = seq_gather((n2 * (1.0 + mod[4]) + mod[3]).astype(BF16), 4)
    hidden = contract(a2, whole_in, 1, 0)
    active = gelu_tanh(hidden).astype(BF16)
    final = middle + mod[5] * seq_scatter(contract(active, whole_back, 1, 1).astype(BF16), 5)
    grad = out_grad[0].astype(F32)
    dm = seq_gather((mod[5] * grad).astype(BF16), 6)
    dg = contract(dm, whole_back, 1, 0)
    _, pullback = jax.vjp(gelu_tanh, hidden)
    du = pullback(dg)[0].astype(BF16)
    back_second = seq_scatter(contract(du, whole_in, 1, 1).astype(BF16), 7)
    grad = grad + norm_back(n2, r2, back_second * (1.0 + mod[4]))
    da = seq_gather((mod[2] * grad).astype(BF16), 8)
    do = contract(da, whole_out, 1, 0).astype(BF16)
    dqkv = attend_back(packed, do, heads, factor)
    back_first = seq_scatter(contract(dqkv, joint, 1, 1).astype(BF16), 9)
    grad = grad + norm_back(n1, r1, back_first * (1.0 + mod[1]))
    terms = jnp.concatenate(
        [grad_term(a1, dqkv), grad_term(da, attended), grad_term(a2, du), grad_term(dm, active)], axis=1
    )
    sums = torus_scatter(terms.reshape(4, 4, 2, ROWS, 3 * GROUP))
    return (
        final.astype(BF16)[None],
        grad[None],
        sums[:, : 3 * own_width].reshape(1, ROWS, 3, own_width),
        sums[:, 3 * own_width : GROUP].T[None],
        sums[:, GROUP : 2 * GROUP][None],
        sums[:, 2 * GROUP :].T[None],
    )


def solution(mesh):
    weights = (
        P(None, "fsdp", None, "sp"),
        P(None, "sp", "fsdp"),
        P(None, "fsdp", "sp"),
        P(None, "sp", "fsdp"),
    )
    rows = P("fsdp", "sp", None)
    return jax.shard_map(
        local,
        mesh=mesh,
        in_specs=(rows, P("fsdp", None, None, None), *weights, rows),
        out_specs=(rows, rows, *weights),
        check_vma=False,
    )
```

```python
import functools
import math

import jax
import jax.numpy as jnp
from jax import lax
from jax.experimental import pallas as pl
from jax.experimental.pallas import tpu as pltpu
from jax.sharding import PartitionSpec as P

HEAD_DIM = 128
LN_EPS = 1e-06
TEMPER = 2.5
F32 = jnp.float32
BF16 = jnp.bfloat16
MESH = pl.DeviceIdType.MESH
GROUP = 1536
HALF = GROUP // 2
QUART = GROUP // 4
ROWS = 48


def rem(a, n):
    return lax.rem(a, n)


class Place:
    def __init__(self):
        f = lax.axis_index("fsdp")
        s = lax.axis_index("sp")
        self.z, self.y, self.xh = lax.div(f, 8), rem(lax.div(f, 2), 4), rem(f, 2)
        self.xl, self.c = lax.div(s, 2), rem(s, 2)
        self.s = s

    def dev(self, **kw):
        v = {k: kw.get(k, getattr(self, k)) for k in ("z", "y", "xh", "xl", "c")}
        return (v["z"] * 8 + v["y"] * 2 + v["xh"], v["xl"] * 2 + v["c"])

    def ring(self, axis, step):
        return rem(getattr(self, axis) + step + 4, 4)

    def near(self, axis, step):
        return self.dev(**{axis: self.ring(axis, step)})

    def across(self):
        return self.dev(xh=1 - self.xh)

    def chip(self):
        return self.dev(xl=1 - self.xl)

    def core(self):
        return self.dev(c=1 - self.c)


def greet(devices):
    barrier = pltpu.get_barrier_semaphore()
    for d in devices:
        pl.semaphore_signal(barrier, inc=1, device_id=d, device_id_type=MESH)
    pl.semaphore_wait(barrier, len(devices))


def torus_peers(me):
    return [me.near(a, s) for a in ("z", "y") for s in (1, -1)] + [me.across()]


class Sends:
    def __init__(self):
        self.open = []

    def start(self, src, dst, ssem, rsem, dev):
        copy = pltpu.make_async_remote_copy(
            src_ref=src, dst_ref=dst, send_sem=ssem, recv_sem=rsem, device_id=dev, device_id_type=MESH
        )
        copy.start()
        self.open.append(copy)

    def close(self):
        for copy in self.open:
            copy.wait_send()
        self.open = []


def arrive(ref, rsem, dev):
    pltpu.make_async_remote_copy(
        src_ref=ref, dst_ref=ref, send_sem=rsem, recv_sem=rsem, device_id=dev, device_id_type=MESH
    ).wait_recv()


class Gather:
    def __init__(self, me, w, half, col, xb, ssem, rsem, sends):
        self.me, self.w, self.xb, self.ssem, self.rsem, self.sends = me, w, xb, ssem, rsem, sends
        self.axes = ("y", "z") if half == 0 else ("z", "y")
        self.c0 = col + half * HALF

    def part(self, level, step, cols):
        axis = self.axes[level]
        at = {"z": self.me.z, "y": self.me.y}
        at[axis] = self.me.ring(axis, step)
        if level == 1:
            at[self.axes[0]] = slice(None)
        return self.w.at[at["z"], at["y"], self.xb, :, cols]

    def cols(self, which):
        return {
            "all": pl.ds(self.c0, HALF),
            "lo": pl.ds(self.c0, QUART),
            "hi": pl.ds(self.c0 + QUART, QUART),
        }[which]

    def go(self, level, step, which, to, i):
        ref = self.part(level, step, self.cols(which))
        i = level * 4 + i
        self.sends.start(ref, ref, self.ssem.at[i], self.rsem.at[i], self.me.near(self.axes[level], to))

    def got(self, level, step, which, i):
        arrive(self.part(level, step, self.cols(which)), self.rsem.at[level * 4 + i], self.me.near(self.axes[level], 1))

    def first(self, level):
        self.go(level, 0, "all", 1, 0)
        self.go(level, 0, "all", -1, 1)

    def second(self, level):
        self.got(level, -1, "all", 0)
        self.go(level, -1, "lo", 1, 2)
        self.got(level, 1, "all", 1)
        self.go(level, 1, "hi", -1, 3)

    def last(self, level):
        self.got(level, 2, "lo", 2)
        self.got(level, 2, "hi", 3)


def wider(ref_value):
    return ref_value.astype(F32)


def pack(total):
    return total.astype(BF16)


class Scatter:
    def __init__(self, me, g, half, xb, bufs, ssem, rsem, sends):
        self.me, self.g, self.xb, self.ssem, self.rsem, self.sends = me, g, xb, ssem, rsem, sends
        self.axes = ("z", "y") if half == 0 else ("y", "z")
        self.c0 = half * HALF
        self.bufs = bufs

    def spot(self, level, step, which):
        axis = self.axes[level]
        at = {"z": self.me.z, "y": self.me.y}
        at[axis] = self.me.ring(axis, step)
        if level == 0:
            at[self.axes[1]] = slice(None)
        cols = {
            "all": pl.ds(self.c0, HALF),
            "lo": pl.ds(self.c0, QUART),
            "hi": pl.ds(self.c0 + QUART, QUART),
        }[which]
        return (at["z"], at["y"], self.xb, slice(None), cols)

    def far(self, level):
        for to, which, i in ((1, "lo", 0), (-1, "hi", 1)):
            j = level * 4 + i
            self.sends.start(
                self.g.at[self.spot(level, 2, which)], self.bufs[level][0].at[i],
                self.ssem.at[j], self.rsem.at[j], self.me.near(self.axes[level], to),
            )

    def relay(self, level):
        for to, which, i in ((1, "lo", 0), (-1, "hi", 1)):
            buf = self.bufs[level][0].at[i]
            arrive(buf, self.rsem.at[level * 4 + i], self.me.near(self.axes[level], -to))
            spot = self.spot(level, to, which)
            self.g[spot] = (wider(self.g[spot]) + wider(buf[...])).astype(BF16)
        for to, i in ((1, 0), (-1, 1)):
            j = level * 4 + 2 + i
            self.sends.start(
                self.g.at[self.spot(level, to, "all")], self.bufs[level][1].at[i],
                self.ssem.at[j], self.rsem.at[j], self.me.near(self.axes[level], to),
            )

    def total(self, level):
        near = self.bufs[level][1]
        for to, i in ((1, 0), (-1, 1)):
            arrive(near.at[i], self.rsem.at[level * 4 + 2 + i], self.me.near(self.axes[level], -to))
        spot = self.spot(level, 0, "all")
        return spot, wider(self.g[spot]) + wider(near[0]) + wider(near[1])

    def fold(self):
        spot, total = self.total(0)
        self.g[spot] = total.astype(BF16)


DMA = pltpu.SemaphoreType.DMA
VM = pl.BlockSpec(memory_space=pltpu.VMEM)
OWN = 128
WIDTH = 1536
HEADS = 3
QKV = HEADS * HEAD_DIM
GELU_A = math.sqrt(2.0 / math.pi)
GELU_B = 0.044715


class SeqGather:
    def __init__(self, me, buf, ssem, rsem, sends):
        self.me, self.buf, self.ssem, self.rsem, self.sends = me, buf, ssem, rsem, sends

    def push(self, block, i, dev):
        self.sends.start(self.buf.at[block], self.buf.at[block], self.ssem.at[i], self.rsem.at[i], dev)

    def start(self):
        self.push(self.me.s, 0, self.me.chip())
        self.push(self.me.s, 1, self.me.core())

    def relay(self):
        other = (1 - self.me.xl) * 2 + self.me.c
        arrive(self.buf.at[other], self.rsem.at[0], self.me.chip())
        self.push(other, 2, self.me.core())

    def near(self):
        arrive(self.buf.at[self.me.xl * 2 + 1 - self.me.c], self.rsem.at[1], self.me.core())

    def far(self):
        arrive(self.buf.at[(1 - self.me.xl) * 2 + 1 - self.me.c], self.rsem.at[2], self.me.core())


class SeqScatter:
    def __init__(self, me, part, swap, mine, theirs, ssem, rsem):
        self.me, self.part, self.swap, self.mine, self.theirs = me, part, swap, mine, theirs
        self.ssem, self.rsem, self.sends = ssem, rsem, Sends()

    def give(self, i):
        xl = self.me.xl if i else 1 - self.me.xl
        self.sends.start(
            self.part.at[xl * 2 + 1 - self.me.c], self.swap.at[i], self.ssem.at[i], self.rsem.at[i], self.me.core()
        )

    def cross(self):
        arrive(self.swap.at[0], self.rsem.at[0], self.me.core())

        @pl.loop(0, 4)
        def _(i):
            r = pl.ds(i * 32, 32)
            self.mine[r] = pack(wider(self.part[(1 - self.me.xl) * 2 + self.me.c, r]) + wider(self.swap[0, r]))

        self.sends.start(self.mine, self.theirs, self.ssem.at[2], self.rsem.at[2], self.me.chip())

    def wait(self):
        arrive(self.swap.at[1], self.rsem.at[1], self.me.core())
        arrive(self.theirs, self.rsem.at[2], self.me.chip())

    def rows(self, r):
        return wider(self.part[self.me.s, r]) + wider(self.swap[1, r]) + wider(self.theirs[r])


def normalize(stream):
    centred = stream - jnp.mean(stream, axis=-1, keepdims=True)
    rstd = lax.rsqrt(jnp.mean(centred * centred, axis=-1, keepdims=True) + LN_EPS)
    return (centred * rstd, rstd)


def norm_back(normed, rstd, incoming):
    first = jnp.mean(incoming, axis=-1, keepdims=True)
    second = jnp.mean(incoming * normed, axis=-1, keepdims=True)
    return rstd * (incoming - first - normed * second)


def contract(left, right, left_dim, right_dim):
    return lax.dot_general(
        left, right, (((left_dim,), (right_dim,)), ((), ())), preferred_element_type=F32
    )


def softmax_rows(queries, key_rows, factor):
    scores = contract(queries, key_rows, 1, 1) * factor
    scores = jnp.exp(scores - jnp.max(scores, axis=-1, keepdims=True))
    return scores * (1.0 / jnp.sum(scores, axis=-1, keepdims=True))


def by_rows(body):
    @pl.loop(0, OWN // 32)
    def _(i):
        body(pl.ds(pl.multiple_of(i * 32, 32), 32))


def step_kernel(
    grad_scale, factor,
    tok, mod, blk, og,
    final, grad, oq, oo, oi, ob,
    w, g, r1, r2, p1, p2, xbuf, part, a1, a2, dm, da, packed, att, datt, act, slope, du,
    pa, pb, swaps, mines, theirs, middle,
    gs, gr, ss, rs, xs, xr, ys, yr, es, er, csem,
):
    me = Place()
    own = pltpu.make_async_copy(blk, w.at[me.z, me.y, me.xh], csem)
    own.start()
    greet(torus_peers(me) + [me.chip(), me.core()])
    own.wait()
    mine, other = me.xl, 1 - me.xl

    def m(i):
        return mod[pl.ds(i, 1), :]

    sends = Sends()
    pieces = []
    for group in range(3):
        for side in range(2):
            xb = me.xh if side == 0 else 1 - me.xh
            k = (group * 2 + side) * 2
            pieces.append([Gather(me, w, h, group * GROUP, xb, gs.at[k + h], gr.at[k + h], sends) for h in range(2)])

    def gather_event(k, what, level):
        if what == "first" and level == 0 and k % 2 == 1:
            arrive(w.at[me.z, me.y, 1 - me.xh, :, pl.ds(k // 2 * GROUP, GROUP)], xr.at[k // 2], me.across())
        for half in pieces[k]:
            getattr(half, what)(level)

    def cross(group):
        ref = w.at[me.z, me.y, me.xh, :, pl.ds(group * GROUP, GROUP)]
        sends.start(ref, ref, xs.at[group], xr.at[group], me.across())

    events = [(0, "first", 0), (0, "second", 0), (1, "first", 0), (0, "last", 0)]
    for k in range(7):
        events += [
            (k, "first", 1), (k + 2, "first", 0), (k + 1, "second", 0),
            (k - 1, "last", 1), (k, "second", 1), (k + 1, "last", 0),
        ]
    events = [e for e in events if 0 <= e[0] < 6]

    def ag(*upto):
        while events:
            event = events.pop(0)
            gather_event(*event)
            if event == upto:
                return

    scatters = []
    for n, group in enumerate((2, 1, 0)):
        for side in range(2):
            xb = 1 - me.xh if side == 0 else me.xh
            k = n * 2 + side
            halves = []
            for h in range(2):
                bufs = ((r1.at[k % 3, h], r2.at[k % 3, h]), (p1.at[k % 3, h], p2.at[k % 3, h]))
                halves.append(Scatter(me, g.at[group], h, xb, bufs, ss.at[k * 2 + h], rs.at[k * 2 + h], sends))
            scatters.append((group, side, halves))

    def slots(group, h):
        if group == 0:
            outs = ((oq.at[0], oq.at[1]), (oq.at[2], oo))[h]
            return [(outs[i], slice(i * QUART, (i + 1) * QUART)) for i in range(2)]
        ref = oi if group == 1 else ob
        return [(ref.at[:, pl.ds(h * HALF, HALF)], slice(0, HALF))]

    def finish(k):
        group, side, halves = scatters[k]
        cols = pl.ds(group * GROUP, GROUP)
        if side == 1:
            arrive(xbuf.at[:, cols], yr.at[group], me.across())
        for h, half in enumerate(halves):
            _, total = half.total(1)
            here = pl.ds(group * GROUP + h * HALF, HALF)
            if side == 0:
                part[:, here] = pack(total)
            else:
                total = total + wider(xbuf[:, here])
                for ref, sl in slots(group, h):
                    ref[...] = total[:, sl]
        if side == 0:
            sends.start(part.at[:, cols], xbuf.at[:, cols], ys.at[group], yr.at[group], me.across())

    def scatter_event(k, what, *args):
        if what == "finish":
            finish(k)
        else:
            for half in scatters[k][2]:
                getattr(half, what)(*args)

    reduce = [(0, "far", 0)]
    for t in range(9):
        reduce += [
            (t + 1, "far", 0), (t, "relay", 0), (t - 1, "fold"),
            (t - 1, "far", 1), (t - 2, "relay", 1), (t - 3, "finish"),
        ]
    reduce = [e for e in reduce if 0 <= e[0] < 6]

    def rsc(*upto):
        while reduce:
            event = reduce.pop(0)
            scatter_event(*event)
            if event == upto:
                return

    def rows_of(ref, side, cols=slice(None)):
        value = ref[pl.ds(side * 2, 2), :, cols]
        return value.reshape(2 * OWN, value.shape[-1])

    def forward(src, side, col, width, tile, emit):
        @pl.loop(0, width // tile)
        def _(j):
            at = pl.multiple_of(j * tile, 128)
            weight = w[:, :, :, :, pl.ds(col + at, tile)].reshape(WIDTH, tile)
            emit(pl.ds(at, tile), contract(rows_of(src, side), weight, 1, 0).reshape(2, OWN, tile))

    def backward(src, side, col, width, out):
        @pl.loop(0, 2)
        def _(j):
            weight = w[pl.ds(j * 2, 2), :, :, :, pl.ds(col, width)].reshape(HALF, width)
            at = pl.multiple_of(j * HALF, 128)
            value = contract(rows_of(src, side), weight, 1, 1)
            out[pl.ds(side * 2, 2), :, pl.ds(at, HALF)] = pack(value).reshape(2, OWN, HALF)

    def gradient(left, right, group, col, width):
        @pl.loop(0, 4)
        def _(j):
            rows = left[:, :, pl.ds(pl.multiple_of(j * 384, 128), 384)].reshape(4 * OWN, 384)
            value = contract(rows, right[...].reshape(4 * OWN, width), 0, 0) * grad_scale
            g[group, j, :, :, :, pl.ds(col, width)] = pack(value).reshape(4, 2, ROWS, width)

    gather = [SeqGather(me, buf, es.at[i], er.at[i], sends) for i, buf in enumerate((a1, a2, dm, da))]
    give = [
        SeqScatter(me, (pa, pa, pa, pb)[i], swaps.at[i // 3], mines.at[i // 3], theirs.at[i // 3], es.at[4 + i], er.at[4 + i])
        for i in range(4)
    ]
    x_a1, x_a2, x_dm, x_da = gather
    y_att, y_back, y_first, y_ffn = give

    def share(y, src, col, width, close=None):
        backward(src, other, col, width, y.part)
        y.give(0)
        backward(src, mine, col, width, y.part)
        y.give(1)
        y.cross()

    cross(0)
    ag(0, "first", 0)

    def first_norm(r):
        n1, _ = normalize(wider(tok[r]))
        a1[me.s, r] = pack(n1 * (1.0 + m(1)) + m(0))

    by_rows(first_norm)
    x_a1.start()
    cross(1)
    cross(2)

    def gate(r):
        dm[me.s, r] = pack(m(5) * wider(og[r]))

    by_rows(gate)
    ag(1, "second", 0)
    x_a1.relay()
    ag(2, "last", 0)
    x_a1.near()
    x_a1.far()
    x_dm.start()
    ag(1, "last", 1)

    def put_qkv(side):
        def emit(cols, value):
            packed[pl.ds(side * 2, 2), :, cols] = pack(value)
        return emit

    forward(a1, mine, 0, 3 * QKV, QKV, put_qkv(mine))
    forward(a1, other, 0, 3 * QKV, QKV, put_qkv(other))
    ag(5, "first", 0)
    x_dm.relay()

    def head_cols(place, head):
        return pl.ds(pl.multiple_of(place * QKV + head * HEAD_DIM, HEAD_DIM), HEAD_DIM)

    def head_rows(ref, cols):
        return ref[:, :, cols].reshape(4 * OWN, HEAD_DIM)

    @pl.loop(0, HEADS)
    def _(head):
        q, k, v = (head_rows(packed, head_cols(i, head)) for i in range(3))
        probs = softmax_rows(q, k, factor)
        att[:, :, head_cols(0, head)] = pack(contract(pack(probs), v, 1, 0)).reshape(4, OWN, HEAD_DIM)

    share(y_att, att, 3 * QKV, QKV)
    x_dm.near()
    x_dm.far()
    ag(4, "first", 1)
    y_att.wait()

    def second_norm(r):
        mid = wider(tok[r]) + m(2) * y_att.rows(r)
        middle[r] = mid
        n2, _ = normalize(mid)
        a2[me.s, r] = pack(n2 * (1.0 + m(4)) + m(3))

    by_rows(second_norm)
    y_att.sends.close()
    x_a2.start()
    ag(3, "last", 1)
    x_a2.near()

    def put_hidden(side):
        def emit(cols, u):
            t = jnp.tanh(GELU_A * (u + GELU_B * (u * u * u)))
            at = (pl.ds(side * 2, 2), slice(None), cols)
            act[at] = pack(0.5 * u * (1.0 + t))
            slope[at] = 0.5 * (1.0 + t) + (0.5 * GELU_A) * u * (1.0 - t * t) * (1.0 + (3.0 * GELU_B) * (u * u))
        return emit

    forward(a2, mine, GROUP, GROUP, 512, put_hidden(mine))
    ag(5, "first", 1)
    x_a2.relay()
    ag(4, "last", 1)
    x_a2.far()
    forward(a2, other, GROUP, GROUP, 512, put_hidden(other))
    ag(5, "second", 1)

    gradient(dm, act, 2, 0, GROUP)
    rsc(1, "far", 0)
    ag()

    def put_du(side):
        def emit(cols, dg):
            at = (pl.ds(side * 2, 2), slice(None), cols)
            du[at] = pack(slope[at] * dg)
        return emit

    forward(dm, other, 2 * GROUP, GROUP, 512, put_du(other))
    forward(dm, mine, 2 * GROUP, GROUP, 512, put_du(mine))
    share(y_back, du, GROUP, GROUP)
    rsc(0, "relay", 0)
    gradient(a2, du, 1, 0, GROUP)
    rsc(1, "relay", 0)
    y_back.wait()

    def middle_back(r):
        n2, rstd = normalize(middle[r])
        up = wider(og[r]) + norm_back(n2, rstd, y_back.rows(r) * (1.0 + m(4)))
        grad[r] = up
        da[me.s, r] = pack(m(2) * up)

    by_rows(middle_back)
    y_back.sends.close()
    x_da.start()
    rsc(3, "far", 0)
    backward(act, other, 2 * GROUP, GROUP, pb)
    backward(act, mine, 2 * GROUP, GROUP, pb)
    x_da.relay()
    x_da.near()
    y_ffn.give(0)
    y_ffn.give(1)

    def put_do(side):
        def emit(cols, value):
            datt[pl.ds(side * 2, 2), :, cols] = pack(value)
        return emit

    forward(da, mine, 3 * QKV, QKV, QKV, put_do(mine))
    x_da.far()
    y_ffn.cross()
    forward(da, other, 3 * QKV, QKV, QKV, put_do(other))
    rsc(2, "relay", 0)

    @pl.loop(0, HEADS)
    def _(head):
        q, k, v = (head_rows(packed, head_cols(i, head)) for i in range(3))
        up = head_rows(datt, head_cols(0, head))
        probs = softmax_rows(q, k, factor)
        dprobs = contract(up, v, 1, 1)
        dscores = pack(probs * (dprobs - jnp.sum(probs * dprobs, axis=-1, keepdims=True)) * factor)
        parts = (contract(dscores, k, 1, 0), contract(dscores, q, 0, 0), contract(pack(probs), up, 0, 0))
        for i, value in enumerate(parts):
            packed[:, :, head_cols(i, head)] = pack(value).reshape(4, OWN, HEAD_DIM)

    share(y_first, packed, 0, 3 * QKV)
    rsc(0, "relay", 1)
    gradient(a1, packed, 0, 0, 3 * QKV)
    gradient(da, att, 0, 3 * QKV, QKV)
    rsc(3, "relay", 0)
    y_ffn.wait()

    def last_out(r):
        final[r] = pack(middle[r] + m(5) * y_ffn.rows(r))

    by_rows(last_out)
    rsc(2, "far", 1)
    y_first.wait()

    def first_back(r):
        n1, rstd = normalize(wider(tok[r]))
        grad[r] = grad[r] + norm_back(n1, rstd, y_first.rows(r) * (1.0 + m(1)))

    by_rows(first_back)
    rsc()
    sends.close()
    y_first.sends.close()
    y_ffn.sends.close()


def local(tokens, modulation, w_qkv, w_out, w_in, w_back, out_grad):
    grad_scale = 1.0 / math.sqrt(OWN * lax.axis_size("sp") * lax.axis_size("fsdp"))
    factor = TEMPER / math.sqrt(HEAD_DIM)
    block = jnp.concatenate([w_qkv[0].reshape(ROWS, 3 * QKV), w_out[0].T, w_in[0], w_back[0].T], axis=1)

    def shape(dims, dtype=BF16):
        return jax.ShapeDtypeStruct(dims, dtype)

    def vm(*dims, dtype=BF16):
        return pltpu.VMEM(dims, dtype)

    seq = (4, OWN, WIDTH)
    final, grad, oq, oo, oi, ob = pl.pallas_call(
        functools.partial(step_kernel, grad_scale, factor),
        out_shape=(
            shape((OWN, WIDTH)), shape((OWN, WIDTH), F32), shape((3, ROWS, QKV), F32),
            shape((ROWS, QKV), F32), shape((ROWS, GROUP), F32), shape((ROWS, GROUP), F32),
        ),
        in_specs=[VM] * 4,
        out_specs=(VM,) * 6,
        scratch_shapes=[
            vm(4, 4, 2, ROWS, 3 * GROUP), vm(3, 4, 4, 2, ROWS, GROUP),
            vm(3, 2, 2, 4, ROWS, QUART), vm(3, 2, 2, 4, ROWS, HALF),
            vm(3, 2, 2, ROWS, QUART), vm(3, 2, 2, ROWS, HALF),
            vm(ROWS, 3 * GROUP), vm(ROWS, 3 * GROUP),
            vm(*seq), vm(*seq), vm(*seq), vm(*seq),
            vm(4, OWN, 3 * QKV), vm(4, OWN, QKV), vm(4, OWN, QKV),
            vm(*seq), vm(*seq, dtype=F32), vm(*seq),
            vm(*seq), vm(*seq), vm(2, 2, OWN, WIDTH), vm(2, OWN, WIDTH), vm(2, OWN, WIDTH),
            vm(OWN, WIDTH, dtype=F32),
            DMA((12, 8)), DMA((12, 8)), DMA((12, 8)), DMA((12, 8)),
            DMA((3,)), DMA((3,)), DMA((3,)), DMA((3,)), DMA((8, 3)), DMA((8, 3)), DMA,
        ],
        compiler_params=pltpu.CompilerParams(
            collective_id=0, has_side_effects=True, vmem_limit_bytes=67043328
        ),
    )(tokens[0], modulation[0, 0], block, out_grad[0])
    return (
        final[None], grad[None], oq.transpose(1, 0, 2)[None], oo.T[None], oi[None], ob.T[None],
    )


def solution(mesh):
    weights = (
        P(None, "fsdp", None, "sp"),
        P(None, "sp", "fsdp"),
        P(None, "fsdp", "sp"),
        P(None, "sp", "fsdp"),
    )
    rows = P("fsdp", "sp", None)
    return jax.shard_map(
        local,
        mesh=mesh,
        in_specs=(rows, P("fsdp", None, None, None), *weights, rows),
        out_specs=(rows, rows, *weights),
        check_vma=False,
    )
```

```python
import functools
import math

import jax
import jax.numpy as jnp
from jax import lax
from jax.experimental import pallas as pl
from jax.experimental.pallas import tpu as pltpu
from jax.sharding import PartitionSpec as P

HEAD_DIM = 128
LN_EPS = 1e-06
TEMPER = 2.5
F32 = jnp.float32
BF16 = jnp.bfloat16
MESH = pl.DeviceIdType.MESH
GROUP = 1536
HALF = GROUP // 2
QUART = GROUP // 4
ROWS = 48


def rem(a, n):
    return lax.rem(a, n)


class Place:
    def __init__(self):
        f = lax.axis_index("fsdp")
        s = lax.axis_index("sp")
        self.z, self.y, self.xh = lax.div(f, 8), rem(lax.div(f, 2), 4), rem(f, 2)
        self.xl, self.c = lax.div(s, 2), rem(s, 2)
        self.s = s
        self.x = self.xh * 2 + self.xl
        self.n = self.x * 2 + self.c

    def dev(self, **kw):
        v = {k: kw.get(k, getattr(self, k)) for k in ("z", "y", "xh", "xl", "c")}
        return (v["z"] * 8 + v["y"] * 2 + v["xh"], v["xl"] * 2 + v["c"])

    def ring(self, axis, step):
        return rem(getattr(self, axis) + step + 4, 4)

    def near(self, axis, step):
        return self.dev(**{axis: self.ring(axis, step)})

    def along(self, step):
        x = rem(self.x + step + 4, 4)
        return self.dev(xh=lax.div(x, 2), xl=rem(x, 2))

    def chip_at(self, step):
        return rem(self.x + step + 4, 4)

    def across(self):
        return self.dev(xh=1 - self.xh)

    def chip(self):
        return self.dev(xl=1 - self.xl)

    def core(self):
        return self.dev(c=1 - self.c)


def greet(devices):
    barrier = pltpu.get_barrier_semaphore()
    for d in devices:
        pl.semaphore_signal(barrier, inc=1, device_id=d, device_id_type=MESH)
    pl.semaphore_wait(barrier, len(devices))


def torus_peers(me):
    return [me.near(a, s) for a in ("z", "y") for s in (1, -1)] + [me.across(), me.along(1), me.along(-1), me.core()]


class Sends:
    def __init__(self):
        self.open = []

    def start(self, src, dst, ssem, rsem, dev):
        copy = pltpu.make_async_remote_copy(
            src_ref=src, dst_ref=dst, send_sem=ssem, recv_sem=rsem, device_id=dev, device_id_type=MESH
        )
        copy.start()
        self.open.append(copy)

    def close(self):
        for copy in self.open:
            copy.wait_send()
        self.open = []


def arrive(ref, rsem, dev):
    pltpu.make_async_remote_copy(
        src_ref=ref, dst_ref=ref, send_sem=rsem, recv_sem=rsem, device_id=dev, device_id_type=MESH
    ).wait_recv()


class Gather:
    def __init__(self, me, w, half, col, xb, ssem, rsem, sends):
        self.me, self.w, self.xb, self.ssem, self.rsem, self.sends = me, w, xb, ssem, rsem, sends
        self.axes = ("y", "z") if half == 0 else ("z", "y")
        self.c0 = col + half * HALF

    def part(self, level, step, cols):
        axis = self.axes[level]
        at = {"z": self.me.z, "y": self.me.y}
        at[axis] = self.me.ring(axis, step)
        if level == 1:
            at[self.axes[0]] = slice(None)
        return self.w.at[at["z"], at["y"], self.xb, :, cols]

    def cols(self, which):
        return {
            "all": pl.ds(self.c0, HALF),
            "lo": pl.ds(self.c0, QUART),
            "hi": pl.ds(self.c0 + QUART, QUART),
        }[which]

    def go(self, level, step, which, to, i):
        ref = self.part(level, step, self.cols(which))
        i = level * 4 + i
        self.sends.start(ref, ref, self.ssem.at[i], self.rsem.at[i], self.me.near(self.axes[level], to))

    def got(self, level, step, which, i):
        arrive(self.part(level, step, self.cols(which)), self.rsem.at[level * 4 + i], self.me.near(self.axes[level], 1))

    def first(self, level):
        self.go(level, 0, "all", 1, 0)
        self.go(level, 0, "all", -1, 1)

    def second(self, level):
        self.got(level, -1, "all", 0)
        self.go(level, -1, "lo", 1, 2)
        self.got(level, 1, "all", 1)
        self.go(level, 1, "hi", -1, 3)

    def last(self, level):
        self.got(level, 2, "lo", 2)
        self.got(level, 2, "hi", 3)


def wider(ref_value):
    return ref_value.astype(F32)


def pack(total):
    return total.astype(BF16)


class Scatter:
    def __init__(self, me, g, half, xb, bufs, ssem, rsem, sends):
        self.me, self.g, self.xb, self.ssem, self.rsem, self.sends = me, g, xb, ssem, rsem, sends
        self.axes = ("z", "y") if half == 0 else ("y", "z")
        self.c0 = half * HALF
        self.bufs = bufs

    def spot(self, level, step, which):
        axis = self.axes[level]
        at = {"z": self.me.z, "y": self.me.y}
        at[axis] = self.me.ring(axis, step)
        if level == 0:
            at[self.axes[1]] = slice(None)
        cols = {
            "all": pl.ds(self.c0, HALF),
            "lo": pl.ds(self.c0, QUART),
            "hi": pl.ds(self.c0 + QUART, QUART),
        }[which]
        return (at["z"], at["y"], self.xb, slice(None), cols)

    def far(self, level):
        for to, which, i in ((1, "lo", 0), (-1, "hi", 1)):
            j = level * 4 + i
            self.sends.start(
                self.g.at[self.spot(level, 2, which)], self.bufs[level][0].at[i],
                self.ssem.at[j], self.rsem.at[j], self.me.near(self.axes[level], to),
            )

    def relay(self, level):
        for to, which, i in ((1, "lo", 0), (-1, "hi", 1)):
            buf = self.bufs[level][0].at[i]
            arrive(buf, self.rsem.at[level * 4 + i], self.me.near(self.axes[level], -to))
            spot = self.spot(level, to, which)
            self.g[spot] = (wider(self.g[spot]) + wider(buf[...])).astype(BF16)
        for to, i in ((1, 0), (-1, 1)):
            j = level * 4 + 2 + i
            self.sends.start(
                self.g.at[self.spot(level, to, "all")], self.bufs[level][1].at[i],
                self.ssem.at[j], self.rsem.at[j], self.me.near(self.axes[level], to),
            )

    def total(self, level):
        near = self.bufs[level][1]
        for to, i in ((1, 0), (-1, 1)):
            arrive(near.at[i], self.rsem.at[level * 4 + 2 + i], self.me.near(self.axes[level], -to))
        spot = self.spot(level, 0, "all")
        return spot, wider(self.g[spot]) + wider(near[0]) + wider(near[1])

    def fold(self):
        spot, total = self.total(0)
        self.g[spot] = total.astype(BF16)


DMA = pltpu.SemaphoreType.DMA
VM = pl.BlockSpec(memory_space=pltpu.VMEM)
ANY = pl.BlockSpec(memory_space=pl.ANY)
OWN = 128
WIDTH = 1536
HEADS = 3
QKV = HEADS * HEAD_DIM
GELU_A = math.sqrt(2.0 / math.pi)
GELU_B = 0.044715


class SeqGather:
    def __init__(self, me, buf, ssem, rsem, sends):
        self.me, self.buf, self.ssem, self.rsem, self.sends = me, buf, ssem, rsem, sends

    def push(self, block, i, dev):
        self.sends.start(self.buf.at[block], self.buf.at[block], self.ssem.at[i], self.rsem.at[i], dev)

    def start(self):
        self.push(self.me.s, 0, self.me.chip())
        self.push(self.me.s, 1, self.me.core())

    def relay(self):
        other = (1 - self.me.xl) * 2 + self.me.c
        arrive(self.buf.at[other], self.rsem.at[0], self.me.chip())
        self.push(other, 2, self.me.core())

    def near(self):
        arrive(self.buf.at[self.me.xl * 2 + 1 - self.me.c], self.rsem.at[1], self.me.core())

    def far(self):
        arrive(self.buf.at[(1 - self.me.xl) * 2 + 1 - self.me.c], self.rsem.at[2], self.me.core())


class SeqScatter:
    def __init__(self, me, part, swap, mine, theirs, ssem, rsem):
        self.me, self.part, self.swap, self.mine, self.theirs = me, part, swap, mine, theirs
        self.ssem, self.rsem, self.sends = ssem, rsem, Sends()

    def give(self, i):
        xl = self.me.xl if i else 1 - self.me.xl
        self.sends.start(
            self.part.at[xl * 2 + 1 - self.me.c], self.swap.at[i], self.ssem.at[i], self.rsem.at[i], self.me.core()
        )

    def cross(self):
        arrive(self.swap.at[0], self.rsem.at[0], self.me.core())

        @pl.loop(0, 4)
        def _(i):
            r = pl.ds(i * 32, 32)
            self.mine[r] = pack(wider(self.part[(1 - self.me.xl) * 2 + self.me.c, r]) + wider(self.swap[0, r]))

        self.sends.start(self.mine, self.theirs, self.ssem.at[2], self.rsem.at[2], self.me.chip())

    def wait(self):
        arrive(self.swap.at[1], self.rsem.at[1], self.me.core())
        arrive(self.theirs, self.rsem.at[2], self.me.chip())

    def rows(self, r):
        return wider(self.part[self.me.s, r]) + wider(self.swap[1, r]) + wider(self.theirs[r])


LEFT, RIGHT = pl.ds(0, HALF), pl.ds(HALF, HALF)


class RingGather:
    def __init__(self, me, buf, ssem, rsem, sends):
        self.me, self.buf, self.ssem, self.rsem, self.sends = me, buf, ssem, rsem, sends

    def at(self, step, mine=True, cols=pl.ds(0, WIDTH)):
        return self.buf.at[self.me.chip_at(step) * 2 + (self.me.c if mine else 1 - self.me.c), :, cols]

    def push(self, ref, i, dev):
        self.sends.start(ref, ref, self.ssem.at[i], self.rsem.at[i], dev)

    def start(self):
        self.push(self.at(0), 0, self.me.along(1))
        self.push(self.at(0), 1, self.me.along(-1))
        self.push(self.at(0), 2, self.me.core())

    def relay(self):
        for step, cols, i in ((-1, LEFT, 0), (1, RIGHT, 1)):
            arrive(self.at(step), self.rsem.at[i], self.me.core())
            self.push(self.at(step, cols=cols), 3 + i, self.me.along(-step))
            self.push(self.at(step), 5 + i, self.me.core())

    def last(self):
        for cols, i in ((LEFT, 0), (RIGHT, 1)):
            arrive(self.at(2, cols=cols), self.rsem.at[3 + i], self.me.core())
            self.push(self.at(2, cols=cols), 7 + i, self.me.core())

    def own(self):
        arrive(self.at(0, False), self.rsem.at[2], self.me.core())

    def sides(self):
        for step, i in ((-1, 5), (1, 6)):
            arrive(self.at(step, False), self.rsem.at[i], self.me.core())

    def far(self):
        for cols, i in ((LEFT, 7), (RIGHT, 8)):
            arrive(self.at(2, False, cols), self.rsem.at[i], self.me.core())


class RingScatter:
    order = (2, 1, -1, 0)

    def __init__(self, me, part, swap, away, near, ssem, rsem):
        self.me, self.part, self.swap, self.away, self.near = me, part, swap, away, near
        self.ssem, self.rsem, self.sends = ssem, rsem, Sends()

    def block(self, step):
        return self.me.chip_at(step) * 2 + self.me.c

    def give(self, j):
        src = self.part.at[self.me.chip_at(self.order[j]) * 2 + 1 - self.me.c]
        self.sends.start(src, self.swap.at[j], self.ssem.at[j], self.rsem.at[j], self.me.core())

    def out(self):
        arrive(self.swap.at[0], self.rsem.at[0], self.me.core())
        block = self.block(2)

        def merge(r):
            self.part[block, r] = pack(wider(self.part[block, r]) + wider(self.swap[0, r]))

        by_rows(merge)
        for cols, step, i in ((LEFT, 1, 0), (RIGHT, -1, 1)):
            self.sends.start(
                self.part.at[block, :, cols], self.away.at[i], self.ssem.at[4 + i], self.rsem.at[4 + i], self.me.along(step)
            )

    def relay(self):
        for step, j, i, same, rest in ((1, 1, 0, LEFT, RIGHT), (-1, 2, 1, RIGHT, LEFT)):
            arrive(self.swap.at[j], self.rsem.at[j], self.me.core())
            arrive(self.away.at[i], self.rsem.at[4 + i], self.me.core())
            block = self.block(step)

            def merge(r):
                both = wider(self.part[block, r, same]) + wider(self.swap[j, r, same])
                self.part[block, r, same] = pack(both + wider(self.away[i, r]))
                self.part[block, r, rest] = pack(wider(self.part[block, r, rest]) + wider(self.swap[j, r, rest]))

            by_rows(merge)
            self.sends.start(
                self.part.at[block], self.near.at[i], self.ssem.at[6 + i], self.rsem.at[6 + i], self.me.along(step)
            )

    def wait(self):
        arrive(self.swap.at[3], self.rsem.at[3], self.me.core())
        for i in range(2):
            arrive(self.near.at[i], self.rsem.at[6 + i], self.me.core())

    def rows(self, r):
        own = wider(self.part[self.block(0), r]) + wider(self.swap[3, r])
        return own + (wider(self.near[0, r]) + wider(self.near[1, r]))


def normalize(stream):
    centred = stream - jnp.mean(stream, axis=-1, keepdims=True)
    rstd = lax.rsqrt(jnp.mean(centred * centred, axis=-1, keepdims=True) + LN_EPS)
    return (centred * rstd, rstd)


def norm_back(normed, rstd, incoming):
    first = jnp.mean(incoming, axis=-1, keepdims=True)
    second = jnp.mean(incoming * normed, axis=-1, keepdims=True)
    return rstd * (incoming - first - normed * second)


def contract(left, right, left_dim, right_dim):
    return lax.dot_general(
        left, right, (((left_dim,), (right_dim,)), ((), ())), preferred_element_type=F32
    )


def softmax_rows(queries, key_rows, factor):
    scores = contract(queries, key_rows, 1, 1) * factor
    scores = jnp.exp(scores - jnp.max(scores, axis=-1, keepdims=True))
    return scores * (1.0 / jnp.sum(scores, axis=-1, keepdims=True))


def by_rows(body):
    @pl.loop(0, OWN // 32)
    def _(i):
        body(pl.ds(pl.multiple_of(i * 32, 32), 32))


def step_kernel(
    grad_scale, factor,
    tok, mod, wq, wo, wi, wb, og,
    final, grad, oq, oo, oi, ob,
    wa, wf, ga, gf, r1, r2, p1, p2, xbuf, part, partf, a1, a2, dm, da, packed, att, datt, act, slope, du,
    pa, pf, swap, own_sum, theirs, swapf, away, near, middle,
    gs, gr, ss, rs, xs, xr, ys, yr, es, er, csem,
):
    me = Place()
    mine_f = pl.multiple_of(me.xh * HALF, HALF)
    other_f = pl.multiple_of((1 - me.xh) * HALF, HALF)
    home_a, home_f = wa.at[me.z, me.y, me.xh], wf.at[me.z, me.y, me.xh]
    parts = [(wq.at[j], home_a.at[:, pl.ds(j * QKV, QKV)]) for j in range(3)] + [
        (wo, home_a.at[:, pl.ds(3 * QKV, QKV)]),
        (wi.at[:, pl.ds(mine_f, HALF)], home_f.at[:, LEFT]),
        (wb.at[:, pl.ds(mine_f, HALF)], home_f.at[:, RIGHT]),
    ]
    loads = [pltpu.make_async_copy(src, dst, csem.at[i]) for i, (src, dst) in enumerate(parts)]
    for load in loads:
        load.start()
    greet(torus_peers(me))
    for load in loads:
        load.wait()
    mine, other = me.xl, 1 - me.xl

    def m(i):
        return mod[i]

    sends = Sends()
    pieces = []
    for group, ref in enumerate((wa, wf)):
        for side in range(2):
            xb = me.xh if side == 0 else 1 - me.xh
            k = (group * 2 + side) * 2
            pieces.append([Gather(me, ref, h, 0, xb, gs.at[k + h], gr.at[k + h], sends) for h in range(2)])

    def gather_event(k, what, level):
        if what == "first" and level == 0 and k == 1:
            arrive(wa.at[me.z, me.y, 1 - me.xh], xr.at[0], me.across())
        if what == "first" and level == 0 and k == 3:
            for i, cols in ((1, LEFT), (2, RIGHT)):
                arrive(wf.at[me.z, me.y, 1 - me.xh, :, cols], xr.at[i], me.across())
        for half in pieces[k]:
            getattr(half, what)(level)

    def cross(group):
        if group == 0:
            sends.start(home_a, home_a, xs.at[0], xr.at[0], me.across())
        else:
            for i, ref, cols in ((1, wi, LEFT), (2, wb, RIGHT)):
                sends.start(ref.at[:, pl.ds(other_f, HALF)], home_f.at[:, cols], xs.at[i], xr.at[i], me.across())

    def ag(*steps):
        for step in steps:
            what = {"f": "first", "s": "second", "l": "last"}[step[0]]
            gather_event(int(step[2]), what, int(step[1]))

    scatters = []
    for n, ref in enumerate((gf, ga)):
        for side in range(2):
            xb = 1 - me.xh if side == 0 else me.xh
            k = n * 2 + side
            halves = []
            for h in range(2):
                bufs = ((r1.at[k, h], r2.at[k, h]), (p1.at[k, h], p2.at[k, h]))
                halves.append(Scatter(me, ref, h, xb, bufs, ss.at[k * 2 + h], rs.at[k * 2 + h], sends))
            scatters.append(halves)

    def finish(k, h):
        _, total = scatters[k][h].total(1)
        if k < 2:
            out = (oi, ob)[h]
            if k == 0:
                partf[h] = total
                sends.start(partf.at[h], out.at[:, pl.ds(mine_f, HALF)], ys.at[h], yr.at[h], me.across())
            else:
                out[:, pl.ds(mine_f, HALF)] = total
        elif k == 2:
            part[h] = pack(total)
            sends.start(part.at[h], xbuf.at[h], ys.at[2 + h], yr.at[2 + h], me.across())
        else:
            arrive(xbuf.at[h], yr.at[2 + h], me.across())
            total = total + wider(xbuf[h])
            outs = ((oq.at[0], oq.at[1]), (oq.at[2], oo))[h]
            for i, out in enumerate(outs):
                out[...] = total[:, i * QUART : (i + 1) * QUART]

    def rsc(*steps):
        names = {"f": ("far", 0), "r": ("relay", 0), "d": ("fold",), "g": ("far", 1), "s": ("relay", 1)}
        for step in steps:
            k = int(step[1])
            for h in (0, 1) if len(step) == 2 else (int(step[2]),):
                scatter_event(step, k, h, names)

    def scatter_event(step, k, h, names):
        if step[0] == "e":
            finish(k, h)
        else:
            name, *args = names[step[0]]
            getattr(scatters[k][h], name)(*args)

    def rows_of(ref, side, cols=slice(None)):
        value = ref[pl.ds(side * 2, 2), :, cols]
        return value.reshape(2 * OWN, value.shape[-1])

    def forward(src, side, w, col, width, emit):
        weight = w[:, :, :, :, pl.ds(col, width)].reshape(WIDTH, width)
        emit(contract(rows_of(src, side), weight, 1, 0).reshape(2, OWN, width))

    def backward(src, side, w, col, width, out):
        @pl.loop(0, 2)
        def _(j):
            weight = w[pl.ds(j * 2, 2), :, :, :, pl.ds(col, width)].reshape(HALF, width)
            at = pl.multiple_of(j * HALF, 128)
            value = contract(rows_of(src, side), weight, 1, 1)
            out[pl.ds(side * 2, 2), :, pl.ds(at, HALF)] = pack(value).reshape(2, OWN, HALF)

    def gradient(left, right, g, col, width):
        count = left.shape[0] * OWN

        @pl.loop(0, 4)
        def _(j):
            rows = left[:, :, pl.ds(pl.multiple_of(j * 384, 128), 384)].reshape(count, 384)
            value = contract(rows, right[...].reshape(count, width), 0, 0) * grad_scale
            g[j, :, :, :, pl.ds(col, width)] = pack(value).reshape(4, 2, ROWS, width)

    x_a1 = SeqGather(me, a1, es.at[0], er.at[0], sends)
    x_da = SeqGather(me, da, es.at[1], er.at[1], sends)
    x_a2 = RingGather(me, a2, es.at[2], er.at[2], sends)
    x_dm = RingGather(me, dm, es.at[3], er.at[3], sends)
    y_att = SeqScatter(me, pa, swap, own_sum, theirs, es.at[4], er.at[4])
    y_first = SeqScatter(me, pa, swap, own_sum, theirs, es.at[5], er.at[5])
    y_back = RingScatter(me, pf, swapf, away.at[0], near.at[0], es.at[6], er.at[6])
    y_ffn = RingScatter(me, pf, swapf, away.at[1], near.at[1], es.at[7], er.at[7])

    def share(y, src, col, width):
        backward(src, other, wa, col, width, y.part)
        y.give(0)
        backward(src, mine, wa, col, width, y.part)
        y.give(1)
        y.cross()

    def first_norm(r):
        n1, _ = normalize(wider(tok[r]))
        a1[me.s, r] = pack(n1 * (1.0 + m(1)) + m(0))

    def gate(r):
        dm[me.n, r] = pack(m(5) * wider(og[r]))

    def put(dst, side):
        def emit(value):
            dst[pl.ds(side * 2, 2)] = pack(value)
        return emit

    def head_cols(place, head):
        return pl.ds(pl.multiple_of(place * QKV + head * HEAD_DIM, HEAD_DIM), HEAD_DIM)

    def head_rows(ref, cols):
        return ref[:, :, cols].reshape(4 * OWN, HEAD_DIM)

    def attend(head):
        q, k, v = (head_rows(packed, head_cols(i, head)) for i in range(3))
        probs = softmax_rows(q, k, factor)
        att[:, :, head_cols(0, head)] = pack(contract(pack(probs), v, 1, 0)).reshape(4, OWN, HEAD_DIM)

    def attend_back(head):
        q, k, v = (head_rows(packed, head_cols(i, head)) for i in range(3))
        up = head_rows(datt, head_cols(0, head))
        probs = softmax_rows(q, k, factor)
        dprobs = contract(up, v, 1, 1)
        dscores = pack(probs * (dprobs - jnp.sum(probs * dprobs, axis=-1, keepdims=True)) * factor)
        parts = (contract(dscores, k, 1, 0), contract(dscores, q, 0, 0), contract(pack(probs), up, 0, 0))
        for i, value in enumerate(parts):
            packed[:, :, head_cols(i, head)] = pack(value).reshape(4, OWN, HEAD_DIM)

    def heads(body):
        pl.loop(0, HEADS)(body)

    def second_norm(r):
        mid = wider(tok[r]) + m(2) * y_att.rows(r)
        middle[r] = mid
        n2, _ = normalize(mid)
        a2[me.n, r] = pack(n2 * (1.0 + m(4)) + m(3))

    def hidden(chip):
        def emit(u):
            t = jnp.tanh(GELU_A * (u + GELU_B * (u * u * u)))
            at = pl.ds(chip * 2, 2)
            act[at] = pack(0.5 * u * (1.0 + t))
            slope[at] = 0.5 * (1.0 + t) + (0.5 * GELU_A) * u * (1.0 - t * t) * (1.0 + (3.0 * GELU_B) * (u * u))
        forward(a2, chip, wf, 0, HALF, emit)

    def hidden_back(step):
        chip = me.chip_at(step)

        def emit(dg):
            at = pl.ds(chip * 2, 2)
            du[at] = pack(slope[at] * dg)
        forward(dm, chip, wf, HALF, HALF, emit)

    def middle_back(r):
        n2, rstd = normalize(middle[r])
        up = wider(og[r]) + norm_back(n2, rstd, y_back.rows(r) * (1.0 + m(4)))
        grad[r] = up
        da[me.s, r] = pack(m(2) * up)

    def last_out(r):
        final[r] = pack(middle[r] + m(5) * y_ffn.rows(r))

    def first_back(r):
        n1, rstd = normalize(wider(tok[r]))
        grad[r] = grad[r] + norm_back(n1, rstd, y_first.rows(r) * (1.0 + m(1)))

    def sides(i):
        hidden(me.chip_at(2 * i - 1))

    cross(0)
    ag("f00", "f02")
    by_rows(first_norm)
    x_a1.start()
    cross(1)
    by_rows(gate)
    ag("s00", "f01", "l00", "f10", "s01", "s02")
    x_a1.relay()
    ag("l01", "f11", "s10", "l02", "f03", "s11", "f12", "s03")
    x_a1.near()
    x_a1.far()
    x_dm.start()
    ag("l10", "l03", "l11")
    forward(a1, mine, wa, 0, 3 * QKV, put(packed, mine))
    forward(a1, other, wa, 0, 3 * QKV, put(packed, other))
    ag("f13")
    heads(attend)
    share(y_att, att, 3 * QKV, QKV)
    ag("s12")
    x_dm.relay()
    ag("s13")
    x_dm.last()
    y_att.wait()
    by_rows(second_norm)
    y_att.sends.close()
    x_a2.start()
    x_dm.own()
    x_dm.sides()
    x_dm.far()
    ag("l12", "l13")
    x_a2.own()
    hidden(me.x)
    x_a2.relay()
    x_a2.sides()
    pl.loop(0, 2)(sides)
    x_a2.last()
    x_a2.far()
    hidden(me.chip_at(2))

    pl.loop(0, 4)(hidden_back)
    backward(du, me.chip_at(2), wf, 0, HALF, pf)
    y_back.give(0)
    backward(du, me.chip_at(1), wf, 0, HALF, pf)
    y_back.give(1)
    y_back.out()
    backward(du, me.chip_at(-1), wf, 0, HALF, pf)
    y_back.give(2)
    backward(du, me.chip_at(0), wf, 0, HALF, pf)
    y_back.give(3)
    gradient(dm, act, gf, HALF, HALF)
    rsc("f01", "f11")
    y_back.relay()
    gradient(a2, du, gf, 0, HALF)
    rsc("f00", "f10", "r01", "r11")
    rsc("r00", "r10")
    y_back.wait()
    by_rows(middle_back)
    y_back.sends.close()
    x_da.start()
    rsc("d01", "g01", "d11", "g11")
    backward(act, me.chip_at(2), wf, HALF, HALF, pf)
    backward(act, me.chip_at(1), wf, HALF, HALF, pf)
    rsc("d00", "g00", "d10", "g10", "s01", "s11")
    backward(act, me.chip_at(-1), wf, HALF, HALF, pf)
    backward(act, me.chip_at(0), wf, HALF, HALF, pf)
    x_da.relay()
    x_da.near()
    forward(da, mine, wa, 3 * QKV, QKV, put(datt, mine))
    y_ffn.give(0)
    y_ffn.give(1)
    y_ffn.give(2)
    y_ffn.give(3)
    x_da.far()
    forward(da, other, wa, 3 * QKV, QKV, put(datt, other))
    y_ffn.out()
    rsc("s00", "s10")
    heads(attend_back)
    gradient(a1, packed, ga, 0, 3 * QKV)
    rsc("f20", "f30")
    gradient(da, att, ga, 3 * QKV, QKV)
    rsc("f21", "f31")
    y_ffn.relay()
    rsc("r20", "r30")
    share(y_first, packed, 0, 3 * QKV)
    rsc("r21", "r31")
    rsc("e0", "e1")
    y_ffn.wait()
    by_rows(last_out)
    rsc("d2", "g2")
    y_first.wait()
    by_rows(first_back)
    rsc("d3", "g3", "s2", "s3", "e2", "e3")
    for h, out in enumerate((oi, ob)):
        arrive(out.at[:, pl.ds(other_f, HALF)], yr.at[h], me.across())
    sends.close()
    y_first.sends.close()
    y_ffn.sends.close()


def copy_kernel(*refs):
    n = len(refs) // 2
    sem = refs[-1]
    copies = [pltpu.make_async_copy(refs[i], refs[n + i], sem.at[i]) for i in range(n)]
    for copy in copies:
        copy.start()
    for copy in copies:
        copy.wait()


def copy_out(arrays):
    return pl.pallas_call(
        copy_kernel,
        out_shape=[jax.ShapeDtypeStruct(a.shape, a.dtype) for a in arrays],
        in_specs=[VM] * len(arrays),
        out_specs=[ANY] * len(arrays),
        scratch_shapes=[DMA((len(arrays),))],
    )(*arrays)


def local(tokens, modulation, w_qkv, w_out, w_in, w_back, out_grad):
    grad_scale = 1.0 / math.sqrt(OWN * lax.axis_size("sp") * lax.axis_size("fsdp"))
    factor = TEMPER / math.sqrt(HEAD_DIM)

    def shape(dims, dtype=BF16):
        return jax.ShapeDtypeStruct(dims, dtype)

    def vm(*dims, dtype=BF16):
        return pltpu.VMEM(dims, dtype)

    seq, ring = (4, OWN, WIDTH), (8, OWN, WIDTH)
    results = pl.pallas_call(
        functools.partial(step_kernel, grad_scale, factor),
        out_shape=(
            shape((OWN, WIDTH)), shape((OWN, WIDTH), F32), shape((3, ROWS, QKV), F32),
            shape((ROWS, QKV), F32), shape((ROWS, GROUP), F32), shape((ROWS, GROUP), F32),
        ),
        in_specs=[VM, VM, ANY, ANY, ANY, ANY, VM],
        out_specs=(VM,) * 6,
        scratch_shapes=[
            vm(4, 4, 2, ROWS, GROUP), vm(4, 4, 2, ROWS, GROUP), vm(4, 4, 2, ROWS, GROUP), vm(4, 4, 2, ROWS, GROUP),
            vm(4, 2, 2, 4, ROWS, QUART), vm(4, 2, 2, 4, ROWS, HALF),
            vm(4, 2, 2, ROWS, QUART), vm(4, 2, 2, ROWS, HALF),
            vm(2, ROWS, HALF), vm(2, ROWS, HALF), vm(2, ROWS, HALF, dtype=F32),
            vm(*seq), vm(*ring), vm(*ring), vm(*seq),
            vm(4, OWN, 3 * QKV), vm(4, OWN, QKV), vm(4, OWN, QKV),
            vm(8, OWN, HALF), vm(8, OWN, HALF, dtype=F32), vm(8, OWN, HALF),
            vm(*seq), vm(*ring), vm(2, OWN, WIDTH), vm(OWN, WIDTH), vm(OWN, WIDTH),
            vm(4, OWN, WIDTH), vm(2, 2, OWN, HALF), vm(2, 2, OWN, WIDTH), vm(OWN, WIDTH, dtype=F32),
            DMA((8, 8)), DMA((8, 8)), DMA((8, 8)), DMA((8, 8)),
            DMA((3,)), DMA((3,)), DMA((4,)), DMA((4,)), DMA((8, 9)), DMA((8, 9)), DMA((6,)),
        ],
        compiler_params=pltpu.CompilerParams(
            collective_id=0, has_side_effects=True, vmem_limit_bytes=67043328
        ),
    )(
        tokens[0], modulation.transpose(2, 0, 1, 3)[:, 0],
        w_qkv[0].transpose(1, 0, 2), w_out[0].T, w_in[0], w_back[0].T, out_grad[0],
    )
    final, grad, oq, oo, oi, ob = copy_out(results)
    return (
        final[None], grad[None], oq.transpose(1, 0, 2)[None], oo.T[None], oi[None], ob.T[None],
    )


def solution(mesh):
    weights = (
        P(None, "fsdp", None, "sp"),
        P(None, "sp", "fsdp"),
        P(None, "fsdp", "sp"),
        P(None, "sp", "fsdp"),
    )
    rows = P("fsdp", "sp", None)
    return jax.shard_map(
        local,
        mesh=mesh,
        in_specs=(rows, P("fsdp", None, None, None), *weights, rows),
        out_specs=(rows, rows, *weights),
        check_vma=False,
    )
```

```python
import functools
import math

import jax
import jax.numpy as jnp
from jax import lax
from jax.experimental import pallas as pl
from jax.experimental.pallas import tpu as pltpu
from jax.sharding import PartitionSpec as P

HEAD_DIM = 128
LN_EPS = 1e-06
TEMPER = 2.5
F32 = jnp.float32
BF16 = jnp.bfloat16
MESH = pl.DeviceIdType.MESH
GROUP = 1536
HALF = GROUP // 2
QUART = GROUP // 4
ROWS = 48


def rem(a, n):
    return lax.rem(a, n)


class Place:
    def __init__(self):
        f = lax.axis_index("fsdp")
        s = lax.axis_index("sp")
        self.z, self.y, self.xh = lax.div(f, 8), rem(lax.div(f, 2), 4), rem(f, 2)
        self.xl, self.c = lax.div(s, 2), rem(s, 2)
        self.s = s
        self.x = self.xh * 2 + self.xl
        self.n = self.x * 2 + self.c

    def dev(self, **kw):
        v = {k: kw.get(k, getattr(self, k)) for k in ("z", "y", "xh", "xl", "c")}
        return (v["z"] * 8 + v["y"] * 2 + v["xh"], v["xl"] * 2 + v["c"])

    def ring(self, axis, step):
        return rem(getattr(self, axis) + step + 4, 4)

    def near(self, axis, step):
        return self.dev(**{axis: self.ring(axis, step)})

    def along(self, step):
        x = rem(self.x + step + 4, 4)
        return self.dev(xh=lax.div(x, 2), xl=rem(x, 2))

    def chip_at(self, step):
        return rem(self.x + step + 4, 4)

    def across(self):
        return self.dev(xh=1 - self.xh)

    def chip(self):
        return self.dev(xl=1 - self.xl)

    def core(self):
        return self.dev(c=1 - self.c)


def greet(devices):
    barrier = pltpu.get_barrier_semaphore()
    for d in devices:
        pl.semaphore_signal(barrier, inc=1, device_id=d, device_id_type=MESH)
    pl.semaphore_wait(barrier, len(devices))


def torus_peers(me):
    return [me.near(a, s) for a in ("z", "y") for s in (1, -1)] + [me.across(), me.along(1), me.along(-1), me.core()]


class Sends:
    def __init__(self):
        self.open = []

    def start(self, src, dst, ssem, rsem, dev):
        copy = pltpu.make_async_remote_copy(
            src_ref=src, dst_ref=dst, send_sem=ssem, recv_sem=rsem, device_id=dev, device_id_type=MESH
        )
        copy.start()
        self.open.append(copy)

    def close(self):
        for copy in self.open:
            copy.wait_send()
        self.open = []


def arrive(ref, rsem, dev):
    pltpu.make_async_remote_copy(
        src_ref=ref, dst_ref=ref, send_sem=rsem, recv_sem=rsem, device_id=dev, device_id_type=MESH
    ).wait_recv()


def columns(start, low, high):
    return {"all": pl.ds(start, low + high), "lo": pl.ds(start, low), "hi": pl.ds(start + low, high)}


class Gather:
    def __init__(self, me, w, axes, span, xb, ssem, rsem, sends):
        self.me, self.w, self.axes, self.xb = me, w, axes, xb
        self.ssem, self.rsem, self.sends = ssem, rsem, sends
        self.cols = columns(*span)

    def part(self, p, q, which):
        first, second = self.axes
        at = {first: slice(None) if p is None else self.me.ring(first, p), second: self.me.ring(second, q)}
        return self.w.at[at["z"], at["y"], self.xb, :, self.cols[which]]

    def go(self, level, to, p, q, which, i):
        ref = self.part(p, q, which)
        self.sends.start(ref, ref, self.ssem.at[i], self.rsem.at[i], self.me.near(self.axes[level], to))

    def got(self, p, q, which, i):
        arrive(self.part(p, q, which), self.rsem.at[i], self.me.near(self.axes[0], 1))

    def first(self):
        self.go(0, 1, 0, 0, "all", 0)
        self.go(0, -1, 0, 0, "all", 1)

    def second(self):
        self.got(-1, 0, "all", 0)
        self.go(0, 1, -1, 0, "lo", 2)
        self.got(1, 0, "all", 1)
        self.go(0, -1, 1, 0, "hi", 3)

    def last(self):
        self.got(2, 0, "lo", 2)
        self.got(2, 0, "hi", 3)

    def out(self, *ps):
        for p in ps:
            i = 4 + (p + 1) * 2
            self.go(1, 1, p, 0, "all", i)
            self.go(1, -1, p, 0, "all", i + 1)

    def own(self):
        self.out(0)

    def sides(self):
        self.out(-1, 1)

    def end(self):
        self.out(2)

    def relay(self):
        for p in (0, -1, 1, 2):
            self.got(p, -1, "all", 4 + (p + 1) * 2)
        self.go(1, 1, None, -1, "lo", 12)
        for p in (0, -1, 1, 2):
            self.got(p, 1, "all", 5 + (p + 1) * 2)
        self.go(1, -1, None, 1, "hi", 13)

    def close(self):
        self.got(None, 2, "lo", 12)
        self.got(None, 2, "hi", 13)


def wider(ref_value):
    return ref_value.astype(F32)


def pack(total):
    return total.astype(BF16)


class Scatter:
    def __init__(self, me, g, axes, span, xb, bufs, ssem, rsem, sends):
        self.me, self.g, self.axes, self.xb = me, g, axes, xb
        self.bufs, self.ssem, self.rsem, self.sends = bufs, ssem, rsem, sends
        self.cols = columns(*span)
        self.inner = columns(0, *span[1:])

    def spot(self, level, step, which):
        axis = self.axes[level]
        at = {"z": self.me.z, "y": self.me.y}
        at[axis] = self.me.ring(axis, step)
        if level == 0:
            at[self.axes[1]] = slice(None)
        return (at["z"], at["y"], self.xb, slice(None), self.cols[which])

    def way(self, level, i, which):
        if level == 0:
            return self.bufs[0][0].at[i, :, :, columns(0, *self.sizes(which))["lo"]]
        return self.bufs[1][0].at[i, :, columns(0, *self.sizes(which))["lo"]]

    def sizes(self, which):
        return self.inner[which].size, 0

    def send(self, level, step, which, dst, i, to):
        i = level * 6 + i
        self.sends.start(
            self.g.at[self.spot(level, step, which)], dst, self.ssem.at[i], self.rsem.at[i],
            self.me.near(self.axes[level], to),
        )

    def near(self, level, i, which):
        cols = self.inner[which]
        if level == 0:
            return self.bufs[level][1].at[i, :, :, cols]
        return self.bufs[level][1].at[i, :, cols]

    def far(self, level):
        for to, which, i in ((1, "lo", 0), (-1, "hi", 1)):
            self.send(level, 2, which, self.way(level, i, which), i, to)

    def rest(self, level):
        for to, which, i in ((1, "hi", 0), (-1, "lo", 1)):
            self.send(level, to, which, self.near(level, i, which), 4 + i, to)

    def both(self, level):
        self.far(level)
        self.rest(level)

    def relay(self, level):
        for to, which, i in ((1, "lo", 0), (-1, "hi", 1)):
            buf = self.way(level, i, which)
            arrive(buf, self.rsem.at[level * 6 + i], self.me.near(self.axes[level], -to))
            spot = self.spot(level, to, which)
            self.g[spot] = (wider(self.g[spot]) + wider(buf[...])).astype(BF16)
        for to, which, i in ((1, "lo", 0), (-1, "hi", 1)):
            self.send(level, to, which, self.near(level, i, which), 2 + i, to)

    def total(self, level):
        near = self.bufs[level][1]
        for which, i, j in (("hi", 0, 4), ("lo", 1, 5), ("lo", 0, 2), ("hi", 1, 3)):
            arrive(self.near(level, i, which), self.rsem.at[level * 6 + j], self.me.near(self.axes[level], 1))
        spot = self.spot(level, 0, "all")
        return spot, wider(self.g[spot]) + wider(near[0]) + wider(near[1])

    def fold(self):
        spot, total = self.total(0)
        self.g[spot] = total.astype(BF16)


class FineScatter(Scatter):
    slots = {2: 0, 1: 1, -1: 2, 0: 3}
    lines = (0, 12, 18, 24)

    def place(self, q, p, which):
        at = {self.axes[0]: self.me.ring(self.axes[0], q), self.axes[1]: self.me.ring(self.axes[1], p)}
        return (at["z"], at["y"], self.xb, slice(None), self.cols[which])

    def give(self, q, p, which, dst, i, to):
        i = self.lines[self.slots[p]] + i
        self.sends.start(
            self.g.at[self.place(q, p, which)], dst, self.ssem.at[i], self.rsem.at[i], self.me.near(self.axes[0], to)
        )

    def take(self, dst, p, i):
        arrive(dst, self.rsem.at[self.lines[self.slots[p]] + i], self.me.near(self.axes[0], 1))

    def side(self, i, p, which):
        return self.bufs[0][1].at[i, self.slots[p], :, self.inner[which]]

    def step(self, i, p, which):
        return self.bufs[0][0].at[i, self.slots[p], :, pl.ds(0, self.inner[which].size)]

    def far0(self, *ps):
        for p in ps:
            for to, which, i in ((1, "lo", 0), (-1, "hi", 1)):
                self.give(2, p, which, self.step(i, p, which), i, to)

    def rest0(self, *ps):
        for p in ps:
            for to, which, i in ((1, "hi", 0), (-1, "lo", 1)):
                self.give(to, p, which, self.side(i, p, which), 4 + i, to)

    def relay0(self, *ps):
        for p in ps:
            for to, which, i in ((1, "lo", 0), (-1, "hi", 1)):
                buf = self.step(i, p, which)
                self.take(buf, p, i)
                spot = self.place(to, p, which)
                self.g[spot] = pack(wider(self.g[spot]) + wider(buf[...]))
            for to, which, i in ((1, "lo", 0), (-1, "hi", 1)):
                self.give(to, p, which, self.side(i, p, which), 2 + i, to)

    def fold0(self, *ps):
        for p in ps:
            for which, i, j in (("hi", 0, 4), ("lo", 1, 5), ("lo", 0, 2), ("hi", 1, 3)):
                self.take(self.side(i, p, which), p, j)
            spot = self.place(0, p, "all")
            near = self.bufs[0][1]
            total = wider(self.g[spot]) + wider(near[0, self.slots[p]]) + wider(near[1, self.slots[p]])
            self.g[spot] = pack(total)


DMA = pltpu.SemaphoreType.DMA
VM = pl.BlockSpec(memory_space=pltpu.VMEM)
ANY = pl.BlockSpec(memory_space=pl.ANY)
OWN = 128
WIDTH = 1536
HEADS = 3
QKV = HEADS * HEAD_DIM
GELU_A = math.sqrt(2.0 / math.pi)
GELU_B = 0.044715


CHUNKS = ((0, OWN // 2), (OWN // 2, OWN // 2))


class SeqGather:
    def __init__(self, me, buf, rows, ssem, rsem, sends):
        self.me, self.buf, self.rows, self.ssem, self.rsem, self.sends = me, buf, pl.ds(*rows), ssem, rsem, sends

    def push(self, block, i, dev):
        ref = self.buf.at[block, self.rows]
        self.sends.start(ref, ref, self.ssem.at[i], self.rsem.at[i], dev)

    def start(self):
        self.push(self.me.s, 0, self.me.chip())
        self.push(self.me.s, 1, self.me.core())

    def relay(self):
        other = (1 - self.me.xl) * 2 + self.me.c
        arrive(self.buf.at[other, self.rows], self.rsem.at[0], self.me.chip())
        self.push(other, 2, self.me.core())

    def near(self):
        arrive(self.buf.at[self.me.xl * 2 + 1 - self.me.c, self.rows], self.rsem.at[1], self.me.core())

    def far(self):
        arrive(self.buf.at[(1 - self.me.xl) * 2 + 1 - self.me.c, self.rows], self.rsem.at[2], self.me.core())


class SeqScatter:
    def __init__(self, me, part, swap, mine, theirs, ssem, rsem):
        self.me, self.part, self.swap, self.mine, self.theirs = me, part, swap, mine, theirs
        self.ssem, self.rsem, self.sends = ssem, rsem, Sends()

    def give(self, i):
        xl = self.me.xl if i else 1 - self.me.xl
        self.sends.start(
            self.part.at[xl * 2 + 1 - self.me.c], self.swap.at[i], self.ssem.at[i], self.rsem.at[i], self.me.core()
        )

    def cross(self):
        arrive(self.swap.at[0], self.rsem.at[0], self.me.core())

        def merge(r):
            self.mine[r] = pack(wider(self.part[(1 - self.me.xl) * 2 + self.me.c, r]) + wider(self.swap[0, r]))

        for i, rows in enumerate(CHUNKS):
            by_rows(merge, rows)
            r = pl.ds(*rows)
            self.sends.start(
                self.mine.at[r], self.theirs.at[r], self.ssem.at[2 + i], self.rsem.at[2 + i], self.me.chip()
            )

    def wait(self, i):
        if i == 0:
            arrive(self.swap.at[1], self.rsem.at[1], self.me.core())
        arrive(self.theirs.at[pl.ds(*CHUNKS[i])], self.rsem.at[2 + i], self.me.chip())

    def rows(self, r):
        return wider(self.part[self.me.s, r]) + wider(self.swap[1, r]) + wider(self.theirs[r])


LEFT, RIGHT = pl.ds(0, HALF), pl.ds(HALF, HALF)


class RingGather:
    def __init__(self, me, buf, rows, ssem, rsem, sends):
        self.me, self.buf, self.rows, self.ssem, self.rsem, self.sends = me, buf, pl.ds(*rows), ssem, rsem, sends

    def at(self, step, mine=True, cols=pl.ds(0, WIDTH)):
        return self.buf.at[self.me.chip_at(step) * 2 + (self.me.c if mine else 1 - self.me.c), self.rows, cols]

    def push(self, ref, i, dev):
        self.sends.start(ref, ref, self.ssem.at[i], self.rsem.at[i], dev)

    def start(self):
        for cols, step, i in ((LEFT, 1, 0), (RIGHT, -1, 1), (RIGHT, 1, 9), (LEFT, -1, 10)):
            self.push(self.at(0, cols=cols), i, self.me.along(step))
        self.push(self.at(0), 2, self.me.core())

    def relay(self):
        for step, cols, i in ((-1, LEFT, 0), (1, RIGHT, 1)):
            arrive(self.at(step, cols=cols), self.rsem.at[i], self.me.core())
            self.push(self.at(step, cols=cols), 3 + i, self.me.along(-step))

    def spread(self):
        for step, cols, i in ((-1, RIGHT, 0), (1, LEFT, 1)):
            arrive(self.at(step, cols=cols), self.rsem.at[9 + i], self.me.core())
            self.push(self.at(step), 5 + i, self.me.core())

    def last(self):
        for cols, i in ((LEFT, 0), (RIGHT, 1)):
            arrive(self.at(2, cols=cols), self.rsem.at[3 + i], self.me.core())
            self.push(self.at(2, cols=cols), 7 + i, self.me.core())

    def own(self):
        arrive(self.at(0, False), self.rsem.at[2], self.me.core())

    def sides(self):
        for step, i in ((-1, 5), (1, 6)):
            arrive(self.at(step, False), self.rsem.at[i], self.me.core())

    def far(self):
        for cols, i in ((LEFT, 7), (RIGHT, 8)):
            arrive(self.at(2, False, cols), self.rsem.at[i], self.me.core())


class RingScatter:
    order = (2, 1, -1, 0)

    def __init__(self, me, part, swap, away, near, rows, ssem, rsem):
        self.me, self.part, self.swap, self.away, self.near = me, part, swap, away, near
        self.span, self.ssem, self.rsem, self.sends = rows, ssem, rsem, Sends()
        self.r = pl.ds(*rows)

    def block(self, step):
        return self.me.chip_at(step) * 2 + self.me.c

    def give(self, j):
        src = self.part.at[self.me.chip_at(self.order[j]) * 2 + 1 - self.me.c]
        self.sends.start(src, self.swap.at[j], self.ssem.at[j], self.rsem.at[j], self.me.core())

    def swapped(self, j):
        if self.span[0] == 0:
            arrive(self.swap.at[j], self.rsem.at[j], self.me.core())

    def push(self, step, cols, dst, i, to):
        self.sends.start(
            self.part.at[self.block(step), self.r, cols], dst, self.ssem.at[i], self.rsem.at[i], self.me.along(to)
        )

    def out(self):
        self.swapped(0)
        block = self.block(2)

        def merge(r):
            self.part[block, r] = pack(wider(self.part[block, r]) + wider(self.swap[0, r]))

        by_rows(merge, self.span)
        self.push(2, LEFT, self.away.at[0, self.r], 4, 1)
        self.push(2, RIGHT, self.away.at[1, self.r], 5, -1)

    def rest(self):
        for step, j, i, cols in ((1, 1, 0, RIGHT), (-1, 2, 1, LEFT)):
            self.swapped(j)
            block = self.block(step)

            def merge(r):
                self.part[block, r, cols] = pack(wider(self.part[block, r, cols]) + wider(self.swap[j, r, cols]))

            by_rows(merge, self.span)
            self.push(step, cols, self.near.at[i, self.r, cols], 8 + i, step)

    def relay(self):
        for step, j, i, cols in ((1, 1, 0, LEFT), (-1, 2, 1, RIGHT)):
            arrive(self.away.at[i, self.r], self.rsem.at[4 + i], self.me.core())
            block = self.block(step)

            def merge(r):
                both = wider(self.part[block, r, cols]) + wider(self.swap[j, r, cols])
                self.part[block, r, cols] = pack(both + wider(self.away[i, r]))

            by_rows(merge, self.span)
            self.push(step, cols, self.near.at[i, self.r, cols], 6 + i, step)

    def wait(self):
        self.swapped(3)
        for i, cols, rest in ((0, LEFT, RIGHT), (1, RIGHT, LEFT)):
            arrive(self.near.at[i, self.r, rest], self.rsem.at[8 + i], self.me.core())
            arrive(self.near.at[i, self.r, cols], self.rsem.at[6 + i], self.me.core())

    def rows(self, r):
        own = wider(self.part[self.block(0), r]) + wider(self.swap[3, r])
        return own + (wider(self.near[0, r]) + wider(self.near[1, r]))


def normalize(stream):
    centred = stream - jnp.mean(stream, axis=-1, keepdims=True)
    rstd = lax.rsqrt(jnp.mean(centred * centred, axis=-1, keepdims=True) + LN_EPS)
    return (centred * rstd, rstd)


def norm_back(normed, rstd, incoming):
    first = jnp.mean(incoming, axis=-1, keepdims=True)
    second = jnp.mean(incoming * normed, axis=-1, keepdims=True)
    return rstd * (incoming - first - normed * second)


def contract(left, right, left_dim, right_dim):
    return lax.dot_general(
        left, right, (((left_dim,), (right_dim,)), ((), ())), preferred_element_type=F32
    )


def softmax_rows(queries, key_rows, factor):
    scores = contract(queries, key_rows, 1, 1) * factor
    scores = jnp.exp(scores - jnp.max(scores, axis=-1, keepdims=True))
    return scores * (1.0 / jnp.sum(scores, axis=-1, keepdims=True))


def by_rows(body, rows=(0, OWN)):
    @pl.loop(rows[0] // 32, (rows[0] + rows[1]) // 32)
    def _(i):
        body(pl.ds(pl.multiple_of(i * 32, 32), 32))


def step_kernel(
    grad_scale, factor,
    tok, mod, wq, wo, wi, wb, og,
    final, grad, oq, oo, oi, ob,
    wa, wf, ga, gf, r1, r2, p1, p2, r3, r4, p3, p4, xbuf, part, partf, xf, a1, a2, dm, da, packed, att, datt, act, dg, du,
    pf, swap, own_sum, theirs, swapf, away, near, middle,
    gs, gr, ss, rs, xs, xr, ys, yr, es, er, csem,
):
    me = Place()
    mine_f = pl.multiple_of(me.xh * HALF, HALF)
    other_f = pl.multiple_of((1 - me.xh) * HALF, HALF)
    home_a, home_f = wa.at[me.z, me.y, me.xh], wf.at[me.z, me.y, me.xh]
    parts = [
        (wq.at[j, :, pl.ds(h * HEAD_DIM, HEAD_DIM)], home_a.at[:, pl.ds(h * QKV + j * HEAD_DIM, HEAD_DIM)])
        for h in range(HEADS) for j in range(3)
    ] + [
        (wo, home_a.at[:, pl.ds(3 * QKV, QKV)]),
        (wi.at[:, pl.ds(mine_f, HALF)], home_f.at[:, LEFT]),
        (wb.at[:, pl.ds(mine_f, HALF)], home_f.at[:, RIGHT]),
    ]
    loads = [pltpu.make_async_copy(src, dst, csem.at[i]) for i, (src, dst) in enumerate(parts)]
    for load in loads:
        load.start()
    greet(torus_peers(me))
    for load in loads:
        load.wait()
    mine, other = me.xl, 1 - me.xl

    def m(i):
        return mod[i]

    sends = Sends()
    yz, zy = ("y", "z"), ("z", "y")
    plan = [
        (wa, 0, [(yz, (0, 384, 256)), (zy, (640, 256, 256))]), (wa, 1, [(zy, (0, 384, 256)), (yz, (640, 256, 256))]),
        (wa, 0, [(yz, (1152, 256, 128))]), (wa, 1, [(zy, (1152, 256, 128))]),
        (wf, 0, [(yz, (0, 384, 384)), (zy, (768, 384, 384))]), (wf, 1, [(yz, (0, 384, 384)), (zy, (768, 384, 384))]),
    ]
    pieces = []
    count = 0
    for ref, side, halves in plan:
        pieces.append([])
        for axes, span in halves:
            xb = 1 - me.xh if side else me.xh
            pieces[-1].append(Gather(me, ref, axes, span, xb, gs.at[count], gr.at[count], sends))
            count += 1

    def gather_event(k, what):
        if what == "first" and k % 2:
            for i, ref, cols in crossed[k]:
                arrive(ref.at[me.z, me.y, 1 - me.xh, :, cols], xr.at[i], me.across())
        for half in pieces[k]:
            getattr(half, what)()

    crossed = {1: [(0, wa, pl.ds(0, 3 * QKV))], 3: [(1, wa, pl.ds(3 * QKV, QKV))], 5: [(2, wf, LEFT), (3, wf, RIGHT)]}

    def cross(group):
        if group < 2:
            ref = home_a.at[:, crossed[2 * group + 1][0][2]]
            sends.start(ref, ref, xs.at[group], xr.at[group], me.across())
        else:
            for i, ref, cols in ((2, wi, LEFT), (3, wb, RIGHT)):
                sends.start(ref.at[:, pl.ds(other_f, HALF)], home_f.at[:, cols], xs.at[i], xr.at[i], me.across())

    def ag(*steps):
        names = {
            "f": "first", "s": "second", "l": "last", "o": "own", "i": "sides", "e": "end", "r": "relay", "c": "close"
        }
        for step in steps:
            gather_event(int(step[1]), names[step[0]])

    scatters = []
    for k in range(10):
        side = k % 2
        xb = me.xh if side else 1 - me.xh
        if k < 4:
            span, axes = ((HALF, 384, 384), (0, 384, 384))[k // 2], (yz, zy, zy, yz)[k]
        else:
            span, axes = ((3 * QKV, 256, 128), (0, 384, 384), (2 * QKV, 256, 128))[k // 2 - 2], (zy, yz, zy, yz, yz, zy)[k - 4]
        kind = Scatter if k < 4 else FineScatter
        if span[1] == 384:
            n = k if k < 4 else k - 2
            bufs = ((r1.at[n], r2.at[n]), (p1.at[n], p2.at[n]))
        else:
            n = k - 4 if k < 6 else k - 6
            bufs = ((r3.at[n], r4.at[n]), (p3.at[n], p4.at[n]))
        scatters.append(kind(me, gf if k < 4 else ga, axes, span, xb, bufs, ss.at[k], rs.at[k], sends))

    def finish(k):
        scatter = scatters[k]
        _, total = scatter.total(1)
        cols = scatter.cols["all"]
        group = k // 2
        if k < 4:
            out = (ob, oi)[group].at[:, pl.ds(mine_f, HALF)]
            if k % 2:
                out[...] = total
            else:
                partf[group] = pack(total)
                sends.start(partf.at[group], xf.at[group], ys.at[group], yr.at[group], me.across())
        elif k % 2 == 0:
            part[:, cols] = pack(total)
            sends.start(part.at[:, cols], xbuf.at[:, cols], ys.at[group], yr.at[group], me.across())
        else:
            arrive(xbuf.at[:, cols], yr.at[group], me.across())
            total = total + wider(xbuf[:, cols])
            for i in range(cols.size // QKV):
                value = total[:, i * QKV : (i + 1) * QKV]
                head = cols.start // QKV + i
                if head == HEADS:
                    oo[...] = value
                else:
                    for j in range(3):
                        oq[j, :, pl.ds(head * HEAD_DIM, HEAD_DIM)] = value[:, j * HEAD_DIM : (j + 1) * HEAD_DIM]

    def rsc(*steps):
        names = {
            "f": ("both", 0), "r": ("relay", 0), "d": ("fold",), "g": ("both", 1), "s": ("relay", 1),
            "F": ("far0",), "N": ("rest0",), "R": ("relay0",), "D": ("fold0",), "G": ("far", 1), "H": ("rest", 1),
        }
        spots = {"": (2, 1, -1, 0), "a": (2,), "b": (1, -1), "c": (0,), "ab": (2, 1, -1), "bc": (1, -1, 0)}
        for step in steps:
            scatter_event(step, int(step[1]), names, spots)

    def scatter_event(step, k, names, spots):
        if step[0] == "e":
            finish(k)
        else:
            name, *args = names[step[0]]
            if step[0] in "FNRD":
                args = spots[step[2:]]
            getattr(scatters[k], name)(*args)

    def rows_of(ref, side, cols=slice(None)):
        value = ref[pl.ds(side * 2, 2), :, cols]
        return value.reshape(2 * OWN, value.shape[-1])

    def forward(src, side, w, col, width, emit):
        weight = w[:, :, :, :, pl.ds(col, width)].reshape(WIDTH, width)
        emit(contract(rows_of(src, side), weight, 1, 0).reshape(2, OWN, width))

    def backward(src, side, w, col, width, out):
        @pl.loop(0, 2)
        def _(j):
            weight = w[pl.ds(j * 2, 2), :, :, :, pl.ds(col, width)].reshape(HALF, width)
            at = pl.multiple_of(j * HALF, 128)
            value = contract(rows_of(src, side), weight, 1, 1)
            out[pl.ds(side * 2, 2), :, pl.ds(at, HALF)] = pack(value).reshape(2, OWN, HALF)

    def gradient(left, right, g, col, width):
        count = left.shape[0] * OWN

        @pl.loop(0, 4)
        def _(j):
            rows = left[:, :, pl.ds(pl.multiple_of(j * 384, 128), 384)].reshape(count, 384)
            value = contract(rows, right[...].reshape(count, width), 0, 0) * grad_scale
            g[j, :, :, :, pl.ds(col, width)] = pack(value).reshape(4, 2, ROWS, width)

    every = (0, OWN)
    x_a1 = SeqGather(me, a1, every, es.at[0], er.at[0], sends)
    x_das = [SeqGather(me, da, rows, es.at[1 + i], er.at[1 + i], sends) for i, rows in enumerate(CHUNKS)]
    a2_sends = Sends()
    x_a2s = [RingGather(me, a2, rows, es.at[3 + i], er.at[3 + i], a2_sends) for i, rows in enumerate(CHUNKS)]
    x_dm = RingGather(me, dm, every, es.at[5], er.at[5], sends)
    y_att = SeqScatter(me, pf.at[pl.ds(0, 4)], swap, own_sum, theirs, es.at[6], er.at[6])
    y_first = SeqScatter(me, a2.at[pl.ds(0, 4)], swap, own_sum, theirs, es.at[7], er.at[7])
    y_backs = [
        RingScatter(me, pf, swapf.at[0], away.at[0], near.at[0], rows, es.at[8 + i], er.at[8 + i])
        for i, rows in enumerate(CHUNKS)
    ]
    y_back = y_backs[0]
    y_ffn = RingScatter(me, pf, swapf.at[1], away.at[1], near.at[1], every, es.at[10], er.at[10])

    def all_of(objects, *names):
        for name in names:
            for item in objects:
                getattr(item, name)()

    def share(y, src, col, width):
        backward(src, other, wa, col, width, y.part)
        y.give(0)
        backward(src, mine, wa, col, width, y.part)
        y.give(1)
        y.cross()

    def first_norm(r):
        n1, _ = normalize(wider(tok[r]))
        a1[me.s, r] = pack(n1 * (1.0 + m(1)) + m(0))

    def gate(r):
        dm[me.n, r] = pack(m(5) * wider(og[r]))

    def put(dst, side):
        def emit(value):
            dst[pl.ds(side * 2, 2)] = pack(value)
        return emit

    def head_cols(place, head):
        return pl.ds(pl.multiple_of(head * QKV + place * HEAD_DIM, HEAD_DIM), HEAD_DIM)

    def own_cols(head):
        return pl.ds(pl.multiple_of(head * HEAD_DIM, HEAD_DIM), HEAD_DIM)

    def head_rows(ref, cols):
        return ref[:, :, cols].reshape(4 * OWN, HEAD_DIM)

    def attend(head):
        q, k, v = (head_rows(packed, head_cols(i, head)) for i in range(3))
        probs = softmax_rows(q, k, factor)
        att[:, :, own_cols(head)] = pack(contract(pack(probs), v, 1, 0)).reshape(4, OWN, HEAD_DIM)

    def attend_back(head):
        q, k, v = (head_rows(packed, head_cols(i, head)) for i in range(3))
        up = head_rows(datt, own_cols(head))
        probs = softmax_rows(q, k, factor)
        dprobs = contract(up, v, 1, 1)
        dscores = pack(probs * (dprobs - jnp.sum(probs * dprobs, axis=-1, keepdims=True)) * factor)
        parts = (contract(dscores, k, 1, 0), contract(dscores, q, 0, 0), contract(pack(probs), up, 0, 0))
        for i, value in enumerate(parts):
            packed[:, :, head_cols(i, head)] = pack(value).reshape(4, OWN, HEAD_DIM)

    def heads(body, low=0, high=HEADS):
        pl.loop(low, high)(body)

    def second_norm(r):
        mid = wider(tok[r]) + m(2) * y_att.rows(r)
        middle[r] = mid
        n2, _ = normalize(mid)
        a2[me.n, r] = pack(n2 * (1.0 + m(4)) + m(3))

    def hidden(chip):
        def emit(u):
            t = jnp.tanh(GELU_A * (u + GELU_B * (u * u * u)))
            at = pl.ds(chip * 2, 2)
            act[at] = pack(0.5 * u * (1.0 + t))
            slope = 0.5 * (1.0 + t) + (0.5 * GELU_A) * u * (1.0 - t * t) * (1.0 + (3.0 * GELU_B) * (u * u))
            du[at] = pack(slope * dg[at])
        forward(a2, chip, wf, 0, HALF, emit)

    def hidden_back(chip):
        def emit(value):
            dg[pl.ds(chip * 2, 2)] = value
        forward(dm, chip, wf, HALF, HALF, emit)

    def middle_back(r):
        n2, rstd = normalize(middle[r])
        up = wider(og[r]) + norm_back(n2, rstd, y_back.rows(r) * (1.0 + m(4)))
        grad[r] = up
        da[me.s, r] = pack(m(2) * up)

    def last_out(r):
        final[r] = pack(middle[r] + m(5) * y_ffn.rows(r))

    def first_back(r):
        n1, rstd = normalize(wider(tok[r]))
        grad[r] = grad[r] + norm_back(n1, rstd, y_first.rows(r) * (1.0 + m(1)))

    def sides(i):
        hidden(me.chip_at(2 * i - 1))

    def backs(i):
        hidden_back(me.chip_at(i))

    def norm_and_send(i):
        y_att.wait(i)
        by_rows(second_norm, CHUNKS[i])
        x_a2s[i].start()

    def back_and_send(i):
        y_backs[i].wait()
        by_rows(middle_back, CHUNKS[i])
        x_das[i].start()

    def norm_and_send(i):
        y_att.wait(i)
        by_rows(second_norm, CHUNKS[i])
        x_a2s[i].start()

    def back_and_send(i):
        y_backs[i].wait()
        by_rows(middle_back, CHUNKS[i])
        x_das[i].start()

    cross(0)
    ag("f0", "o0", "f4", "o4")
    by_rows(first_norm)
    x_a1.start()
    cross(1)
    cross(2)
    by_rows(gate)
    x_dm.start()
    ag("s0", "i0", "f1", "o1", "l0", "e0", "f2", "s1", "i1", "l1", "e1", "r0", "s2", "f3")
    x_a1.relay()
    ag("o2", "i2", "l2", "r1", "e2", "o3", "s3", "i3")
    x_dm.relay()
    ag("l3", "e3", "c0")
    x_a1.near()
    x_a1.far()
    ag("c1")
    forward(a1, mine, wa, 0, 3 * QKV, put(packed, mine))
    forward(a1, other, wa, 0, 3 * QKV, put(packed, other))
    ag("s4", "r2")
    heads(attend, 0, 1)
    ag("r3", "i4", "f5")
    heads(attend, 1, 3)
    ag("c2", "c3")
    share(y_att, att, 3 * QKV, QKV)
    x_dm.spread()
    ag("l4", "e4", "s5", "o5", "i5", "l5", "e5")
    x_dm.last()
    x_dm.own()
    x_dm.sides()
    x_dm.far()
    ag("r4")
    norm_and_send(0)
    norm_and_send(1)
    ag("r5")
    x_a2s[0].relay()
    y_att.sends.close()
    all_of(x_a2s, "own")
    ag("c4", "c5")
    pl.loop(0, 2)(backs)
    x_a2s[1].relay()
    hidden(me.x)
    pl.loop(2, 4)(backs)
    all_of(x_a2s, "spread", "sides")
    pl.loop(0, 2)(sides)
    all_of(x_a2s, "last")

    backward(du, me.chip_at(1), wf, 0, HALF, pf)
    y_back.give(1)
    all_of(x_a2s, "far")
    hidden(me.chip_at(2))
    backward(du, me.chip_at(2), wf, 0, HALF, pf)
    y_back.give(0)
    backward(du, me.chip_at(-1), wf, 0, HALF, pf)
    y_back.give(2)
    all_of(y_backs, "out")
    backward(du, me.chip_at(0), wf, 0, HALF, pf)
    y_back.give(3)
    all_of(y_backs, "rest")
    gradient(dm, act, gf, HALF, HALF)
    rsc("f0", "f1")
    all_of(y_backs, "relay")
    gradient(a2, du, gf, 0, HALF)
    rsc("r0", "r1", "f2", "f3")
    back_and_send(0)
    back_and_send(1)
    y_backs[0].sends.close()
    y_backs[1].sends.close()
    a2_sends.close()
    backward(act, me.chip_at(2), wf, HALF, HALF, pf)
    y_ffn.give(0)
    backward(act, me.chip_at(1), wf, HALF, HALF, pf)
    y_ffn.give(1)
    rsc("d0", "g0", "d1", "g1")
    x_das[0].relay()
    backward(act, me.chip_at(-1), wf, HALF, HALF, pf)
    y_ffn.give(2)
    rsc("r2", "r3")
    backward(act, me.chip_at(0), wf, HALF, HALF, pf)
    y_ffn.give(3)
    x_das[1].relay()
    all_of(x_das, "near")
    forward(da, mine, wa, 3 * QKV, QKV, put(datt, mine))
    all_of(x_das, "far")
    forward(da, other, wa, 3 * QKV, QKV, put(datt, other))
    y_ffn.out()
    gradient(da, att, ga, 3 * QKV, QKV)
    rsc("F4", "F5", "N4", "N5")
    heads(attend_back, 0, 2)
    y_ffn.rest()
    rsc("d2", "g2", "d3", "g3", "s0", "s1")
    gradient(a1, packed.at[:, :, pl.ds(0, HALF)], ga, 0, HALF)
    rsc("F6", "F7", "N6", "N7", "R4", "R5")
    heads(attend_back, 2, 3)
    gradient(a1, packed.at[:, :, pl.ds(HALF, QKV)], ga, HALF, QKV)
    rsc("F8", "F9", "N8", "N9", "s2", "s3", "R6a", "R7a", "R6b", "R7b", "R6c", "R7c", "e0")
    y_ffn.relay()
    share(y_first, packed, 0, 3 * QKV)
    rsc("R8a", "R9a", "R8b", "R9b", "R8c", "R9c", "e2", "D4", "G4", "H4", "D5", "G5", "H5")
    rsc("D6a", "G6", "D7a", "G7", "D6b", "H6", "D7b", "H7", "D6c", "D7c")
    rsc("D8a", "G8", "D9a", "G9", "D8b", "H8", "D9b", "H9", "D8c", "D9c", "s4", "s5", "s6", "s7", "s8", "s9")
    rsc("e4", "e6", "e8")
    y_ffn.wait()
    by_rows(last_out)
    y_first.wait(0)
    y_first.wait(1)
    by_rows(first_back)
    rsc("e1", "e3")
    for group, out in enumerate((ob, oi)):
        arrive(xf.at[group], yr.at[group], me.across())
        out[:, pl.ds(other_f, HALF)] = wider(xf[group])
    rsc("e5", "e7", "e9")
    sends.close()
    y_first.sends.close()
    y_ffn.sends.close()


def copy_kernel(*refs):
    n = len(refs) // 2
    sem = refs[-1]
    copies = [pltpu.make_async_copy(refs[i], refs[n + i], sem.at[i]) for i in range(n)]
    for copy in copies:
        copy.start()
    for copy in copies:
        copy.wait()


def copy_out(arrays):
    return pl.pallas_call(
        copy_kernel,
        out_shape=[jax.ShapeDtypeStruct(a.shape, a.dtype) for a in arrays],
        in_specs=[VM] * len(arrays),
        out_specs=[ANY] * len(arrays),
        scratch_shapes=[DMA((len(arrays),))],
    )(*arrays)


def local(tokens, modulation, w_qkv, w_out, w_in, w_back, out_grad):
    grad_scale = 1.0 / math.sqrt(OWN * lax.axis_size("sp") * lax.axis_size("fsdp"))
    factor = TEMPER / math.sqrt(HEAD_DIM)

    def shape(dims, dtype=BF16):
        return jax.ShapeDtypeStruct(dims, dtype)

    def vm(*dims, dtype=BF16):
        return pltpu.VMEM(dims, dtype)

    seq, ring = (4, OWN, WIDTH), (8, OWN, WIDTH)
    results = pl.pallas_call(
        functools.partial(step_kernel, grad_scale, factor),
        out_shape=(
            shape((OWN, WIDTH)), shape((OWN, WIDTH), F32), shape((3, ROWS, QKV), F32),
            shape((ROWS, QKV), F32), shape((ROWS, GROUP), F32), shape((ROWS, GROUP), F32),
        ),
        in_specs=[VM, VM, ANY, ANY, ANY, ANY, VM],
        out_specs=(VM,) * 6,
        scratch_shapes=[
            vm(4, 4, 2, ROWS, GROUP), vm(4, 4, 2, ROWS, GROUP), vm(4, 4, 2, ROWS, GROUP), vm(4, 4, 2, ROWS, GROUP),
            vm(6, 2, 4, ROWS, QUART), vm(6, 2, 4, ROWS, HALF), vm(6, 2, ROWS, QUART), vm(6, 2, ROWS, HALF),
            vm(4, 2, 4, ROWS, 256), vm(4, 2, 4, ROWS, 384), vm(4, 2, ROWS, 256), vm(4, 2, ROWS, 384),
            vm(ROWS, GROUP), vm(ROWS, GROUP), vm(2, ROWS, HALF), vm(2, ROWS, HALF),
            vm(*seq), vm(*ring), vm(*ring), vm(*seq),
            vm(4, OWN, 3 * QKV), vm(4, OWN, QKV), vm(4, OWN, QKV),
            vm(8, OWN, HALF), vm(8, OWN, HALF, dtype=F32), vm(8, OWN, HALF),
            vm(*ring), vm(2, OWN, WIDTH), vm(OWN, WIDTH), vm(OWN, WIDTH),
            vm(2, 4, OWN, WIDTH), vm(2, 2, OWN, HALF), vm(2, 2, OWN, WIDTH), vm(OWN, WIDTH, dtype=F32),
            DMA((10, 14)), DMA((10, 14)), DMA((10, 30)), DMA((10, 30)),
            DMA((4,)), DMA((4,)), DMA((5,)), DMA((5,)), DMA((11, 11)), DMA((11, 11)), DMA((12,)),
        ],
        compiler_params=pltpu.CompilerParams(
            collective_id=0, has_side_effects=True, vmem_limit_bytes=67043328
        ),
    )(
        tokens[0], modulation.transpose(2, 0, 1, 3)[:, 0],
        w_qkv[0].transpose(1, 0, 2), w_out[0].T, w_in[0], w_back[0].T, out_grad[0],
    )
    final, grad, oq, oo, oi, ob = copy_out(results)
    return (
        final[None], grad[None], oq.transpose(1, 0, 2)[None], oo.T[None], oi[None], ob.T[None],
    )


def solution(mesh):
    weights = (
        P(None, "fsdp", None, "sp"),
        P(None, "sp", "fsdp"),
        P(None, "fsdp", "sp"),
        P(None, "sp", "fsdp"),
    )
    rows = P("fsdp", "sp", None)
    return jax.shard_map(
        local,
        mesh=mesh,
        in_specs=(rows, P("fsdp", None, None, None), *weights, rows),
        out_specs=(rows, rows, *weights),
        check_vma=False,
    )
```

```python
import functools
import math

import jax
import jax.numpy as jnp
from jax import lax
from jax.experimental import pallas as pl
from jax.experimental.pallas import tpu as pltpu
from jax.sharding import PartitionSpec as P

HEAD_DIM = 128
LN_EPS = 1e-06
TEMPER = 2.5
F32 = jnp.float32
BF16 = jnp.bfloat16
MESH = pl.DeviceIdType.MESH
GROUP = 1536
HALF = GROUP // 2
QUART = GROUP // 4
ROWS = 48


def rem(a, n):
    return lax.rem(a, n)


class Place:
    def __init__(self):
        f = lax.axis_index("fsdp")
        s = lax.axis_index("sp")
        self.z, self.y, self.xh = lax.div(f, 8), rem(lax.div(f, 2), 4), rem(f, 2)
        self.xl, self.c = lax.div(s, 2), rem(s, 2)
        self.s = s
        self.x = self.xh * 2 + self.xl
        self.n = self.x * 2 + self.c

    def dev(self, **kw):
        v = {k: kw.get(k, getattr(self, k)) for k in ("z", "y", "xh", "xl", "c")}
        return (v["z"] * 8 + v["y"] * 2 + v["xh"], v["xl"] * 2 + v["c"])

    def ring(self, axis, step):
        return rem(getattr(self, axis) + step + 4, 4)

    def near(self, axis, step):
        return self.dev(**{axis: self.ring(axis, step)})

    def along(self, step):
        x = rem(self.x + step + 4, 4)
        return self.dev(xh=lax.div(x, 2), xl=rem(x, 2))

    def chip_at(self, step):
        return rem(self.x + step + 4, 4)

    def across(self):
        return self.dev(xh=1 - self.xh)

    def chip(self):
        return self.dev(xl=1 - self.xl)

    def core(self):
        return self.dev(c=1 - self.c)


def greet(devices):
    barrier = pltpu.get_barrier_semaphore()
    for d in devices:
        pl.semaphore_signal(barrier, inc=1, device_id=d, device_id_type=MESH)
    pl.semaphore_wait(barrier, len(devices))


def torus_peers(me):
    return [me.near(a, s) for a in ("z", "y") for s in (1, -1)] + [me.across(), me.along(1), me.along(-1), me.core()]


class Sends:
    def __init__(self):
        self.open = []

    def start(self, src, dst, ssem, rsem, dev):
        copy = pltpu.make_async_remote_copy(
            src_ref=src, dst_ref=dst, send_sem=ssem, recv_sem=rsem, device_id=dev, device_id_type=MESH
        )
        copy.start()
        self.open.append(copy)

    def close(self):
        for copy in self.open:
            copy.wait_send()
        self.open = []


def launch(src, dst, ssem, rsem, dev):
    pltpu.make_async_remote_copy(
        src_ref=src, dst_ref=dst, send_sem=ssem, recv_sem=rsem, device_id=dev, device_id_type=MESH
    ).start()


def drained(ref, ssem, dev):
    pltpu.make_async_remote_copy(
        src_ref=ref, dst_ref=ref, send_sem=ssem, recv_sem=ssem, device_id=dev, device_id_type=MESH
    ).wait_send()


def arrive(ref, rsem, dev):
    pltpu.make_async_remote_copy(
        src_ref=ref, dst_ref=ref, send_sem=rsem, recv_sem=rsem, device_id=dev, device_id_type=MESH
    ).wait_recv()


def columns(start, low, high):
    return {"all": pl.ds(start, low + high), "lo": pl.ds(start, low), "hi": pl.ds(start + low, high)}


class Gather:
    def __init__(self, me, w, axes, span, xb, ssem, rsem, sends):
        self.me, self.w, self.axes, self.xb = me, w, axes, xb
        self.ssem, self.rsem, self.sends = ssem, rsem, sends
        self.cols = columns(*span)

    def part(self, p, q, which):
        first, second = self.axes
        at = {first: slice(None) if p is None else self.me.ring(first, p), second: self.me.ring(second, q)}
        return self.w.at[at["z"], at["y"], self.xb, :, self.cols[which]]

    def go(self, level, to, p, q, which, i):
        ref = self.part(p, q, which)
        launch(ref, ref, self.ssem.at[level], self.rsem.at[i], self.me.near(self.axes[level], to))

    def got(self, p, q, which, i):
        arrive(self.part(p, q, which), self.rsem.at[i], self.me.near(self.axes[0], 1))

    def first(self):
        self.go(0, 1, 0, 0, "all", 0)
        self.go(0, -1, 0, 0, "all", 1)

    def second(self):
        self.got(-1, 0, "all", 0)
        self.go(0, 1, -1, 0, "lo", 2)
        self.got(1, 0, "all", 1)
        self.go(0, -1, 1, 0, "hi", 2)

    def last(self):
        self.got(2, 0, "all", 2)

    def out(self, *ps):
        for p in ps:
            self.go(1, 1, p, 0, "all", 3)
            self.go(1, -1, p, 0, "all", 4)

    def own(self):
        self.out(0)

    def sides(self):
        self.out(-1, 1)

    def end(self):
        self.out(2)

    def relay(self):
        self.got(None, -1, "all", 3)
        self.go(1, 1, None, -1, "lo", 5)
        self.got(None, 1, "all", 4)
        self.go(1, -1, None, 1, "hi", 5)

    def close(self):
        self.got(None, 2, "all", 5)

    def drain(self):
        cols = self.cols["all"]
        drained(self.w.at[0, pl.ds(0, 3), 0, :, cols], self.ssem.at[0], self.me.near("z", 1))
        drained(self.w.at[pl.ds(0, 3), pl.ds(0, 4), 0, :, cols], self.ssem.at[1], self.me.near("z", 1))


def wider(ref_value):
    return ref_value.astype(F32)


def pack(total):
    return total.astype(BF16)


class Scatter:
    def __init__(self, me, g, axes, span, xb, bufs, ssem, rsem, sends):
        self.me, self.g, self.axes, self.xb = me, g, axes, xb
        self.bufs, self.ssem, self.rsem, self.sends = bufs, ssem, rsem, sends
        self.cols = columns(*span)
        self.inner = columns(0, *span[1:])

    def spot(self, level, step, which):
        axis = self.axes[level]
        at = {"z": self.me.z, "y": self.me.y}
        at[axis] = self.me.ring(axis, step)
        if level == 0:
            at[self.axes[1]] = slice(None)
        return (at["z"], at["y"], self.xb, slice(None), self.cols[which])

    def way(self, level, i, which):
        if level == 0:
            return self.bufs[0][0].at[i, :, :, columns(0, *self.sizes(which))["lo"]]
        return self.bufs[1][0].at[i, :, columns(0, *self.sizes(which))["lo"]]

    def sizes(self, which):
        return self.inner[which].size, 0

    def send(self, level, step, which, dst, i, to):
        launch(
            self.g.at[self.spot(level, step, which)], dst, self.ssem.at[level], self.rsem.at[level * 2 + i],
            self.me.near(self.axes[level], to),
        )

    def near(self, level, i, which):
        cols = self.inner[which]
        if level == 0:
            return self.bufs[level][1].at[i, :, :, cols]
        return self.bufs[level][1].at[i, :, cols]

    def far(self, level):
        for to, which, i in ((1, "lo", 0), (-1, "hi", 1)):
            self.send(level, 2, which, self.way(level, i, which), 0, to)

    def rest(self, level):
        for to, which, i in ((1, "hi", 0), (-1, "lo", 1)):
            self.send(level, to, which, self.near(level, i, which), 1, to)

    def both(self, level):
        self.far(level)
        self.rest(level)

    def relay(self, level):
        arrive(self.g.at[self.spot(level, 0, "all")], self.rsem.at[level * 2], self.me.near(self.axes[level], 1))
        for to, which, i in ((1, "lo", 0), (-1, "hi", 1)):
            buf = self.way(level, i, which)
            spot = self.spot(level, to, which)
            self.g[spot] = (wider(self.g[spot]) + wider(buf[...])).astype(BF16)
        for to, which, i in ((1, "lo", 0), (-1, "hi", 1)):
            self.send(level, to, which, self.near(level, i, which), 1, to)

    def total(self, level):
        near = self.bufs[level][1]
        arrive(near, self.rsem.at[level * 2 + 1], self.me.near(self.axes[level], 1))
        spot = self.spot(level, 0, "all")
        return spot, wider(self.g[spot]) + wider(near[0]) + wider(near[1])

    def drain_at(self, level):
        places = pl.ds(0, 3) if level == 0 else 0
        wide = pl.ds(0, 4) if level == 0 else pl.ds(0, 3)
        drained(self.g.at[places, wide, 0, :, self.cols["all"]], self.ssem.at[level], self.me.near("z", 1))

    def drain(self):
        self.drain_at(0)
        self.drain_at(1)

    def fold(self):
        spot, total = self.total(0)
        self.g[spot] = total.astype(BF16)


class FineScatter(Scatter):
    slots = {2: 0, 1: 1, -1: 2, 0: 3}

    def place(self, q, p, which):
        at = {self.axes[0]: self.me.ring(self.axes[0], q), self.axes[1]: self.me.ring(self.axes[1], p)}
        return (at["z"], at["y"], self.xb, slice(None), self.cols[which])

    def give(self, q, p, which, dst, i, to):
        slot = self.slots[p]
        launch(
            self.g.at[self.place(q, p, which)], dst, self.ssem.at[2 + slot], self.rsem.at[4 + slot * 2 + i],
            self.me.near(self.axes[0], to),
        )

    def take(self, ref, p, i):
        arrive(ref, self.rsem.at[4 + self.slots[p] * 2 + i], self.me.near(self.axes[0], 1))

    def side(self, i, p, which):
        return self.bufs[0][1].at[i, self.slots[p], :, self.inner[which]]

    def step(self, i, p, which):
        return self.bufs[0][0].at[i, self.slots[p], :, pl.ds(0, self.inner[which].size)]

    def far0(self, *ps):
        for p in ps:
            for to, which, i in ((1, "lo", 0), (-1, "hi", 1)):
                self.give(2, p, which, self.step(i, p, which), 0, to)

    def rest0(self, *ps):
        for p in ps:
            for to, which, i in ((1, "hi", 0), (-1, "lo", 1)):
                self.give(to, p, which, self.side(i, p, which), 1, to)

    def relay0(self, *ps):
        for p in ps:
            self.take(self.g.at[self.place(0, p, "all")], p, 0)
            for to, which, i in ((1, "lo", 0), (-1, "hi", 1)):
                spot = self.place(to, p, which)
                self.g[spot] = pack(wider(self.g[spot]) + wider(self.step(i, p, which)[...]))
            for to, which, i in ((1, "lo", 0), (-1, "hi", 1)):
                self.give(to, p, which, self.side(i, p, which), 1, to)

    def fold0(self, *ps):
        for p in ps:
            near = self.bufs[0][1]
            self.take(near.at[:, self.slots[p]], p, 1)
            spot = self.place(0, p, "all")
            total = wider(self.g[spot]) + wider(near[0, self.slots[p]]) + wider(near[1, self.slots[p]])
            self.g[spot] = pack(total)

    def drain(self):
        self.drain_at(1)
        for slot in range(4):
            ref = self.g.at[0, pl.ds(0, 3), 0, :, self.cols["all"]]
            drained(ref, self.ssem.at[2 + slot], self.me.near("z", 1))


DMA = pltpu.SemaphoreType.DMA
VM = pl.BlockSpec(memory_space=pltpu.VMEM)
ANY = pl.BlockSpec(memory_space=pl.ANY)
OWN = 128
WIDTH = 1536
HEADS = 3
QKV = HEADS * HEAD_DIM
GELU_A = math.sqrt(2.0 / math.pi)
GELU_B = 0.044715


CHUNKS = ((0, OWN // 2), (OWN // 2, OWN // 2))


class SeqGather:
    def __init__(self, me, buf, rows, ssem, rsem, sends):
        self.me, self.buf, self.rows, self.ssem, self.rsem, self.sends = me, buf, pl.ds(*rows), ssem, rsem, sends

    def push(self, block, i, dev):
        ref = self.buf.at[block, self.rows]
        self.sends.start(ref, ref, self.ssem.at[i], self.rsem.at[i], dev)

    def start(self):
        self.push(self.me.s, 0, self.me.chip())
        self.push(self.me.s, 1, self.me.core())

    def relay(self):
        other = (1 - self.me.xl) * 2 + self.me.c
        arrive(self.buf.at[other, self.rows], self.rsem.at[0], self.me.chip())
        self.push(other, 2, self.me.core())

    def near(self):
        arrive(self.buf.at[self.me.xl * 2 + 1 - self.me.c, self.rows], self.rsem.at[1], self.me.core())

    def far(self):
        arrive(self.buf.at[(1 - self.me.xl) * 2 + 1 - self.me.c, self.rows], self.rsem.at[2], self.me.core())


class SeqScatter:
    def __init__(self, me, part, swap, mine, theirs, ssem, rsem):
        self.me, self.part, self.swap, self.mine, self.theirs = me, part, swap, mine, theirs
        self.ssem, self.rsem, self.sends = ssem, rsem, Sends()

    def give(self, i):
        xl = self.me.xl if i else 1 - self.me.xl
        self.sends.start(
            self.part.at[xl * 2 + 1 - self.me.c], self.swap.at[i], self.ssem.at[i], self.rsem.at[i], self.me.core()
        )

    def cross(self):
        arrive(self.swap.at[0], self.rsem.at[0], self.me.core())

        def merge(r):
            self.mine[r] = pack(wider(self.part[(1 - self.me.xl) * 2 + self.me.c, r]) + wider(self.swap[0, r]))

        for i, rows in enumerate(CHUNKS):
            by_rows(merge, rows)
            r = pl.ds(*rows)
            self.sends.start(
                self.mine.at[r], self.theirs.at[r], self.ssem.at[2 + i], self.rsem.at[2 + i], self.me.chip()
            )

    def wait(self, i):
        if i == 0:
            arrive(self.swap.at[1], self.rsem.at[1], self.me.core())
        arrive(self.theirs.at[pl.ds(*CHUNKS[i])], self.rsem.at[2 + i], self.me.chip())

    def rows(self, r):
        return wider(self.part[self.me.s, r]) + wider(self.swap[1, r]) + wider(self.theirs[r])


LEFT, RIGHT = pl.ds(0, HALF), pl.ds(HALF, HALF)


class RingGather:
    def __init__(self, me, buf, rows, ssem, rsem, sends):
        self.me, self.buf, self.rows, self.ssem, self.rsem, self.sends = me, buf, pl.ds(*rows), ssem, rsem, sends

    def at(self, step, mine=True, cols=pl.ds(0, WIDTH)):
        return self.buf.at[self.me.chip_at(step) * 2 + (self.me.c if mine else 1 - self.me.c), self.rows, cols]

    def push(self, ref, i, dev):
        self.sends.start(ref, ref, self.ssem.at[i], self.rsem.at[i], dev)

    def start(self):
        for cols, step, i in ((LEFT, 1, 0), (RIGHT, -1, 1), (RIGHT, 1, 9), (LEFT, -1, 10)):
            self.push(self.at(0, cols=cols), i, self.me.along(step))
        self.push(self.at(0), 2, self.me.core())

    def relay(self):
        for step, cols, i in ((-1, LEFT, 0), (1, RIGHT, 1)):
            arrive(self.at(step, cols=cols), self.rsem.at[i], self.me.core())
            self.push(self.at(step, cols=cols), 3 + i, self.me.along(-step))

    def spread(self):
        for step, cols, i in ((-1, RIGHT, 0), (1, LEFT, 1)):
            arrive(self.at(step, cols=cols), self.rsem.at[9 + i], self.me.core())
            self.push(self.at(step), 5 + i, self.me.core())

    def last(self):
        for cols, i in ((LEFT, 0), (RIGHT, 1)):
            arrive(self.at(2, cols=cols), self.rsem.at[3 + i], self.me.core())
            self.push(self.at(2, cols=cols), 7 + i, self.me.core())

    def own(self):
        arrive(self.at(0, False), self.rsem.at[2], self.me.core())

    def sides(self):
        for step, i in ((-1, 5), (1, 6)):
            arrive(self.at(step, False), self.rsem.at[i], self.me.core())

    def far(self):
        for cols, i in ((LEFT, 7), (RIGHT, 8)):
            arrive(self.at(2, False, cols), self.rsem.at[i], self.me.core())


class RingScatter:
    order = (2, 1, -1, 0)

    def __init__(self, me, part, swap, away, near, rows, ssem, rsem):
        self.me, self.part, self.swap, self.away, self.near = me, part, swap, away, near
        self.span, self.ssem, self.rsem, self.sends = rows, ssem, rsem, Sends()
        self.r = pl.ds(*rows)

    def block(self, step):
        return self.me.chip_at(step) * 2 + self.me.c

    def give(self, j):
        src = self.part.at[self.me.chip_at(self.order[j]) * 2 + 1 - self.me.c]
        self.sends.start(src, self.swap.at[j], self.ssem.at[j], self.rsem.at[j], self.me.core())

    def swapped(self, j):
        if self.span[0] == 0:
            arrive(self.swap.at[j], self.rsem.at[j], self.me.core())

    def push(self, step, cols, dst, i, to):
        self.sends.start(
            self.part.at[self.block(step), self.r, cols], dst, self.ssem.at[i], self.rsem.at[i], self.me.along(to)
        )

    def out(self):
        self.swapped(0)
        block = self.block(2)

        def merge(r):
            self.part[block, r] = pack(wider(self.part[block, r]) + wider(self.swap[0, r]))

        by_rows(merge, self.span)
        self.push(2, LEFT, self.away.at[0, self.r], 4, 1)
        self.push(2, RIGHT, self.away.at[1, self.r], 5, -1)

    def rest(self):
        for step, j, i, cols in ((1, 1, 0, RIGHT), (-1, 2, 1, LEFT)):
            self.swapped(j)
            block = self.block(step)

            def merge(r):
                self.part[block, r, cols] = pack(wider(self.part[block, r, cols]) + wider(self.swap[j, r, cols]))

            by_rows(merge, self.span)
            self.push(step, cols, self.near.at[i, self.r, cols], 8 + i, step)

    def relay(self):
        for step, j, i, cols in ((1, 1, 0, LEFT), (-1, 2, 1, RIGHT)):
            arrive(self.away.at[i, self.r], self.rsem.at[4 + i], self.me.core())
            block = self.block(step)

            def merge(r):
                both = wider(self.part[block, r, cols]) + wider(self.swap[j, r, cols])
                self.part[block, r, cols] = pack(both + wider(self.away[i, r]))

            by_rows(merge, self.span)
            self.push(step, cols, self.near.at[i, self.r, cols], 6 + i, step)

    def wait(self):
        self.swapped(3)
        for i, cols, rest in ((0, LEFT, RIGHT), (1, RIGHT, LEFT)):
            arrive(self.near.at[i, self.r, rest], self.rsem.at[8 + i], self.me.core())
            arrive(self.near.at[i, self.r, cols], self.rsem.at[6 + i], self.me.core())

    def rows(self, r):
        own = wider(self.part[self.block(0), r]) + wider(self.swap[3, r])
        return own + (wider(self.near[0, r]) + wider(self.near[1, r]))


def normalize(stream):
    centred = stream - jnp.mean(stream, axis=-1, keepdims=True)
    rstd = lax.rsqrt(jnp.mean(centred * centred, axis=-1, keepdims=True) + LN_EPS)
    return (centred * rstd, rstd)


def norm_back(normed, rstd, incoming):
    first = jnp.mean(incoming, axis=-1, keepdims=True)
    second = jnp.mean(incoming * normed, axis=-1, keepdims=True)
    return rstd * (incoming - first - normed * second)


def contract(left, right, left_dim, right_dim):
    return lax.dot_general(
        left, right, (((left_dim,), (right_dim,)), ((), ())), preferred_element_type=F32
    )


def softmax_rows(queries, key_rows, factor):
    scores = contract(queries, key_rows, 1, 1) * factor
    scores = jnp.exp(scores - jnp.max(scores, axis=-1, keepdims=True))
    return scores * (1.0 / jnp.sum(scores, axis=-1, keepdims=True))


def by_rows(body, rows=(0, OWN)):
    @pl.loop(rows[0] // 32, (rows[0] + rows[1]) // 32)
    def _(i):
        body(pl.ds(pl.multiple_of(i * 32, 32), 32))


def step_kernel(
    grad_scale, factor,
    tok, mod, wq, wo, wi, wb, og,
    final, grad, oq, oo, oi, ob,
    wa, wf, ga, gf, r1, r2, p1, p2, r3, r4, p3, p4, xbuf, part, partf, xf, a1, a2, dm, da, packed, att, datt, act, dg, du,
    pf, swap, own_sum, theirs, swapf, away, near, middle,
    gs, gr, ss, rs, xs, xr, ys, yr, es, er, csem,
):
    me = Place()
    mine_f = pl.multiple_of(me.xh * HALF, HALF)
    other_f = pl.multiple_of((1 - me.xh) * HALF, HALF)
    home_a, home_f = wa.at[me.z, me.y, me.xh], wf.at[me.z, me.y, me.xh]
    parts = [
        (wq.at[j, :, pl.ds(h * HEAD_DIM, HEAD_DIM)], home_a.at[:, pl.ds(h * QKV + j * HEAD_DIM, HEAD_DIM)])
        for h in range(HEADS) for j in range(3)
    ] + [
        (wo, home_a.at[:, pl.ds(3 * QKV, QKV)]),
        (wi.at[:, pl.ds(mine_f, HALF)], home_f.at[:, LEFT]),
        (wb.at[:, pl.ds(mine_f, HALF)], home_f.at[:, RIGHT]),
    ]
    loads = [pltpu.make_async_copy(src, dst, csem.at[i]) for i, (src, dst) in enumerate(parts)]
    for load in loads:
        load.start()
    greet(torus_peers(me))
    for load in loads:
        load.wait()
    mine, other = me.xl, 1 - me.xl

    def m(i):
        return mod[i]

    sends = Sends()
    yz, zy = ("y", "z"), ("z", "y")
    plan = [
        (wa, 0, [(yz, (0, 384, 256)), (zy, (640, 256, 256))]), (wa, 1, [(zy, (0, 384, 256)), (yz, (640, 256, 256))]),
        (wa, 0, [(yz, (1152, 256, 128))]), (wa, 1, [(zy, (1152, 256, 128))]),
        (wf, 0, [(yz, (0, 384, 384)), (zy, (768, 384, 384))]), (wf, 1, [(yz, (0, 384, 384)), (zy, (768, 384, 384))]),
    ]
    pieces = []
    count = 0
    for ref, side, halves in plan:
        pieces.append([])
        for axes, span in halves:
            xb = 1 - me.xh if side else me.xh
            pieces[-1].append(Gather(me, ref, axes, span, xb, gs.at[count], gr.at[count], sends))
            count += 1

    def gather_event(k, what):
        if what == "first" and k % 2:
            for i, ref, cols in crossed[k]:
                arrive(ref.at[me.z, me.y, 1 - me.xh, :, cols], xr.at[i], me.across())
        for half in pieces[k]:
            getattr(half, what)()

    crossed = {1: [(0, wa, pl.ds(0, 3 * QKV))], 3: [(1, wa, pl.ds(3 * QKV, QKV))], 5: [(2, wf, LEFT), (3, wf, RIGHT)]}

    def cross(group):
        if group < 2:
            ref = home_a.at[:, crossed[2 * group + 1][0][2]]
            sends.start(ref, ref, xs.at[group], xr.at[group], me.across())
        else:
            for i, ref, cols in ((2, wi, LEFT), (3, wb, RIGHT)):
                sends.start(ref.at[:, pl.ds(other_f, HALF)], home_f.at[:, cols], xs.at[i], xr.at[i], me.across())

    def ag(*steps):
        names = {
            "f": "first", "s": "second", "l": "last", "o": "own", "i": "sides", "e": "end", "r": "relay", "c": "close"
        }
        for step in steps:
            gather_event(int(step[1]), names[step[0]])

    scatters = []
    for k in range(10):
        side = k % 2
        xb = me.xh if side else 1 - me.xh
        if k < 4:
            span, axes = ((HALF, 384, 384), (0, 384, 384))[k // 2], (yz, zy, zy, yz)[k]
        else:
            span, axes = ((3 * QKV, 256, 128), (0, 384, 384), (2 * QKV, 256, 128))[k // 2 - 2], (zy, yz, zy, yz, yz, zy)[k - 4]
        kind = Scatter if k < 4 else FineScatter
        if span[1] == 384:
            n = k if k < 4 else k - 2
            bufs = ((r1.at[n], r2.at[n]), (p1.at[n], p2.at[n]))
        else:
            n = k - 4 if k < 6 else k - 6
            bufs = ((r3.at[n], r4.at[n]), (p3.at[n], p4.at[n]))
        scatters.append(kind(me, gf if k < 4 else ga, axes, span, xb, bufs, ss.at[k], rs.at[k], sends))

    def finish(k):
        scatter = scatters[k]
        _, total = scatter.total(1)
        cols = scatter.cols["all"]
        group = k // 2
        if k < 4:
            out = (ob, oi)[group].at[:, pl.ds(mine_f, HALF)]
            if k % 2:
                out[...] = total
            else:
                partf[group] = pack(total)
                sends.start(partf.at[group], xf.at[group], ys.at[group], yr.at[group], me.across())
        elif k % 2 == 0:
            part[:, cols] = pack(total)
            sends.start(part.at[:, cols], xbuf.at[:, cols], ys.at[group], yr.at[group], me.across())
        else:
            arrive(xbuf.at[:, cols], yr.at[group], me.across())
            total = total + wider(xbuf[:, cols])
            for i in range(cols.size // QKV):
                value = total[:, i * QKV : (i + 1) * QKV]
                head = cols.start // QKV + i
                if head == HEADS:
                    oo[...] = value
                else:
                    for j in range(3):
                        oq[j, :, pl.ds(head * HEAD_DIM, HEAD_DIM)] = value[:, j * HEAD_DIM : (j + 1) * HEAD_DIM]

    def rsc(*steps):
        names = {
            "f": ("both", 0), "r": ("relay", 0), "d": ("fold",), "g": ("both", 1), "s": ("relay", 1),
            "F": ("far0",), "N": ("rest0",), "R": ("relay0",), "D": ("fold0",), "G": ("far", 1), "H": ("rest", 1),
        }
        spots = {"": (2, 1, -1, 0), "a": (2,), "b": (1, -1), "c": (0,), "ab": (2, 1, -1), "bc": (1, -1, 0)}
        for step in steps:
            scatter_event(step, int(step[1]), names, spots)

    def scatter_event(step, k, names, spots):
        if step[0] == "e":
            finish(k)
        else:
            name, *args = names[step[0]]
            if step[0] in "FNRD":
                args = spots[step[2:]]
            getattr(scatters[k], name)(*args)

    def rows_of(ref, side, cols=slice(None)):
        value = ref[pl.ds(side * 2, 2), :, cols]
        return value.reshape(2 * OWN, value.shape[-1])

    def forward(src, side, w, col, width, emit):
        weight = w[:, :, :, :, pl.ds(col, width)].reshape(WIDTH, width)
        emit(contract(rows_of(src, side), weight, 1, 0).reshape(2, OWN, width))

    def backward(src, side, w, col, width, out):
        @pl.loop(0, 2)
        def _(j):
            weight = w[pl.ds(j * 2, 2), :, :, :, pl.ds(col, width)].reshape(HALF, width)
            at = pl.multiple_of(j * HALF, 128)
            value = contract(rows_of(src, side), weight, 1, 1)
            out[pl.ds(side * 2, 2), :, pl.ds(at, HALF)] = pack(value).reshape(2, OWN, HALF)

    def gradient(left, right, g, col, width):
        count = left.shape[0] * OWN

        @pl.loop(0, 4)
        def _(j):
            rows = left[:, :, pl.ds(pl.multiple_of(j * 384, 128), 384)].reshape(count, 384)
            value = contract(rows, right[...].reshape(count, width), 0, 0) * grad_scale
            g[j, :, :, :, pl.ds(col, width)] = pack(value).reshape(4, 2, ROWS, width)

    every = (0, OWN)
    x_a1 = SeqGather(me, a1, every, es.at[0], er.at[0], sends)
    x_das = [SeqGather(me, da, rows, es.at[1 + i], er.at[1 + i], sends) for i, rows in enumerate(CHUNKS)]
    a2_sends = Sends()
    x_a2s = [RingGather(me, a2, rows, es.at[3 + i], er.at[3 + i], a2_sends) for i, rows in enumerate(CHUNKS)]
    x_dm = RingGather(me, dm, every, es.at[5], er.at[5], sends)
    y_att = SeqScatter(me, pf.at[pl.ds(0, 4)], swap, own_sum, theirs, es.at[6], er.at[6])
    y_first = SeqScatter(me, a2.at[pl.ds(0, 4)], swap, own_sum, theirs, es.at[7], er.at[7])
    y_backs = [
        RingScatter(me, pf, swapf.at[0], away.at[0], near.at[0], rows, es.at[8 + i], er.at[8 + i])
        for i, rows in enumerate(CHUNKS)
    ]
    y_back = y_backs[0]
    y_ffn = RingScatter(me, pf, swapf.at[1], away.at[1], near.at[1], every, es.at[10], er.at[10])

    def all_of(objects, *names):
        for name in names:
            for item in objects:
                getattr(item, name)()

    def share(y, src, col, width):
        backward(src, other, wa, col, width, y.part)
        y.give(0)
        backward(src, mine, wa, col, width, y.part)
        y.give(1)
        y.cross()

    def first_norm(r):
        n1, _ = normalize(wider(tok[r]))
        a1[me.s, r] = pack(n1 * (1.0 + m(1)) + m(0))

    def gate(r):
        dm[me.n, r] = pack(m(5) * wider(og[r]))

    def put(dst, side):
        def emit(value):
            dst[pl.ds(side * 2, 2)] = pack(value)
        return emit

    def head_cols(place, head):
        return pl.ds(pl.multiple_of(head * QKV + place * HEAD_DIM, HEAD_DIM), HEAD_DIM)

    def own_cols(head):
        return pl.ds(pl.multiple_of(head * HEAD_DIM, HEAD_DIM), HEAD_DIM)

    def head_rows(ref, cols):
        return ref[:, :, cols].reshape(4 * OWN, HEAD_DIM)

    def attend(head):
        q, k, v = (head_rows(packed, head_cols(i, head)) for i in range(3))
        probs = softmax_rows(q, k, factor)
        att[:, :, own_cols(head)] = pack(contract(pack(probs), v, 1, 0)).reshape(4, OWN, HEAD_DIM)

    def attend_back(head):
        q, k, v = (head_rows(packed, head_cols(i, head)) for i in range(3))
        up = head_rows(datt, own_cols(head))
        probs = softmax_rows(q, k, factor)
        dprobs = contract(up, v, 1, 1)
        dscores = pack(probs * (dprobs - jnp.sum(probs * dprobs, axis=-1, keepdims=True)) * factor)
        parts = (contract(dscores, k, 1, 0), contract(dscores, q, 0, 0), contract(pack(probs), up, 0, 0))
        for i, value in enumerate(parts):
            packed[:, :, head_cols(i, head)] = pack(value).reshape(4, OWN, HEAD_DIM)

    def heads(body, low=0, high=HEADS):
        pl.loop(low, high)(body)

    def second_norm(r):
        mid = wider(tok[r]) + m(2) * y_att.rows(r)
        middle[r] = mid
        n2, _ = normalize(mid)
        a2[me.n, r] = pack(n2 * (1.0 + m(4)) + m(3))

    def hidden(chip):
        def emit(u):
            t = jnp.tanh(GELU_A * (u + GELU_B * (u * u * u)))
            at = pl.ds(chip * 2, 2)
            act[at] = pack(0.5 * u * (1.0 + t))
            slope = 0.5 * (1.0 + t) + (0.5 * GELU_A) * u * (1.0 - t * t) * (1.0 + (3.0 * GELU_B) * (u * u))
            du[at] = pack(slope * dg[at])
        forward(a2, chip, wf, 0, HALF, emit)

    def hidden_back(chip):
        def emit(value):
            dg[pl.ds(chip * 2, 2)] = value
        forward(dm, chip, wf, HALF, HALF, emit)

    def middle_back(r):
        n2, rstd = normalize(middle[r])
        up = wider(og[r]) + norm_back(n2, rstd, y_back.rows(r) * (1.0 + m(4)))
        grad[r] = up
        da[me.s, r] = pack(m(2) * up)

    def last_out(r):
        final[r] = pack(middle[r] + m(5) * y_ffn.rows(r))

    def first_back(r):
        n1, rstd = normalize(wider(tok[r]))
        grad[r] = grad[r] + norm_back(n1, rstd, y_first.rows(r) * (1.0 + m(1)))

    def sides(i):
        hidden(me.chip_at(2 * i - 1))

    def backs(i):
        hidden_back(me.chip_at(i))

    def norm_and_send(i):
        y_att.wait(i)
        by_rows(second_norm, CHUNKS[i])
        x_a2s[i].start()

    def back_and_send(i):
        y_backs[i].wait()
        by_rows(middle_back, CHUNKS[i])
        x_das[i].start()

    def norm_and_send(i):
        y_att.wait(i)
        by_rows(second_norm, CHUNKS[i])
        x_a2s[i].start()

    def back_and_send(i):
        y_backs[i].wait()
        by_rows(middle_back, CHUNKS[i])
        x_das[i].start()

    cross(0)
    ag("f0", "o0", "f4", "o4")
    by_rows(first_norm)
    x_a1.start()
    cross(1)
    cross(2)
    by_rows(gate)
    x_dm.start()
    ag("s0", "i0", "f1", "o1", "l0", "e0", "f2", "s1", "i1", "l1", "e1", "r0", "s2", "f3")
    x_a1.relay()
    ag("o2", "i2", "r1", "l2", "e2", "o3", "s3", "i3")
    x_dm.relay()
    ag("c0")
    x_a1.near()
    x_a1.far()
    ag("c1")
    forward(a1, mine, wa, 0, 3 * QKV, put(packed, mine))
    ag("l3", "e3")
    forward(a1, other, wa, 0, 3 * QKV, put(packed, other))
    ag("r2", "s4", "i4")
    heads(attend, 0, 1)
    ag("r3", "l4", "e4", "f5", "o5")
    heads(attend, 1, 3)
    ag("c2", "c3")
    share(y_att, att, 3 * QKV, QKV)
    x_dm.spread()
    ag("s5", "i5", "l5", "e5")
    x_dm.last()
    ag("r4")
    norm_and_send(0)
    ag("r5")
    norm_and_send(1)
    x_a2s[0].relay()
    y_att.sends.close()
    x_dm.own()
    x_dm.sides()
    x_dm.far()
    all_of(x_a2s, "own")
    ag("c4", "c5")
    pl.loop(0, 2)(backs)
    x_a2s[1].relay()
    hidden(me.x)
    all_of(x_a2s, "spread")
    pl.loop(2, 4)(backs)
    all_of(x_a2s, "sides")
    pl.loop(0, 2)(sides)
    all_of(x_a2s, "last")

    backward(du, me.chip_at(1), wf, 0, HALF, pf)
    y_back.give(1)
    all_of(x_a2s, "far")
    hidden(me.chip_at(2))
    backward(du, me.chip_at(2), wf, 0, HALF, pf)
    y_back.give(0)
    backward(du, me.chip_at(-1), wf, 0, HALF, pf)
    y_back.give(2)
    all_of(y_backs, "out")
    backward(du, me.chip_at(0), wf, 0, HALF, pf)
    y_back.give(3)
    all_of(y_backs, "rest")
    gradient(dm, act, gf, HALF, HALF)
    rsc("f0", "f1")
    all_of(y_backs, "relay")
    gradient(a2, du, gf, 0, HALF)
    rsc("r0", "r1", "f2", "f3")
    back_and_send(0)
    back_and_send(1)
    y_backs[0].sends.close()
    y_backs[1].sends.close()
    a2_sends.close()
    backward(act, me.chip_at(2), wf, HALF, HALF, pf)
    y_ffn.give(0)
    backward(act, me.chip_at(1), wf, HALF, HALF, pf)
    y_ffn.give(1)
    rsc("d0", "g0", "d1", "g1")
    x_das[0].relay()
    backward(act, me.chip_at(-1), wf, HALF, HALF, pf)
    y_ffn.give(2)
    rsc("r2", "r3")
    backward(act, me.chip_at(0), wf, HALF, HALF, pf)
    y_ffn.give(3)
    x_das[1].relay()
    all_of(x_das, "near")
    forward(da, mine, wa, 3 * QKV, QKV, put(datt, mine))
    all_of(x_das, "far")
    forward(da, other, wa, 3 * QKV, QKV, put(datt, other))
    y_ffn.out()
    gradient(da, att, ga, 3 * QKV, QKV)
    rsc("F4", "F5", "N4", "N5")
    heads(attend_back, 0, 2)
    y_ffn.rest()
    rsc("d2", "g2", "d3", "g3", "s0", "s1")
    gradient(a1, packed.at[:, :, pl.ds(0, HALF)], ga, 0, HALF)
    rsc("F6", "F7", "N6", "N7", "R4", "R5")
    heads(attend_back, 2, 3)
    gradient(a1, packed.at[:, :, pl.ds(HALF, QKV)], ga, HALF, QKV)
    rsc("F8", "F9", "N8", "N9", "s2", "s3", "R6a", "R7a", "R6b", "R7b", "R6c", "R7c", "e0")
    y_ffn.relay()
    share(y_first, packed, 0, 3 * QKV)
    rsc("R8a", "R9a", "R8b", "R9b", "R8c", "R9c", "D4", "G4", "H4", "D5", "G5", "H5")
    rsc("D6a", "G6", "D7a", "G7", "D6b", "H6", "D7b", "H7", "D6c", "D7c", "e2")
    rsc("D8a", "G8", "D9a", "G9", "D8b", "H8", "D9b", "H9", "D8c", "D9c", "s4", "s5", "s6", "s7", "s8", "s9")
    rsc("e4", "e6", "e8")
    y_ffn.wait()
    by_rows(last_out)
    y_first.wait(0)
    y_first.wait(1)
    by_rows(first_back)
    rsc("e1", "e3")
    for group, out in enumerate((ob, oi)):
        arrive(xf.at[group], yr.at[group], me.across())
        out[:, pl.ds(other_f, HALF)] = wider(xf[group])
    rsc("e5", "e7", "e9")
    for piece in pieces:
        for half in piece:
            half.drain()
    for scatter in scatters:
        scatter.drain()
    sends.close()
    y_first.sends.close()
    y_ffn.sends.close()


def copy_kernel(*refs):
    n = len(refs) // 2
    sem = refs[-1]
    copies = [pltpu.make_async_copy(refs[i], refs[n + i], sem.at[i]) for i in range(n)]
    for copy in copies:
        copy.start()
    for copy in copies:
        copy.wait()


def copy_out(arrays):
    return pl.pallas_call(
        copy_kernel,
        out_shape=[jax.ShapeDtypeStruct(a.shape, a.dtype) for a in arrays],
        in_specs=[VM] * len(arrays),
        out_specs=[ANY] * len(arrays),
        scratch_shapes=[DMA((len(arrays),))],
    )(*arrays)


def local(tokens, modulation, w_qkv, w_out, w_in, w_back, out_grad):
    grad_scale = 1.0 / math.sqrt(OWN * lax.axis_size("sp") * lax.axis_size("fsdp"))
    factor = TEMPER / math.sqrt(HEAD_DIM)

    def shape(dims, dtype=BF16):
        return jax.ShapeDtypeStruct(dims, dtype)

    def vm(*dims, dtype=BF16):
        return pltpu.VMEM(dims, dtype)

    seq, ring = (4, OWN, WIDTH), (8, OWN, WIDTH)
    results = pl.pallas_call(
        functools.partial(step_kernel, grad_scale, factor),
        out_shape=(
            shape((OWN, WIDTH)), shape((OWN, WIDTH), F32), shape((3, ROWS, QKV), F32),
            shape((ROWS, QKV), F32), shape((ROWS, GROUP), F32), shape((ROWS, GROUP), F32),
        ),
        in_specs=[VM, VM, ANY, ANY, ANY, ANY, VM],
        out_specs=(VM,) * 6,
        scratch_shapes=[
            vm(4, 4, 2, ROWS, GROUP), vm(4, 4, 2, ROWS, GROUP), vm(4, 4, 2, ROWS, GROUP), vm(4, 4, 2, ROWS, GROUP),
            vm(6, 2, 4, ROWS, QUART), vm(6, 2, 4, ROWS, HALF), vm(6, 2, ROWS, QUART), vm(6, 2, ROWS, HALF),
            vm(4, 2, 4, ROWS, 256), vm(4, 2, 4, ROWS, 384), vm(4, 2, ROWS, 256), vm(4, 2, ROWS, 384),
            vm(ROWS, GROUP), vm(ROWS, GROUP), vm(2, ROWS, HALF), vm(2, ROWS, HALF),
            vm(*seq), vm(*ring), vm(*ring), vm(*seq),
            vm(4, OWN, 3 * QKV), vm(4, OWN, QKV), vm(4, OWN, QKV),
            vm(8, OWN, HALF), vm(8, OWN, HALF, dtype=F32), vm(8, OWN, HALF),
            vm(*ring), vm(2, OWN, WIDTH), vm(OWN, WIDTH), vm(OWN, WIDTH),
            vm(2, 4, OWN, WIDTH), vm(2, 2, OWN, HALF), vm(2, 2, OWN, WIDTH), vm(OWN, WIDTH, dtype=F32),
            DMA((10, 2)), DMA((10, 6)), DMA((10, 6)), DMA((10, 12)),
            DMA((4,)), DMA((4,)), DMA((5,)), DMA((5,)), DMA((11, 11)), DMA((11, 11)), DMA((12,)),
        ],
        compiler_params=pltpu.CompilerParams(
            collective_id=0, has_side_effects=True, vmem_limit_bytes=67043328
        ),
    )(
        tokens[0], modulation.transpose(2, 0, 1, 3)[:, 0],
        w_qkv[0].transpose(1, 0, 2), w_out[0].T, w_in[0], w_back[0].T, out_grad[0],
    )
    final, grad, oq, oo, oi, ob = copy_out(results)
    return (
        final[None], grad[None], oq.transpose(1, 0, 2)[None], oo.T[None], oi[None], ob.T[None],
    )


def solution(mesh):
    weights = (
        P(None, "fsdp", None, "sp"),
        P(None, "sp", "fsdp"),
        P(None, "fsdp", "sp"),
        P(None, "sp", "fsdp"),
    )
    rows = P("fsdp", "sp", None)
    return jax.shard_map(
        local,
        mesh=mesh,
        in_specs=(rows, P("fsdp", None, None, None), *weights, rows),
        out_specs=(rows, rows, *weights),
        check_vma=False,
    )
```

```python
import functools
import math

import jax
import jax.numpy as jnp
from jax import lax
from jax.experimental import pallas as pl
from jax.experimental.pallas import tpu as pltpu
from jax.sharding import PartitionSpec as P

HEAD_DIM = 128
LN_EPS = 1e-06
TEMPER = 2.5
F32 = jnp.float32
BF16 = jnp.bfloat16
MESH = pl.DeviceIdType.MESH
GROUP = 1536
HALF = GROUP // 2
QUART = GROUP // 4
ROWS = 48


def rem(a, n):
    return lax.rem(a, n)


class Place:
    def __init__(self):
        f = lax.axis_index("fsdp")
        s = lax.axis_index("sp")
        self.z, self.y, self.xh = lax.div(f, 8), rem(lax.div(f, 2), 4), rem(f, 2)
        self.xl, self.c = lax.div(s, 2), rem(s, 2)
        self.s = s
        self.x = self.xh * 2 + self.xl
        self.n = self.x * 2 + self.c

    def dev(self, **kw):
        v = {k: kw.get(k, getattr(self, k)) for k in ("z", "y", "xh", "xl", "c")}
        return (v["z"] * 8 + v["y"] * 2 + v["xh"], v["xl"] * 2 + v["c"])

    def ring(self, axis, step):
        return rem(getattr(self, axis) + step + 4, 4)

    def near(self, axis, step):
        return self.dev(**{axis: self.ring(axis, step)})

    def along(self, step):
        x = rem(self.x + step + 4, 4)
        return self.dev(xh=lax.div(x, 2), xl=rem(x, 2))

    def chip_at(self, step):
        return rem(self.x + step + 4, 4)

    def across(self):
        return self.dev(xh=1 - self.xh)

    def chip(self):
        return self.dev(xl=1 - self.xl)

    def core(self):
        return self.dev(c=1 - self.c)


def greet(devices):
    barrier = pltpu.get_barrier_semaphore()
    for d in devices:
        pl.semaphore_signal(barrier, inc=1, device_id=d, device_id_type=MESH)
    pl.semaphore_wait(barrier, len(devices))


def torus_peers(me):
    return [me.near(a, s) for a in ("z", "y") for s in (1, -1)] + [me.across(), me.along(1), me.along(-1), me.core()]


class Sends:
    def __init__(self):
        self.open = []

    def start(self, src, dst, ssem, rsem, dev):
        copy = pltpu.make_async_remote_copy(
            src_ref=src, dst_ref=dst, send_sem=ssem, recv_sem=rsem, device_id=dev, device_id_type=MESH
        )
        copy.start()
        self.open.append(copy)

    def close(self):
        for copy in self.open:
            copy.wait_send()
        self.open = []


def launch(src, dst, ssem, rsem, dev):
    pltpu.make_async_remote_copy(
        src_ref=src, dst_ref=dst, send_sem=ssem, recv_sem=rsem, device_id=dev, device_id_type=MESH
    ).start()


def drained(ref, ssem, dev):
    pltpu.make_async_remote_copy(
        src_ref=ref, dst_ref=ref, send_sem=ssem, recv_sem=ssem, device_id=dev, device_id_type=MESH
    ).wait_send()


def arrive(ref, rsem, dev):
    pltpu.make_async_remote_copy(
        src_ref=ref, dst_ref=ref, send_sem=rsem, recv_sem=rsem, device_id=dev, device_id_type=MESH
    ).wait_recv()


def columns(start, low, high):
    return {"all": pl.ds(start, low + high), "lo": pl.ds(start, low), "hi": pl.ds(start + low, high)}


class Gather:
    def __init__(self, me, w, axes, span, xb, ssem, rsem, sends):
        self.me, self.w, self.axes, self.xb = me, w, axes, xb
        self.ssem, self.rsem, self.sends = ssem, rsem, sends
        self.cols = columns(*span)

    def part(self, p, q, which):
        first, second = self.axes
        at = {first: slice(None) if p is None else self.me.ring(first, p), second: self.me.ring(second, q)}
        return self.w.at[at["z"], at["y"], self.xb, :, self.cols[which]]

    def go(self, level, to, p, q, which, i):
        ref = self.part(p, q, which)
        launch(ref, ref, self.ssem.at[level], self.rsem.at[i], self.me.near(self.axes[level], to))

    def got(self, p, q, which, i):
        arrive(self.part(p, q, which), self.rsem.at[i], self.me.near(self.axes[0], 1))

    def first(self):
        self.go(0, 1, 0, 0, "all", 0)
        self.go(0, -1, 0, 0, "all", 1)

    def second(self):
        self.got(-1, 0, "all", 0)
        self.go(0, 1, -1, 0, "lo", 2)
        self.got(1, 0, "all", 1)
        self.go(0, -1, 1, 0, "hi", 2)

    def last(self):
        self.got(2, 0, "all", 2)

    def out(self, *ps):
        for p in ps:
            self.go(1, 1, p, 0, "all", 3)
            self.go(1, -1, p, 0, "all", 4)

    def own(self):
        self.out(0)

    def sides(self):
        self.out(-1, 1)

    def end(self):
        self.out(2)

    def relay(self):
        self.got(None, -1, "all", 3)
        self.go(1, 1, None, -1, "lo", 5)
        self.got(None, 1, "all", 4)
        self.go(1, -1, None, 1, "hi", 5)

    def close(self):
        self.got(None, 2, "all", 5)

    def drain(self):
        cols = self.cols["all"]
        drained(self.w.at[0, pl.ds(0, 3), 0, :, cols], self.ssem.at[0], self.me.near("z", 1))
        drained(self.w.at[pl.ds(0, 3), pl.ds(0, 4), 0, :, cols], self.ssem.at[1], self.me.near("z", 1))


def wider(ref_value):
    return ref_value.astype(F32)


def pack(total):
    return total.astype(BF16)


class Scatter:
    def __init__(self, me, g, axes, span, xb, bufs, ssem, rsem, sends):
        self.me, self.g, self.axes, self.xb = me, g, axes, xb
        self.bufs, self.ssem, self.rsem, self.sends = bufs, ssem, rsem, sends
        self.cols = columns(*span)
        self.inner = columns(0, *span[1:])

    def spot(self, level, step, which):
        axis = self.axes[level]
        at = {"z": self.me.z, "y": self.me.y}
        at[axis] = self.me.ring(axis, step)
        if level == 0:
            at[self.axes[1]] = slice(None)
        return (at["z"], at["y"], self.xb, slice(None), self.cols[which])

    def way(self, level, i, which):
        if level == 0:
            return self.bufs[0][0].at[i, :, :, columns(0, *self.sizes(which))["lo"]]
        return self.bufs[1][0].at[i, :, columns(0, *self.sizes(which))["lo"]]

    def sizes(self, which):
        return self.inner[which].size, 0

    def send(self, level, step, which, dst, i, to):
        launch(
            self.g.at[self.spot(level, step, which)], dst, self.ssem.at[level], self.rsem.at[level * 2 + i],
            self.me.near(self.axes[level], to),
        )

    def near(self, level, i, which):
        cols = self.inner[which]
        if level == 0:
            return self.bufs[level][1].at[i, :, :, cols]
        return self.bufs[level][1].at[i, :, cols]

    def far(self, level):
        for to, which, i in ((1, "lo", 0), (-1, "hi", 1)):
            self.send(level, 2, which, self.way(level, i, which), 0, to)

    def rest(self, level):
        for to, which, i in ((1, "hi", 0), (-1, "lo", 1)):
            self.send(level, to, which, self.near(level, i, which), 1, to)

    def both(self, level):
        self.far(level)
        self.rest(level)

    def relay(self, level):
        arrive(self.g.at[self.spot(level, 0, "all")], self.rsem.at[level * 2], self.me.near(self.axes[level], 1))
        for to, which, i in ((1, "lo", 0), (-1, "hi", 1)):
            buf = self.way(level, i, which)
            spot = self.spot(level, to, which)
            self.g[spot] = (wider(self.g[spot]) + wider(buf[...])).astype(BF16)
        for to, which, i in ((1, "lo", 0), (-1, "hi", 1)):
            self.send(level, to, which, self.near(level, i, which), 1, to)

    def total(self, level):
        near = self.bufs[level][1]
        arrive(near, self.rsem.at[level * 2 + 1], self.me.near(self.axes[level], 1))
        spot = self.spot(level, 0, "all")
        return spot, wider(self.g[spot]) + wider(near[0]) + wider(near[1])

    def drain_at(self, level):
        places = pl.ds(0, 3) if level == 0 else 0
        wide = pl.ds(0, 4) if level == 0 else pl.ds(0, 3)
        drained(self.g.at[places, wide, 0, :, self.cols["all"]], self.ssem.at[level], self.me.near("z", 1))

    def drain(self):
        self.drain_at(0)
        self.drain_at(1)

    def fold(self):
        spot, total = self.total(0)
        self.g[spot] = total.astype(BF16)


class FineScatter(Scatter):
    slots = {2: 0, 1: 1, -1: 2, 0: 3}

    def place(self, q, p, which):
        at = {self.axes[0]: self.me.ring(self.axes[0], q), self.axes[1]: self.me.ring(self.axes[1], p)}
        return (at["z"], at["y"], self.xb, slice(None), self.cols[which])

    def give(self, q, p, which, dst, i, to):
        slot = self.slots[p]
        launch(
            self.g.at[self.place(q, p, which)], dst, self.ssem.at[2 + slot], self.rsem.at[4 + slot * 2 + i],
            self.me.near(self.axes[0], to),
        )

    def take(self, ref, p, i):
        arrive(ref, self.rsem.at[4 + self.slots[p] * 2 + i], self.me.near(self.axes[0], 1))

    def side(self, i, p, which):
        return self.bufs[0][1].at[i, self.slots[p], :, self.inner[which]]

    def step(self, i, p, which):
        return self.bufs[0][0].at[i, self.slots[p], :, pl.ds(0, self.inner[which].size)]

    def far0(self, *ps):
        for p in ps:
            for to, which, i in ((1, "lo", 0), (-1, "hi", 1)):
                self.give(2, p, which, self.step(i, p, which), 0, to)

    def rest0(self, *ps):
        for p in ps:
            for to, which, i in ((1, "hi", 0), (-1, "lo", 1)):
                self.give(to, p, which, self.side(i, p, which), 1, to)

    def relay0(self, *ps):
        for p in ps:
            self.take(self.g.at[self.place(0, p, "all")], p, 0)
            for to, which, i in ((1, "lo", 0), (-1, "hi", 1)):
                spot = self.place(to, p, which)
                self.g[spot] = pack(wider(self.g[spot]) + wider(self.step(i, p, which)[...]))
            for to, which, i in ((1, "lo", 0), (-1, "hi", 1)):
                self.give(to, p, which, self.side(i, p, which), 1, to)

    def fold0(self, *ps):
        for p in ps:
            near = self.bufs[0][1]
            self.take(near.at[:, self.slots[p]], p, 1)
            spot = self.place(0, p, "all")
            total = wider(self.g[spot]) + wider(near[0, self.slots[p]]) + wider(near[1, self.slots[p]])
            self.g[spot] = pack(total)

    def drain(self):
        self.drain_at(1)
        for slot in range(4):
            ref = self.g.at[0, pl.ds(0, 3), 0, :, self.cols["all"]]
            drained(ref, self.ssem.at[2 + slot], self.me.near("z", 1))


DMA = pltpu.SemaphoreType.DMA
VM = pl.BlockSpec(memory_space=pltpu.VMEM)
ANY = pl.BlockSpec(memory_space=pl.ANY)
OWN = 128
WIDTH = 1536
HEADS = 3
QKV = HEADS * HEAD_DIM
GELU_A = math.sqrt(2.0 / math.pi)
GELU_B = 0.044715


CHUNKS = ((0, OWN // 2), (OWN // 2, OWN // 2))


class SeqGather:
    def __init__(self, me, buf, rows, ssem, rsem, sends):
        self.me, self.buf, self.rows, self.ssem, self.rsem, self.sends = me, buf, pl.ds(*rows), ssem, rsem, sends

    def push(self, block, i, dev):
        ref = self.buf.at[block, self.rows]
        launch(ref, ref, self.ssem.at[0], self.rsem.at[i], dev)

    def drain(self):
        drained(self.buf.at[pl.ds(0, 3), self.rows], self.ssem.at[0], self.me.core())

    def start(self):
        self.push(self.me.s, 0, self.me.chip())
        self.push(self.me.s, 1, self.me.core())

    def relay(self):
        other = (1 - self.me.xl) * 2 + self.me.c
        arrive(self.buf.at[other, self.rows], self.rsem.at[0], self.me.chip())
        self.push(other, 2, self.me.core())

    def near(self):
        arrive(self.buf.at[self.me.xl * 2 + 1 - self.me.c, self.rows], self.rsem.at[1], self.me.core())

    def far(self):
        arrive(self.buf.at[(1 - self.me.xl) * 2 + 1 - self.me.c, self.rows], self.rsem.at[2], self.me.core())


class SeqScatter:
    def __init__(self, me, part, swap, mine, theirs, ssem, rsem):
        self.me, self.part, self.swap, self.mine, self.theirs = me, part, swap, mine, theirs
        self.ssem, self.rsem = ssem, rsem

    def drain(self):
        drained(self.part.at[pl.ds(0, 3)], self.ssem.at[0], self.me.core())

    def give(self, i):
        xl = self.me.xl if i else 1 - self.me.xl
        launch(self.part.at[xl * 2 + 1 - self.me.c], self.swap.at[i], self.ssem.at[0], self.rsem.at[i], self.me.core())

    def cross(self):
        arrive(self.swap.at[0], self.rsem.at[0], self.me.core())

        def merge(r):
            self.mine[r] = pack(wider(self.part[(1 - self.me.xl) * 2 + self.me.c, r]) + wider(self.swap[0, r]))

        for i, rows in enumerate(CHUNKS):
            by_rows(merge, rows)
            r = pl.ds(*rows)
            launch(self.mine.at[r], self.theirs.at[r], self.ssem.at[0], self.rsem.at[2 + i], self.me.chip())

    def wait(self, i):
        if i == 0:
            arrive(self.swap.at[1], self.rsem.at[1], self.me.core())
        arrive(self.theirs.at[pl.ds(*CHUNKS[i])], self.rsem.at[2 + i], self.me.chip())

    def rows(self, r):
        return wider(self.part[self.me.s, r]) + wider(self.swap[1, r]) + wider(self.theirs[r])


LEFT, RIGHT = pl.ds(0, HALF), pl.ds(HALF, HALF)


class RingGather:
    def __init__(self, me, buf, rows, ssem, rsem, sends):
        self.me, self.buf, self.rows, self.ssem, self.rsem, self.sends = me, buf, pl.ds(*rows), ssem, rsem, sends

    def at(self, step, mine=True, cols=pl.ds(0, WIDTH)):
        return self.buf.at[self.me.chip_at(step) * 2 + (self.me.c if mine else 1 - self.me.c), self.rows, cols]

    def push(self, ref, i, dev):
        launch(ref, ref, self.ssem.at[0], self.rsem.at[i], dev)

    def drain(self):
        drained(self.buf.at[pl.ds(0, 7), self.rows], self.ssem.at[0], self.me.core())

    def start(self):
        for cols, step, i in ((LEFT, 1, 0), (RIGHT, -1, 1), (RIGHT, 1, 2), (LEFT, -1, 2)):
            self.push(self.at(0, cols=cols), i, self.me.along(step))
        self.push(self.at(0), 3, self.me.core())

    def relay(self):
        for step, cols, i in ((-1, LEFT, 0), (1, RIGHT, 1)):
            arrive(self.at(step, cols=cols), self.rsem.at[i], self.me.core())
            self.push(self.at(step, cols=cols), 4, self.me.along(-step))

    def spread(self):
        arrive(self.at(1), self.rsem.at[2], self.me.core())
        for step in (-1, 1):
            self.push(self.at(step), 5, self.me.core())

    def last(self):
        arrive(self.at(2), self.rsem.at[4], self.me.core())
        self.push(self.at(2), 6, self.me.core())

    def own(self):
        arrive(self.at(0, False), self.rsem.at[3], self.me.core())

    def sides(self):
        arrive(self.buf.at[pl.ds(0, 2), self.rows], self.rsem.at[5], self.me.core())

    def far(self):
        arrive(self.at(2, False), self.rsem.at[6], self.me.core())


class RingScatter:
    order = (2, 1, -1, 0)

    def __init__(self, me, part, swap, away, near, rows, ssem, rsem):
        self.me, self.part, self.swap, self.away, self.near = me, part, swap, away, near
        self.span, self.ssem, self.rsem = rows, ssem, rsem
        self.r = pl.ds(*rows)

    def block(self, step):
        return self.me.chip_at(step) * 2 + self.me.c

    def give(self, j):
        src = self.part.at[self.me.chip_at(self.order[j]) * 2 + 1 - self.me.c]
        launch(src, self.swap.at[j], self.ssem.at[0], self.rsem.at[j], self.me.core())

    def drain(self):
        if self.span[0] == 0:
            drained(self.part.at[pl.ds(0, 4)], self.ssem.at[0], self.me.core())
        drained(self.part.at[pl.ds(0, 3), self.r], self.ssem.at[1], self.me.core())

    def swapped(self, j):
        if self.span[0] == 0:
            arrive(self.swap.at[j], self.rsem.at[j], self.me.core())

    def push(self, step, cols, dst, i, to):
        launch(self.part.at[self.block(step), self.r, cols], dst, self.ssem.at[1], self.rsem.at[i], self.me.along(to))

    def out(self):
        self.swapped(0)
        block = self.block(2)

        def merge(r):
            self.part[block, r] = pack(wider(self.part[block, r]) + wider(self.swap[0, r]))

        by_rows(merge, self.span)
        self.push(2, LEFT, self.away.at[0, self.r], 4, 1)
        self.push(2, RIGHT, self.away.at[1, self.r], 4, -1)

    def rest(self):
        for step, j, i, cols in ((1, 1, 0, RIGHT), (-1, 2, 1, LEFT)):
            self.swapped(j)
            block = self.block(step)

            def merge(r):
                self.part[block, r, cols] = pack(wider(self.part[block, r, cols]) + wider(self.swap[j, r, cols]))

            by_rows(merge, self.span)
            self.push(step, cols, self.near.at[i, self.r, cols], 5, step)

    def relay(self):
        arrive(self.away.at[:, self.r], self.rsem.at[4], self.me.core())
        for step, j, i, cols in ((1, 1, 0, LEFT), (-1, 2, 1, RIGHT)):
            block = self.block(step)

            def merge(r):
                both = wider(self.part[block, r, cols]) + wider(self.swap[j, r, cols])
                self.part[block, r, cols] = pack(both + wider(self.away[i, r]))

            by_rows(merge, self.span)
            self.push(step, cols, self.near.at[i, self.r, cols], 5, step)

    def wait(self):
        self.swapped(3)
        arrive(self.near.at[:, self.r], self.rsem.at[5], self.me.core())

    def rows(self, r):
        own = wider(self.part[self.block(0), r]) + wider(self.swap[3, r])
        return own + (wider(self.near[0, r]) + wider(self.near[1, r]))


def normalize(stream):
    centred = stream - jnp.mean(stream, axis=-1, keepdims=True)
    rstd = lax.rsqrt(jnp.mean(centred * centred, axis=-1, keepdims=True) + LN_EPS)
    return (centred * rstd, rstd)


def norm_back(normed, rstd, incoming):
    first = jnp.mean(incoming, axis=-1, keepdims=True)
    second = jnp.mean(incoming * normed, axis=-1, keepdims=True)
    return rstd * (incoming - first - normed * second)


def contract(left, right, left_dim, right_dim):
    return lax.dot_general(
        left, right, (((left_dim,), (right_dim,)), ((), ())), preferred_element_type=F32
    )


def softmax_rows(queries, key_rows, factor):
    scores = contract(queries, key_rows, 1, 1) * factor
    scores = jnp.exp(scores - jnp.max(scores, axis=-1, keepdims=True))
    return scores * (1.0 / jnp.sum(scores, axis=-1, keepdims=True))


def by_rows(body, rows=(0, OWN)):
    @pl.loop(rows[0] // 32, (rows[0] + rows[1]) // 32)
    def _(i):
        body(pl.ds(pl.multiple_of(i * 32, 32), 32))


def step_kernel(
    grad_scale, factor,
    tok, mod, wq, wo, wi, wb, og,
    final, grad, oq, oo, oi, ob,
    wa, wf, ga, gf, r1, r2, p1, p2, r3, r4, p3, p4, xbuf, part, partf, xf, a1, a2, dm, da, packed, att, datt, act, dg, du,
    pf, swap, own_sum, theirs, swapf, away, near, middle,
    gs, gr, ss, rs, xs, xr, ys, yr, es, er, csem,
):
    me = Place()
    mine_f = pl.multiple_of(me.xh * HALF, HALF)
    other_f = pl.multiple_of((1 - me.xh) * HALF, HALF)
    home_a, home_f = wa.at[me.z, me.y, me.xh], wf.at[me.z, me.y, me.xh]
    parts = [
        (wq.at[j, :, pl.ds(h * HEAD_DIM, HEAD_DIM)], home_a.at[:, pl.ds(h * QKV + j * HEAD_DIM, HEAD_DIM)])
        for h in range(HEADS) for j in range(3)
    ] + [
        (wo, home_a.at[:, pl.ds(3 * QKV, QKV)]),
        (wi.at[:, pl.ds(mine_f, HALF)], home_f.at[:, LEFT]),
        (wb.at[:, pl.ds(mine_f, HALF)], home_f.at[:, RIGHT]),
    ]
    loads = [pltpu.make_async_copy(src, dst, csem.at[i]) for i, (src, dst) in enumerate(parts)]
    for load in loads:
        load.start()
    greet(torus_peers(me))
    for load in loads:
        load.wait()
    mine, other = me.xl, 1 - me.xl

    def m(i):
        return mod[i]

    sends = Sends()
    yz, zy = ("y", "z"), ("z", "y")
    plan = [
        (wa, 0, [(yz, (0, 384, 256)), (zy, (640, 256, 256))]), (wa, 1, [(zy, (0, 384, 256)), (yz, (640, 256, 256))]),
        (wa, 0, [(yz, (1152, 256, 128))]), (wa, 1, [(zy, (1152, 256, 128))]),
        (wf, 0, [(yz, (0, 384, 384)), (zy, (768, 384, 384))]), (wf, 1, [(yz, (0, 384, 384)), (zy, (768, 384, 384))]),
    ]
    pieces = []
    count = 0
    for ref, side, halves in plan:
        pieces.append([])
        for axes, span in halves:
            xb = 1 - me.xh if side else me.xh
            pieces[-1].append(Gather(me, ref, axes, span, xb, gs.at[count], gr.at[count], sends))
            count += 1

    def gather_event(k, what):
        if what == "first" and k % 2:
            for i, ref, cols in crossed[k]:
                arrive(ref.at[me.z, me.y, 1 - me.xh, :, cols], xr.at[i], me.across())
        for half in pieces[k]:
            getattr(half, what)()

    crossed = {1: [(0, wa, pl.ds(0, 3 * QKV))], 3: [(1, wa, pl.ds(3 * QKV, QKV))], 5: [(2, wf, LEFT), (3, wf, RIGHT)]}

    def cross(group):
        if group < 2:
            ref = home_a.at[:, crossed[2 * group + 1][0][2]]
            sends.start(ref, ref, xs.at[group], xr.at[group], me.across())
        else:
            for i, ref, cols in ((2, wi, LEFT), (3, wb, RIGHT)):
                sends.start(ref.at[:, pl.ds(other_f, HALF)], home_f.at[:, cols], xs.at[i], xr.at[i], me.across())

    def ag(*steps):
        names = {
            "f": "first", "s": "second", "l": "last", "o": "own", "i": "sides", "e": "end", "r": "relay", "c": "close"
        }
        for step in steps:
            gather_event(int(step[1]), names[step[0]])

    scatters = []
    for k in range(10):
        side = k % 2
        xb = me.xh if side else 1 - me.xh
        if k < 4:
            span, axes = ((HALF, 384, 384), (0, 384, 384))[k // 2], (yz, zy, zy, yz)[k]
        else:
            span, axes = ((3 * QKV, 256, 128), (0, 384, 384), (2 * QKV, 256, 128))[k // 2 - 2], (zy, yz, zy, yz, yz, zy)[k - 4]
        kind = Scatter if k < 4 else FineScatter
        if span[1] == 384:
            n = k if k < 4 else k - 2
            bufs = ((r1.at[n], r2.at[n]), (p1.at[n], p2.at[n]))
        else:
            n = k - 4 if k < 6 else k - 6
            bufs = ((r3.at[n], r4.at[n]), (p3.at[n], p4.at[n]))
        scatters.append(kind(me, gf if k < 4 else ga, axes, span, xb, bufs, ss.at[k], rs.at[k], sends))

    def finish(k):
        scatter = scatters[k]
        _, total = scatter.total(1)
        cols = scatter.cols["all"]
        group = k // 2
        if k < 4:
            out = (ob, oi)[group].at[:, pl.ds(mine_f, HALF)]
            if k % 2:
                out[...] = total
            else:
                partf[group] = pack(total)
                sends.start(partf.at[group], xf.at[group], ys.at[group], yr.at[group], me.across())
        elif k % 2 == 0:
            part[:, cols] = pack(total)
            sends.start(part.at[:, cols], xbuf.at[:, cols], ys.at[group], yr.at[group], me.across())
        else:
            arrive(xbuf.at[:, cols], yr.at[group], me.across())
            total = total + wider(xbuf[:, cols])
            for i in range(cols.size // QKV):
                value = total[:, i * QKV : (i + 1) * QKV]
                head = cols.start // QKV + i
                if head == HEADS:
                    oo[...] = value
                else:
                    for j in range(3):
                        oq[j, :, pl.ds(head * HEAD_DIM, HEAD_DIM)] = value[:, j * HEAD_DIM : (j + 1) * HEAD_DIM]

    def rsc(*steps):
        names = {
            "f": ("both", 0), "r": ("relay", 0), "d": ("fold",), "g": ("both", 1), "s": ("relay", 1),
            "F": ("far0",), "N": ("rest0",), "R": ("relay0",), "D": ("fold0",), "G": ("far", 1), "H": ("rest", 1),
        }
        spots = {"": (2, 1, -1, 0), "a": (2,), "b": (1, -1), "c": (0,), "ab": (2, 1, -1), "bc": (1, -1, 0)}
        for step in steps:
            scatter_event(step, int(step[1]), names, spots)

    def scatter_event(step, k, names, spots):
        if step[0] == "e":
            finish(k)
        else:
            name, *args = names[step[0]]
            if step[0] in "FNRD":
                args = spots[step[2:]]
            getattr(scatters[k], name)(*args)

    def rows_of(ref, side, cols=slice(None)):
        value = ref[pl.ds(side * 2, 2), :, cols]
        return value.reshape(2 * OWN, value.shape[-1])

    def forward(src, side, w, col, width, emit):
        weight = w[:, :, :, :, pl.ds(col, width)].reshape(WIDTH, width)
        emit(contract(rows_of(src, side), weight, 1, 0).reshape(2, OWN, width))

    def backward(src, side, w, col, width, out):
        @pl.loop(0, 2)
        def _(j):
            weight = w[pl.ds(j * 2, 2), :, :, :, pl.ds(col, width)].reshape(HALF, width)
            at = pl.multiple_of(j * HALF, 128)
            value = contract(rows_of(src, side), weight, 1, 1)
            out[pl.ds(side * 2, 2), :, pl.ds(at, HALF)] = pack(value).reshape(2, OWN, HALF)

    def gradient(left, right, g, col, width):
        count = left.shape[0] * OWN

        @pl.loop(0, 4)
        def _(j):
            rows = left[:, :, pl.ds(pl.multiple_of(j * 384, 128), 384)].reshape(count, 384)
            value = contract(rows, right[...].reshape(count, width), 0, 0) * grad_scale
            g[j, :, :, :, pl.ds(col, width)] = pack(value).reshape(4, 2, ROWS, width)

    every = (0, OWN)
    x_a1 = SeqGather(me, a1, every, es.at[0], er.at[0], sends)
    x_das = [SeqGather(me, da, rows, es.at[1 + i], er.at[1 + i], sends) for i, rows in enumerate(CHUNKS)]
    a2_sends = Sends()
    x_a2s = [RingGather(me, a2, rows, es.at[3 + i], er.at[3 + i], a2_sends) for i, rows in enumerate(CHUNKS)]
    x_dm = RingGather(me, dm, every, es.at[5], er.at[5], sends)
    y_att = SeqScatter(me, pf.at[pl.ds(0, 4)], swap, own_sum, theirs, es.at[6], er.at[6])
    y_first = SeqScatter(me, a2.at[pl.ds(0, 4)], swap, own_sum, theirs, es.at[7], er.at[7])
    y_backs = [
        RingScatter(me, pf, swapf.at[0], away.at[0], near.at[0], rows, es.at[8 + i], er.at[8 + i])
        for i, rows in enumerate(CHUNKS)
    ]
    y_back = y_backs[0]
    y_ffn = RingScatter(me, pf, swapf.at[1], away.at[1], near.at[1], every, es.at[10], er.at[10])

    def all_of(objects, *names):
        for name in names:
            for item in objects:
                getattr(item, name)()

    def share(y, src, col, width):
        backward(src, other, wa, col, width, y.part)
        y.give(0)
        backward(src, mine, wa, col, width, y.part)
        y.give(1)
        y.cross()

    def first_norm(r):
        n1, _ = normalize(wider(tok[r]))
        a1[me.s, r] = pack(n1 * (1.0 + m(1)) + m(0))

    def gate(r):
        dm[me.n, r] = pack(m(5) * wider(og[r]))

    def put(dst, side):
        def emit(value):
            dst[pl.ds(side * 2, 2)] = pack(value)
        return emit

    def head_cols(place, head):
        return pl.ds(pl.multiple_of(head * QKV + place * HEAD_DIM, HEAD_DIM), HEAD_DIM)

    def own_cols(head):
        return pl.ds(pl.multiple_of(head * HEAD_DIM, HEAD_DIM), HEAD_DIM)

    def head_rows(ref, cols):
        return ref[:, :, cols].reshape(4 * OWN, HEAD_DIM)

    def attend(head):
        q, k, v = (head_rows(packed, head_cols(i, head)) for i in range(3))
        probs = softmax_rows(q, k, factor)
        att[:, :, own_cols(head)] = pack(contract(pack(probs), v, 1, 0)).reshape(4, OWN, HEAD_DIM)

    def attend_back(head):
        q, k, v = (head_rows(packed, head_cols(i, head)) for i in range(3))
        up = head_rows(datt, own_cols(head))
        probs = softmax_rows(q, k, factor)
        dprobs = contract(up, v, 1, 1)
        dscores = pack(probs * (dprobs - jnp.sum(probs * dprobs, axis=-1, keepdims=True)) * factor)
        parts = (contract(dscores, k, 1, 0), contract(dscores, q, 0, 0), contract(pack(probs), up, 0, 0))
        for i, value in enumerate(parts):
            packed[:, :, head_cols(i, head)] = pack(value).reshape(4, OWN, HEAD_DIM)

    def heads(body, low=0, high=HEADS):
        pl.loop(low, high)(body)

    def second_norm(r):
        mid = wider(tok[r]) + m(2) * y_att.rows(r)
        middle[r] = mid
        n2, _ = normalize(mid)
        a2[me.n, r] = pack(n2 * (1.0 + m(4)) + m(3))

    def hidden(chip):
        def emit(u):
            t = jnp.tanh(GELU_A * (u + GELU_B * (u * u * u)))
            at = pl.ds(chip * 2, 2)
            act[at] = pack(0.5 * u * (1.0 + t))
            slope = 0.5 * (1.0 + t) + (0.5 * GELU_A) * u * (1.0 - t * t) * (1.0 + (3.0 * GELU_B) * (u * u))
            du[at] = pack(slope * dg[at])
        forward(a2, chip, wf, 0, HALF, emit)

    def hidden_back(chip):
        def emit(value):
            dg[pl.ds(chip * 2, 2)] = value
        forward(dm, chip, wf, HALF, HALF, emit)

    def middle_back(r):
        n2, rstd = normalize(middle[r])
        up = wider(og[r]) + norm_back(n2, rstd, y_back.rows(r) * (1.0 + m(4)))
        grad[r] = up
        da[me.s, r] = pack(m(2) * up)

    def last_out(r):
        final[r] = pack(middle[r] + m(5) * y_ffn.rows(r))

    def first_back(r):
        n1, rstd = normalize(wider(tok[r]))
        grad[r] = grad[r] + norm_back(n1, rstd, y_first.rows(r) * (1.0 + m(1)))

    def sides(i):
        hidden(me.chip_at(2 * i - 1))

    def backs(i):
        hidden_back(me.chip_at(i))

    def norm_and_send(i):
        y_att.wait(i)
        by_rows(second_norm, CHUNKS[i])
        x_a2s[i].start()

    def back_and_send(i):
        y_backs[i].wait()
        by_rows(middle_back, CHUNKS[i])
        x_das[i].start()

    def norm_and_send(i):
        y_att.wait(i)
        by_rows(second_norm, CHUNKS[i])
        x_a2s[i].start()

    def back_and_send(i):
        y_backs[i].wait()
        by_rows(middle_back, CHUNKS[i])
        x_das[i].start()

    cross(0)
    ag("f0", "o0", "f4", "o4")
    by_rows(first_norm)
    x_a1.start()
    cross(1)
    cross(2)
    by_rows(gate)
    x_dm.start()
    ag("s0", "i0", "f1", "o1", "l0", "e0", "f2", "s1", "i1", "l1", "e1", "r0", "s2", "f3")
    x_a1.relay()
    ag("o2", "i2", "r1", "l2", "e2", "o3", "s3", "i3")
    x_dm.relay()
    ag("c0")
    x_a1.near()
    x_a1.far()
    ag("c1")
    forward(a1, mine, wa, 0, 3 * QKV, put(packed, mine))
    ag("l3", "e3")
    forward(a1, other, wa, 0, 3 * QKV, put(packed, other))
    ag("r2", "s4", "i4")
    heads(attend, 0, 1)
    ag("r3", "l4", "e4", "f5", "o5")
    heads(attend, 1, 3)
    ag("c2", "c3")
    share(y_att, att, 3 * QKV, QKV)
    x_dm.spread()
    ag("s5", "i5", "l5", "e5")
    x_dm.last()
    ag("r4")
    norm_and_send(0)
    ag("r5")
    norm_and_send(1)
    x_a2s[0].relay()
    y_att.drain()
    x_dm.own()
    x_dm.sides()
    x_dm.far()
    all_of(x_a2s, "own")
    ag("c4", "c5")
    pl.loop(0, 2)(backs)
    x_a2s[1].relay()
    hidden(me.x)
    all_of(x_a2s, "spread")
    pl.loop(2, 4)(backs)
    all_of(x_a2s, "sides")
    pl.loop(0, 2)(sides)
    all_of(x_a2s, "last")

    backward(du, me.chip_at(1), wf, 0, HALF, pf)
    y_back.give(1)
    all_of(x_a2s, "far")
    hidden(me.chip_at(2))
    backward(du, me.chip_at(2), wf, 0, HALF, pf)
    y_back.give(0)
    backward(du, me.chip_at(-1), wf, 0, HALF, pf)
    y_back.give(2)
    all_of(y_backs, "out")
    backward(du, me.chip_at(0), wf, 0, HALF, pf)
    y_back.give(3)
    all_of(y_backs, "rest")
    gradient(dm, act, gf, HALF, HALF)
    rsc("f0", "f1")
    all_of(y_backs, "relay")
    gradient(a2, du, gf, 0, HALF)
    rsc("r0", "r1", "f2", "f3")
    back_and_send(0)
    back_and_send(1)
    all_of(y_backs, "drain")
    all_of(x_a2s, "drain")
    backward(act, me.chip_at(2), wf, HALF, HALF, pf)
    y_ffn.give(0)
    backward(act, me.chip_at(1), wf, HALF, HALF, pf)
    y_ffn.give(1)
    rsc("d0", "g0", "d1", "g1")
    x_das[0].relay()
    backward(act, me.chip_at(-1), wf, HALF, HALF, pf)
    y_ffn.give(2)
    rsc("r2", "r3")
    backward(act, me.chip_at(0), wf, HALF, HALF, pf)
    y_ffn.give(3)
    x_das[1].relay()
    all_of(x_das, "near")
    forward(da, mine, wa, 3 * QKV, QKV, put(datt, mine))
    all_of(x_das, "far")
    forward(da, other, wa, 3 * QKV, QKV, put(datt, other))
    y_ffn.out()
    gradient(da, att, ga, 3 * QKV, QKV)
    rsc("F4", "F5", "N4", "N5")
    heads(attend_back, 0, 2)
    y_ffn.rest()
    rsc("d2", "g2", "d3", "g3", "s0", "s1")
    gradient(a1, packed.at[:, :, pl.ds(0, HALF)], ga, 0, HALF)
    rsc("F6", "F7", "N6", "N7", "R4", "R5")
    heads(attend_back, 2, 3)
    gradient(a1, packed.at[:, :, pl.ds(HALF, QKV)], ga, HALF, QKV)
    rsc("F8", "F9", "N8", "N9", "s2", "s3", "R6a", "R7a", "R6b", "R7b", "R6c", "R7c", "e0")
    y_ffn.relay()
    share(y_first, packed, 0, 3 * QKV)
    rsc("R8a", "R9a", "R8b", "R9b", "R8c", "R9c", "D4", "G4", "H4", "D5", "G5", "H5")
    rsc("D6a", "G6", "D7a", "G7", "D6b", "H6", "D7b", "H7", "D6c", "D7c", "e2")
    rsc("D8a", "G8", "D9a", "G9", "D8b", "H8", "D9b", "H9", "D8c", "D9c", "s4", "s5", "s6", "s7", "s8", "s9")
    rsc("e4", "e6", "e8")
    y_ffn.wait()
    by_rows(last_out)
    y_first.wait(0)
    y_first.wait(1)
    by_rows(first_back)
    rsc("e1", "e3")
    for group, out in enumerate((ob, oi)):
        arrive(xf.at[group], yr.at[group], me.across())
        out[:, pl.ds(other_f, HALF)] = wider(xf[group])
    rsc("e5", "e7", "e9")
    for piece in pieces:
        for half in piece:
            half.drain()
    for scatter in scatters:
        scatter.drain()
    all_of([x_a1, x_dm, y_first, y_ffn] + x_das, "drain")
    sends.close()


def copy_kernel(*refs):
    n = len(refs) // 2
    sem = refs[-1]
    copies = [pltpu.make_async_copy(refs[i], refs[n + i], sem.at[i]) for i in range(n)]
    for copy in copies:
        copy.start()
    for copy in copies:
        copy.wait()


def copy_out(arrays):
    return pl.pallas_call(
        copy_kernel,
        out_shape=[jax.ShapeDtypeStruct(a.shape, a.dtype) for a in arrays],
        in_specs=[VM] * len(arrays),
        out_specs=[ANY] * len(arrays),
        scratch_shapes=[DMA((len(arrays),))],
    )(*arrays)


def local(tokens, modulation, w_qkv, w_out, w_in, w_back, out_grad):
    grad_scale = 1.0 / math.sqrt(OWN * lax.axis_size("sp") * lax.axis_size("fsdp"))
    factor = TEMPER / math.sqrt(HEAD_DIM)

    def shape(dims, dtype=BF16):
        return jax.ShapeDtypeStruct(dims, dtype)

    def vm(*dims, dtype=BF16):
        return pltpu.VMEM(dims, dtype)

    seq, ring = (4, OWN, WIDTH), (8, OWN, WIDTH)
    results = pl.pallas_call(
        functools.partial(step_kernel, grad_scale, factor),
        out_shape=(
            shape((OWN, WIDTH)), shape((OWN, WIDTH), F32), shape((3, ROWS, QKV), F32),
            shape((ROWS, QKV), F32), shape((ROWS, GROUP), F32), shape((ROWS, GROUP), F32),
        ),
        in_specs=[VM, VM, ANY, ANY, ANY, ANY, VM],
        out_specs=(VM,) * 6,
        scratch_shapes=[
            vm(4, 4, 2, ROWS, GROUP), vm(4, 4, 2, ROWS, GROUP), vm(4, 4, 2, ROWS, GROUP), vm(4, 4, 2, ROWS, GROUP),
            vm(6, 2, 4, ROWS, QUART), vm(6, 2, 4, ROWS, HALF), vm(6, 2, ROWS, QUART), vm(6, 2, ROWS, HALF),
            vm(4, 2, 4, ROWS, 256), vm(4, 2, 4, ROWS, 384), vm(4, 2, ROWS, 256), vm(4, 2, ROWS, 384),
            vm(ROWS, GROUP), vm(ROWS, GROUP), vm(2, ROWS, HALF), vm(2, ROWS, HALF),
            vm(*seq), vm(*ring), vm(*ring), vm(*seq),
            vm(4, OWN, 3 * QKV), vm(4, OWN, QKV), vm(4, OWN, QKV),
            vm(8, OWN, HALF), vm(8, OWN, HALF, dtype=F32), vm(8, OWN, HALF),
            vm(*ring), vm(2, OWN, WIDTH), vm(OWN, WIDTH), vm(OWN, WIDTH),
            vm(2, 4, OWN, WIDTH), vm(2, 2, OWN, HALF), vm(2, 2, OWN, WIDTH), vm(OWN, WIDTH, dtype=F32),
            DMA((10, 2)), DMA((10, 6)), DMA((10, 6)), DMA((10, 12)),
            DMA((4,)), DMA((4,)), DMA((5,)), DMA((5,)), DMA((11, 2)), DMA((11, 7)), DMA((12,)),
        ],
        compiler_params=pltpu.CompilerParams(
            collective_id=0, has_side_effects=True, vmem_limit_bytes=67043328
        ),
    )(
        tokens[0], modulation.transpose(2, 0, 1, 3)[:, 0],
        w_qkv[0].transpose(1, 0, 2), w_out[0].T, w_in[0], w_back[0].T, out_grad[0],
    )
    final, grad, oq, oo, oi, ob = copy_out(results)
    return (
        final[None], grad[None], oq.transpose(1, 0, 2)[None], oo.T[None], oi[None], ob.T[None],
    )


def solution(mesh):
    weights = (
        P(None, "fsdp", None, "sp"),
        P(None, "sp", "fsdp"),
        P(None, "fsdp", "sp"),
        P(None, "sp", "fsdp"),
    )
    rows = P("fsdp", "sp", None)
    return jax.shard_map(
        local,
        mesh=mesh,
        in_specs=(rows, P("fsdp", None, None, None), *weights, rows),
        out_specs=(rows, rows, *weights),
        check_vma=False,
    )
```

```python
import functools
import math

import jax
import jax.numpy as jnp
from jax import lax
from jax.experimental import pallas as pl
from jax.experimental.pallas import tpu as pltpu
from jax.sharding import PartitionSpec as P

HEAD_DIM = 128
LN_EPS = 1e-06
TEMPER = 2.5
F32 = jnp.float32
BF16 = jnp.bfloat16
MESH = pl.DeviceIdType.MESH
GROUP = 1536
HALF = GROUP // 2
QUART = GROUP // 4
ROWS = 48


def rem(a, n):
    return lax.rem(a, n)


class Place:
    def __init__(self):
        f = lax.axis_index("fsdp")
        s = lax.axis_index("sp")
        self.z, self.y, self.xh = lax.div(f, 8), rem(lax.div(f, 2), 4), rem(f, 2)
        self.xl, self.c = lax.div(s, 2), rem(s, 2)
        self.s = s
        self.x = self.xh * 2 + self.xl
        self.n = self.x * 2 + self.c

    def dev(self, **kw):
        v = {k: kw.get(k, getattr(self, k)) for k in ("z", "y", "xh", "xl", "c")}
        return (v["z"] * 8 + v["y"] * 2 + v["xh"], v["xl"] * 2 + v["c"])

    def ring(self, axis, step):
        return rem(getattr(self, axis) + step + 4, 4)

    def near(self, axis, step):
        return self.dev(**{axis: self.ring(axis, step)})

    def along(self, step):
        x = rem(self.x + step + 4, 4)
        return self.dev(xh=lax.div(x, 2), xl=rem(x, 2))

    def chip_at(self, step):
        return rem(self.x + step + 4, 4)

    def across(self):
        return self.dev(xh=1 - self.xh)

    def chip(self):
        return self.dev(xl=1 - self.xl)

    def core(self):
        return self.dev(c=1 - self.c)


def greet(devices):
    barrier = pltpu.get_barrier_semaphore()
    for d in devices:
        pl.semaphore_signal(barrier, inc=1, device_id=d, device_id_type=MESH)
    pl.semaphore_wait(barrier, len(devices))


def torus_peers(me):
    return [me.near(a, s) for a in ("z", "y") for s in (1, -1)] + [me.across(), me.along(1), me.along(-1), me.core()]


class Sends:
    def __init__(self):
        self.open = []

    def start(self, src, dst, ssem, rsem, dev):
        copy = pltpu.make_async_remote_copy(
            src_ref=src, dst_ref=dst, send_sem=ssem, recv_sem=rsem, device_id=dev, device_id_type=MESH
        )
        copy.start()
        self.open.append(copy)

    def close(self):
        for copy in self.open:
            copy.wait_send()
        self.open = []


def launch(src, dst, ssem, rsem, dev):
    pltpu.make_async_remote_copy(
        src_ref=src, dst_ref=dst, send_sem=ssem, recv_sem=rsem, device_id=dev, device_id_type=MESH
    ).start()


def drained(ref, ssem, dev):
    pltpu.make_async_remote_copy(
        src_ref=ref, dst_ref=ref, send_sem=ssem, recv_sem=ssem, device_id=dev, device_id_type=MESH
    ).wait_send()


def arrive(ref, rsem, dev):
    pltpu.make_async_remote_copy(
        src_ref=ref, dst_ref=ref, send_sem=rsem, recv_sem=rsem, device_id=dev, device_id_type=MESH
    ).wait_recv()


def columns(start, low, high):
    return {"all": pl.ds(start, low + high), "lo": pl.ds(start, low), "hi": pl.ds(start + low, high)}


class Gather:
    def __init__(self, me, w, axes, span, xb, ssem, rsem, sends):
        self.me, self.w, self.axes, self.xb = me, w, axes, xb
        self.ssem, self.rsem, self.sends = ssem, rsem, sends
        self.cols = columns(*span)

    def part(self, p, q, which):
        first, second = self.axes
        at = {first: slice(None) if p is None else self.me.ring(first, p), second: self.me.ring(second, q)}
        return self.w.at[at["z"], at["y"], self.xb, :, self.cols[which]]

    def go(self, level, to, p, q, which, i):
        ref = self.part(p, q, which)
        launch(ref, ref, self.ssem.at[level], self.rsem.at[i], self.me.near(self.axes[level], to))

    def got(self, p, q, which, i):
        arrive(self.part(p, q, which), self.rsem.at[i], self.me.near(self.axes[0], 1))

    def first(self):
        self.go(0, 1, 0, 0, "all", 0)
        self.go(0, -1, 0, 0, "all", 1)

    def second(self):
        self.got(-1, 0, "all", 0)
        self.go(0, 1, -1, 0, "lo", 2)
        self.got(1, 0, "all", 1)
        self.go(0, -1, 1, 0, "hi", 2)

    def last(self):
        self.got(2, 0, "all", 2)

    def out(self, *ps):
        for p in ps:
            self.go(1, 1, p, 0, "all", 3)
            self.go(1, -1, p, 0, "all", 4)

    def own(self):
        self.out(0)

    def sides(self):
        self.out(-1, 1)

    def end(self):
        self.out(2)

    def relay(self):
        self.got(None, -1, "all", 3)
        self.go(1, 1, None, -1, "lo", 5)
        self.got(None, 1, "all", 4)
        self.go(1, -1, None, 1, "hi", 5)

    def close(self):
        self.got(None, 2, "all", 5)

    def drain(self):
        cols = self.cols["all"]
        drained(self.w.at[0, pl.ds(0, 3), 0, :, cols], self.ssem.at[0], self.me.near("z", 1))
        drained(self.w.at[pl.ds(0, 3), pl.ds(0, 4), 0, :, cols], self.ssem.at[1], self.me.near("z", 1))


def wider(ref_value):
    return ref_value.astype(F32)


def pack(total):
    return total.astype(BF16)


class Scatter:
    def __init__(self, me, g, axes, span, xb, bufs, ssem, rsem, sends):
        self.me, self.g, self.axes, self.xb = me, g, axes, xb
        self.bufs, self.ssem, self.rsem, self.sends = bufs, ssem, rsem, sends
        self.cols = columns(*span)
        self.inner = columns(0, *span[1:])

    def spot(self, level, step, which):
        axis = self.axes[level]
        at = {"z": self.me.z, "y": self.me.y}
        at[axis] = self.me.ring(axis, step)
        if level == 0:
            at[self.axes[1]] = slice(None)
        return (at["z"], at["y"], self.xb, slice(None), self.cols[which])

    def way(self, level, i, which):
        if level == 0:
            return self.bufs[0][0].at[i, :, :, columns(0, *self.sizes(which))["lo"]]
        return self.bufs[1][0].at[i, :, columns(0, *self.sizes(which))["lo"]]

    def sizes(self, which):
        return self.inner[which].size, 0

    def send(self, level, step, which, dst, i, to):
        launch(
            self.g.at[self.spot(level, step, which)], dst, self.ssem.at[level], self.rsem.at[level * 2 + i],
            self.me.near(self.axes[level], to),
        )

    def near(self, level, i, which):
        cols = self.inner[which]
        if level == 0:
            return self.bufs[level][1].at[i, :, :, cols]
        return self.bufs[level][1].at[i, :, cols]

    def far(self, level):
        for to, which, i in ((1, "lo", 0), (-1, "hi", 1)):
            self.send(level, 2, which, self.way(level, i, which), 0, to)

    def rest(self, level):
        for to, which, i in ((1, "hi", 0), (-1, "lo", 1)):
            self.send(level, to, which, self.near(level, i, which), 1, to)

    def both(self, level):
        self.far(level)
        self.rest(level)

    def relay(self, level):
        arrive(self.g.at[self.spot(level, 0, "all")], self.rsem.at[level * 2], self.me.near(self.axes[level], 1))
        for to, which, i in ((1, "lo", 0), (-1, "hi", 1)):
            buf = self.way(level, i, which)
            spot = self.spot(level, to, which)
            self.g[spot] = (wider(self.g[spot]) + wider(buf[...])).astype(BF16)
        for to, which, i in ((1, "lo", 0), (-1, "hi", 1)):
            self.send(level, to, which, self.near(level, i, which), 1, to)

    def total(self, level):
        near = self.bufs[level][1]
        arrive(near, self.rsem.at[level * 2 + 1], self.me.near(self.axes[level], 1))
        spot = self.spot(level, 0, "all")
        return spot, wider(self.g[spot]) + wider(near[0]) + wider(near[1])

    def drain_at(self, level):
        places = pl.ds(0, 3) if level == 0 else 0
        wide = pl.ds(0, 4) if level == 0 else pl.ds(0, 3)
        drained(self.g.at[places, wide, 0, :, self.cols["all"]], self.ssem.at[level], self.me.near("z", 1))

    def drain(self):
        self.drain_at(0)
        self.drain_at(1)

    def fold(self):
        spot, total = self.total(0)
        self.g[spot] = total.astype(BF16)


class FineScatter(Scatter):
    slots = {2: 0, 1: 1, -1: 2, 0: 3}

    def place(self, q, p, which):
        at = {self.axes[0]: self.me.ring(self.axes[0], q), self.axes[1]: self.me.ring(self.axes[1], p)}
        return (at["z"], at["y"], self.xb, slice(None), self.cols[which])

    def give(self, q, p, which, dst, i, to):
        slot = self.slots[p]
        launch(
            self.g.at[self.place(q, p, which)], dst, self.ssem.at[2 + slot], self.rsem.at[4 + slot * 2 + i],
            self.me.near(self.axes[0], to),
        )

    def take(self, ref, p, i):
        arrive(ref, self.rsem.at[4 + self.slots[p] * 2 + i], self.me.near(self.axes[0], 1))

    def side(self, i, p, which):
        return self.bufs[0][1].at[i, self.slots[p], :, self.inner[which]]

    def step(self, i, p, which):
        return self.bufs[0][0].at[i, self.slots[p], :, pl.ds(0, self.inner[which].size)]

    def far0(self, *ps):
        for p in ps:
            for to, which, i in ((1, "lo", 0), (-1, "hi", 1)):
                self.give(2, p, which, self.step(i, p, which), 0, to)

    def rest0(self, *ps):
        for p in ps:
            for to, which, i in ((1, "hi", 0), (-1, "lo", 1)):
                self.give(to, p, which, self.side(i, p, which), 1, to)

    def relay0(self, *ps):
        for p in ps:
            self.take(self.g.at[self.place(0, p, "all")], p, 0)
            for to, which, i in ((1, "lo", 0), (-1, "hi", 1)):
                spot = self.place(to, p, which)
                self.g[spot] = pack(wider(self.g[spot]) + wider(self.step(i, p, which)[...]))
            for to, which, i in ((1, "lo", 0), (-1, "hi", 1)):
                self.give(to, p, which, self.side(i, p, which), 1, to)

    def fold0(self, *ps):
        for p in ps:
            near = self.bufs[0][1]
            self.take(near.at[:, self.slots[p]], p, 1)
            spot = self.place(0, p, "all")
            total = wider(self.g[spot]) + wider(near[0, self.slots[p]]) + wider(near[1, self.slots[p]])
            self.g[spot] = pack(total)

    def drain(self):
        self.drain_at(1)
        for slot in range(4):
            ref = self.g.at[0, pl.ds(0, 3), 0, :, self.cols["all"]]
            drained(ref, self.ssem.at[2 + slot], self.me.near("z", 1))


DMA = pltpu.SemaphoreType.DMA
VM = pl.BlockSpec(memory_space=pltpu.VMEM)
ANY = pl.BlockSpec(memory_space=pl.ANY)
OWN = 128
WIDTH = 1536
HEADS = 3
QKV = HEADS * HEAD_DIM
GELU_A = math.sqrt(2.0 / math.pi)
GELU_B = 0.044715


CHUNKS = ((0, OWN // 2), (OWN // 2, OWN // 2))


class SeqGather:
    def __init__(self, me, buf, rows, ssem, rsem, sends):
        self.me, self.buf, self.rows, self.ssem, self.rsem, self.sends = me, buf, pl.ds(*rows), ssem, rsem, sends

    def push(self, block, i, dev):
        ref = self.buf.at[block, self.rows]
        launch(ref, ref, self.ssem.at[0], self.rsem.at[i], dev)

    def drain(self):
        drained(self.buf.at[pl.ds(0, 3), self.rows], self.ssem.at[0], self.me.core())

    def start(self):
        self.push(self.me.s, 0, self.me.chip())
        self.push(self.me.s, 1, self.me.core())

    def relay(self):
        other = (1 - self.me.xl) * 2 + self.me.c
        arrive(self.buf.at[other, self.rows], self.rsem.at[0], self.me.chip())
        self.push(other, 2, self.me.core())

    def near(self):
        arrive(self.buf.at[self.me.xl * 2 + 1 - self.me.c, self.rows], self.rsem.at[1], self.me.core())

    def far(self):
        arrive(self.buf.at[(1 - self.me.xl) * 2 + 1 - self.me.c, self.rows], self.rsem.at[2], self.me.core())


class SeqScatter:
    def __init__(self, me, part, swap, mine, theirs, ssem, rsem):
        self.me, self.part, self.swap, self.mine, self.theirs = me, part, swap, mine, theirs
        self.ssem, self.rsem = ssem, rsem

    def drain(self):
        drained(self.part.at[pl.ds(0, 3)], self.ssem.at[0], self.me.core())

    def give(self, i):
        xl = self.me.xl if i else 1 - self.me.xl
        launch(self.part.at[xl * 2 + 1 - self.me.c], self.swap.at[i], self.ssem.at[0], self.rsem.at[i], self.me.core())

    def cross(self):
        arrive(self.swap.at[0], self.rsem.at[0], self.me.core())

        def merge(r):
            self.mine[r] = pack(wider(self.part[(1 - self.me.xl) * 2 + self.me.c, r]) + wider(self.swap[0, r]))

        for i, rows in enumerate(CHUNKS):
            by_rows(merge, rows)
            r = pl.ds(*rows)
            launch(self.mine.at[r], self.theirs.at[r], self.ssem.at[0], self.rsem.at[2 + i], self.me.chip())

    def wait(self, i):
        if i == 0:
            arrive(self.swap.at[1], self.rsem.at[1], self.me.core())
        arrive(self.theirs.at[pl.ds(*CHUNKS[i])], self.rsem.at[2 + i], self.me.chip())

    def rows(self, r):
        return wider(self.part[self.me.s, r]) + wider(self.swap[1, r]) + wider(self.theirs[r])


LEFT, RIGHT = pl.ds(0, HALF), pl.ds(HALF, HALF)


class RingGather:
    def __init__(self, me, buf, rows, ssem, rsem, sends):
        self.me, self.buf, self.rows, self.ssem, self.rsem, self.sends = me, buf, pl.ds(*rows), ssem, rsem, sends

    def at(self, step, mine=True, cols=pl.ds(0, WIDTH)):
        return self.buf.at[self.me.chip_at(step) * 2 + (self.me.c if mine else 1 - self.me.c), self.rows, cols]

    def push(self, ref, i, dev):
        launch(ref, ref, self.ssem.at[0], self.rsem.at[i], dev)

    def drain(self):
        drained(self.buf.at[pl.ds(0, 7), self.rows], self.ssem.at[0], self.me.core())

    def start(self):
        for cols, step, i in ((LEFT, 1, 0), (RIGHT, -1, 1), (RIGHT, 1, 2), (LEFT, -1, 2)):
            self.push(self.at(0, cols=cols), i, self.me.along(step))
        self.push(self.at(0), 3, self.me.core())

    def relay(self):
        for step, cols, i in ((-1, LEFT, 0), (1, RIGHT, 1)):
            arrive(self.at(step, cols=cols), self.rsem.at[i], self.me.core())
            self.push(self.at(step, cols=cols), 4, self.me.along(-step))

    def spread(self):
        arrive(self.at(1), self.rsem.at[2], self.me.core())
        for step in (-1, 1):
            self.push(self.at(step), 5, self.me.core())

    def last(self):
        arrive(self.at(2), self.rsem.at[4], self.me.core())
        self.push(self.at(2), 6, self.me.core())

    def own(self):
        arrive(self.at(0, False), self.rsem.at[3], self.me.core())

    def sides(self):
        arrive(self.buf.at[pl.ds(0, 2), self.rows], self.rsem.at[5], self.me.core())

    def far(self):
        arrive(self.at(2, False), self.rsem.at[6], self.me.core())


class RingScatter:
    order = (2, 1, -1, 0)

    def __init__(self, me, part, swap, away, near, rows, ssem, rsem):
        self.me, self.part, self.swap, self.away, self.near = me, part, swap, away, near
        self.span, self.ssem, self.rsem = rows, ssem, rsem
        self.r = pl.ds(*rows)

    def block(self, step):
        return self.me.chip_at(step) * 2 + self.me.c

    def give(self, j):
        src = self.part.at[self.me.chip_at(self.order[j]) * 2 + 1 - self.me.c]
        launch(src, self.swap.at[j], self.ssem.at[0], self.rsem.at[j], self.me.core())

    def drain(self):
        if self.span[0] == 0:
            drained(self.part.at[pl.ds(0, 4)], self.ssem.at[0], self.me.core())
        drained(self.part.at[pl.ds(0, 3), self.r], self.ssem.at[1], self.me.core())

    def swapped(self, j):
        if self.span[0] == 0:
            arrive(self.swap.at[j], self.rsem.at[j], self.me.core())

    def push(self, step, cols, dst, i, to):
        launch(self.part.at[self.block(step), self.r, cols], dst, self.ssem.at[1], self.rsem.at[i], self.me.along(to))

    def out(self):
        self.swapped(0)
        block = self.block(2)

        def merge(r):
            self.part[block, r] = pack(wider(self.part[block, r]) + wider(self.swap[0, r]))

        by_rows(merge, self.span)
        self.push(2, LEFT, self.away.at[0, self.r], 4, 1)
        self.push(2, RIGHT, self.away.at[1, self.r], 4, -1)

    def rest(self):
        for step, j, i, cols in ((1, 1, 0, RIGHT), (-1, 2, 1, LEFT)):
            self.swapped(j)
            block = self.block(step)

            def merge(r):
                self.part[block, r, cols] = pack(wider(self.part[block, r, cols]) + wider(self.swap[j, r, cols]))

            by_rows(merge, self.span)
            self.push(step, cols, self.near.at[i, self.r, cols], 5, step)

    def relay(self):
        arrive(self.away.at[:, self.r], self.rsem.at[4], self.me.core())
        for step, j, i, cols in ((1, 1, 0, LEFT), (-1, 2, 1, RIGHT)):
            block = self.block(step)

            def merge(r):
                both = wider(self.part[block, r, cols]) + wider(self.swap[j, r, cols])
                self.part[block, r, cols] = pack(both + wider(self.away[i, r]))

            by_rows(merge, self.span)
            self.push(step, cols, self.near.at[i, self.r, cols], 5, step)

    def wait(self):
        self.swapped(3)
        arrive(self.near.at[:, self.r], self.rsem.at[5], self.me.core())

    def rows(self, r):
        own = wider(self.part[self.block(0), r]) + wider(self.swap[3, r])
        return own + (wider(self.near[0, r]) + wider(self.near[1, r]))


def normalize(stream):
    centred = stream - jnp.mean(stream, axis=-1, keepdims=True)
    rstd = lax.rsqrt(jnp.mean(centred * centred, axis=-1, keepdims=True) + LN_EPS)
    return (centred * rstd, rstd)


def norm_back(normed, rstd, incoming):
    first = jnp.mean(incoming, axis=-1, keepdims=True)
    second = jnp.mean(incoming * normed, axis=-1, keepdims=True)
    return rstd * (incoming - first - normed * second)


def contract(left, right, left_dim, right_dim):
    return lax.dot_general(
        left, right, (((left_dim,), (right_dim,)), ((), ())), preferred_element_type=F32
    )


def softmax_rows(queries, key_rows, factor):
    scores = contract(queries, key_rows, 1, 1) * factor
    scores = jnp.exp(scores - jnp.max(scores, axis=-1, keepdims=True))
    return scores * (1.0 / jnp.sum(scores, axis=-1, keepdims=True))


def by_rows(body, rows=(0, OWN)):
    @pl.loop(rows[0] // 32, (rows[0] + rows[1]) // 32)
    def _(i):
        body(pl.ds(pl.multiple_of(i * 32, 32), 32))


def step_kernel(
    grad_scale, factor,
    tok, mod, wq, wo, wi, wb, og,
    final, grad, oq, oo, oi, ob,
    wa, wf, ga, gf, r1, r2, p1, p2, r3, r4, p3, p4, xbuf, part, partf, xf, a1, a2, dm, da, packed, att, datt, act, dg, du,
    pf, swap, own_sum, theirs, swapf, away, near, middle,
    gs, gr, ss, rs, xs, xr, ys, yr, es, er, csem,
):
    me = Place()
    mine_f = pl.multiple_of(me.xh * HALF, HALF)
    other_f = pl.multiple_of((1 - me.xh) * HALF, HALF)
    home_a, home_f = wa.at[me.z, me.y, me.xh], wf.at[me.z, me.y, me.xh]
    parts = [
        (wq.at[j, :, pl.ds(h * HEAD_DIM, HEAD_DIM)], home_a.at[:, pl.ds(h * QKV + j * HEAD_DIM, HEAD_DIM)])
        for h in range(HEADS) for j in range(3)
    ] + [
        (wo, home_a.at[:, pl.ds(3 * QKV, QKV)]),
        (wi.at[:, pl.ds(mine_f, HALF)], home_f.at[:, LEFT]),
        (wb.at[:, pl.ds(mine_f, HALF)], home_f.at[:, RIGHT]),
    ]
    loads = [pltpu.make_async_copy(src, dst, csem.at[i]) for i, (src, dst) in enumerate(parts)]
    for load in loads:
        load.start()
    greet(torus_peers(me))
    for load in loads:
        load.wait()
    mine, other = me.xl, 1 - me.xl

    def m(i):
        return mod[i]

    sends = Sends()
    yz, zy = ("y", "z"), ("z", "y")
    plan = [
        (wa, 0, [(yz, (0, 384, 256)), (zy, (640, 256, 256))]), (wa, 1, [(zy, (0, 384, 256)), (yz, (640, 256, 256))]),
        (wa, 0, [(yz, (1152, 256, 128))]), (wa, 1, [(zy, (1152, 256, 128))]),
        (wf, 0, [(yz, (0, 384, 384)), (zy, (768, 384, 384))]), (wf, 1, [(yz, (0, 384, 384)), (zy, (768, 384, 384))]),
    ]
    pieces = []
    count = 0
    for ref, side, halves in plan:
        pieces.append([])
        for axes, span in halves:
            xb = 1 - me.xh if side else me.xh
            pieces[-1].append(Gather(me, ref, axes, span, xb, gs.at[count], gr.at[count], sends))
            count += 1

    def gather_event(k, what):
        if what == "first" and k % 2:
            for i, ref, cols in crossed[k]:
                arrive(ref.at[me.z, me.y, 1 - me.xh, :, cols], xr.at[i], me.across())
        for half in pieces[k]:
            getattr(half, what)()

    crossed = {1: [(0, wa, pl.ds(0, 3 * QKV))], 3: [(1, wa, pl.ds(3 * QKV, QKV))], 5: [(2, wf, LEFT), (3, wf, RIGHT)]}

    def cross(group):
        if group < 2:
            ref = home_a.at[:, crossed[2 * group + 1][0][2]]
            sends.start(ref, ref, xs.at[group], xr.at[group], me.across())
        else:
            for i, ref, cols in ((2, wi, LEFT), (3, wb, RIGHT)):
                sends.start(ref.at[:, pl.ds(other_f, HALF)], home_f.at[:, cols], xs.at[i], xr.at[i], me.across())

    def ag(*steps):
        names = {
            "f": "first", "s": "second", "l": "last", "o": "own", "i": "sides", "e": "end", "r": "relay", "c": "close"
        }
        for step in steps:
            gather_event(int(step[1]), names[step[0]])

    scatters = []
    for k in range(10):
        side = k % 2
        xb = me.xh if side else 1 - me.xh
        if k < 4:
            span, axes = ((HALF, 384, 384), (0, 384, 384))[k // 2], (yz, zy, zy, yz)[k]
        else:
            span, axes = ((3 * QKV, 256, 128), (0, 384, 384), (2 * QKV, 256, 128))[k // 2 - 2], (zy, yz, zy, yz, yz, zy)[k - 4]
        kind = Scatter if k < 4 else FineScatter
        if span[1] == 384:
            n = k if k < 4 else k - 2
            bufs = ((r1.at[n], r2.at[n]), (p1.at[n], p2.at[n]))
        else:
            n = k - 4 if k < 6 else k - 6
            bufs = ((r3.at[n], r4.at[n]), (p3.at[n], p4.at[n]))
        scatters.append(kind(me, gf if k < 4 else ga, axes, span, xb, bufs, ss.at[k], rs.at[k], sends))

    def finish(k):
        scatter = scatters[k]
        _, total = scatter.total(1)
        cols = scatter.cols["all"]
        group = k // 2
        if k < 4:
            out = (ob, oi)[group].at[:, pl.ds(mine_f, HALF)]
            if k % 2:
                out[...] = total
            else:
                partf[group] = pack(total)
                sends.start(partf.at[group], xf.at[group], ys.at[group], yr.at[group], me.across())
        elif k % 2 == 0:
            part[:, cols] = pack(total)
            sends.start(part.at[:, cols], xbuf.at[:, cols], ys.at[group], yr.at[group], me.across())
        else:
            arrive(xbuf.at[:, cols], yr.at[group], me.across())
            total = total + wider(xbuf[:, cols])
            for i in range(cols.size // QKV):
                value = total[:, i * QKV : (i + 1) * QKV]
                head = cols.start // QKV + i
                if head == HEADS:
                    oo[...] = value
                else:
                    for j in range(3):
                        oq[j, :, pl.ds(head * HEAD_DIM, HEAD_DIM)] = value[:, j * HEAD_DIM : (j + 1) * HEAD_DIM]

    def rsc(*steps):
        names = {
            "f": ("both", 0), "r": ("relay", 0), "d": ("fold",), "g": ("both", 1), "s": ("relay", 1),
            "F": ("far0",), "N": ("rest0",), "R": ("relay0",), "D": ("fold0",), "G": ("far", 1), "H": ("rest", 1),
        }
        spots = {"": (2, 1, -1, 0), "a": (2,), "b": (1, -1), "c": (0,), "ab": (2, 1, -1), "bc": (1, -1, 0)}
        for step in steps:
            scatter_event(step, int(step[1]), names, spots)

    def scatter_event(step, k, names, spots):
        if step[0] == "e":
            finish(k)
        else:
            name, *args = names[step[0]]
            if step[0] in "FNRD":
                args = spots[step[2:]]
            getattr(scatters[k], name)(*args)

    def rows_of(ref, side, cols=slice(None)):
        value = ref[pl.ds(side * 2, 2), :, cols]
        return value.reshape(2 * OWN, value.shape[-1])

    def forward(src, side, w, col, width, emit):
        weight = w[:, :, :, :, pl.ds(col, width)].reshape(WIDTH, width)
        emit(contract(rows_of(src, side), weight, 1, 0).reshape(2, OWN, width))

    def backward(src, side, w, col, width, out):
        @pl.loop(0, 2)
        def _(j):
            weight = w[pl.ds(j * 2, 2), :, :, :, pl.ds(col, width)].reshape(HALF, width)
            at = pl.multiple_of(j * HALF, 128)
            value = contract(rows_of(src, side), weight, 1, 1)
            out[pl.ds(side * 2, 2), :, pl.ds(at, HALF)] = pack(value).reshape(2, OWN, HALF)

    def gradient(left, right, g, col, width):
        count = left.shape[0] * OWN

        @pl.loop(0, 4)
        def _(j):
            rows = left[:, :, pl.ds(pl.multiple_of(j * 384, 128), 384)].reshape(count, 384)
            value = contract(rows, right[...].reshape(count, width), 0, 0) * grad_scale
            g[j, :, :, :, pl.ds(col, width)] = pack(value).reshape(4, 2, ROWS, width)

    every = (0, OWN)
    x_a1 = SeqGather(me, a1, every, es.at[0], er.at[0], sends)
    x_das = [SeqGather(me, da, rows, es.at[1 + i], er.at[1 + i], sends) for i, rows in enumerate(CHUNKS)]
    a2_sends = Sends()
    x_a2s = [RingGather(me, a2, rows, es.at[3 + i], er.at[3 + i], a2_sends) for i, rows in enumerate(CHUNKS)]
    x_dm = RingGather(me, dm, every, es.at[5], er.at[5], sends)
    y_att = SeqScatter(me, pf.at[pl.ds(0, 4)], swap, own_sum, theirs, es.at[6], er.at[6])
    y_first = SeqScatter(me, a2.at[pl.ds(0, 4)], swap, own_sum, theirs, es.at[7], er.at[7])
    y_backs = [
        RingScatter(me, pf, swapf.at[0], away.at[0], near.at[0], rows, es.at[8 + i], er.at[8 + i])
        for i, rows in enumerate(CHUNKS)
    ]
    y_back = y_backs[0]
    y_ffn = RingScatter(me, pf, swapf.at[1], away.at[1], near.at[1], every, es.at[10], er.at[10])

    def all_of(objects, *names):
        for name in names:
            for item in objects:
                getattr(item, name)()

    def share(y, src, col, width):
        backward(src, other, wa, col, width, y.part)
        y.give(0)
        backward(src, mine, wa, col, width, y.part)
        y.give(1)
        y.cross()

    def first_norm(r):
        n1, _ = normalize(wider(tok[r]))
        a1[me.s, r] = pack(n1 * (1.0 + m(1)) + m(0))

    def gate(r):
        dm[me.n, r] = pack(m(5) * wider(og[r]))

    def put(dst, side):
        def emit(value):
            dst[pl.ds(side * 2, 2)] = pack(value)
        return emit

    def head_cols(place, head):
        return pl.ds(pl.multiple_of(head * QKV + place * HEAD_DIM, HEAD_DIM), HEAD_DIM)

    def own_cols(head):
        return pl.ds(pl.multiple_of(head * HEAD_DIM, HEAD_DIM), HEAD_DIM)

    def head_rows(ref, cols):
        return ref[:, :, cols].reshape(4 * OWN, HEAD_DIM)

    def attend(head):
        q, k, v = (head_rows(packed, head_cols(i, head)) for i in range(3))
        probs = softmax_rows(q, k, factor)
        att[:, :, own_cols(head)] = pack(contract(pack(probs), v, 1, 0)).reshape(4, OWN, HEAD_DIM)

    def attend_back(head):
        q, k, v = (head_rows(packed, head_cols(i, head)) for i in range(3))
        up = head_rows(datt, own_cols(head))
        probs = softmax_rows(q, k, factor)
        dprobs = contract(up, v, 1, 1)
        dscores = pack(probs * (dprobs - jnp.sum(probs * dprobs, axis=-1, keepdims=True)) * factor)
        parts = (contract(dscores, k, 1, 0), contract(dscores, q, 0, 0), contract(pack(probs), up, 0, 0))
        for i, value in enumerate(parts):
            packed[:, :, head_cols(i, head)] = pack(value).reshape(4, OWN, HEAD_DIM)

    def heads(body, low=0, high=HEADS):
        pl.loop(low, high)(body)

    def second_norm(r):
        mid = wider(tok[r]) + m(2) * y_att.rows(r)
        middle[r] = mid
        n2, _ = normalize(mid)
        a2[me.n, r] = pack(n2 * (1.0 + m(4)) + m(3))

    def hidden(chip):
        def emit(u):
            t = jnp.tanh(GELU_A * (u + GELU_B * (u * u * u)))
            at = pl.ds(chip * 2, 2)
            act[at] = pack(0.5 * u * (1.0 + t))
            slope = 0.5 * (1.0 + t) + (0.5 * GELU_A) * u * (1.0 - t * t) * (1.0 + (3.0 * GELU_B) * (u * u))
            du[at] = pack(slope * dg[at])
        forward(a2, chip, wf, 0, HALF, emit)

    def hidden_back(chip):
        def emit(value):
            dg[pl.ds(chip * 2, 2)] = value
        forward(dm, chip, wf, HALF, HALF, emit)

    def middle_back(r):
        n2, rstd = normalize(middle[r])
        up = wider(og[r]) + norm_back(n2, rstd, y_back.rows(r) * (1.0 + m(4)))
        grad[r] = up
        da[me.s, r] = pack(m(2) * up)

    def last_out(r):
        final[r] = pack(middle[r] + m(5) * y_ffn.rows(r))

    def first_back(r):
        n1, rstd = normalize(wider(tok[r]))
        grad[r] = grad[r] + norm_back(n1, rstd, y_first.rows(r) * (1.0 + m(1)))

    def sides(i):
        hidden(me.chip_at(2 * i - 1))

    def backs(i):
        hidden_back(me.chip_at(i))

    def norm_and_send(i):
        y_att.wait(i)
        by_rows(second_norm, CHUNKS[i])
        x_a2s[i].start()

    def back_and_send(i):
        y_backs[i].wait()
        by_rows(middle_back, CHUNKS[i])
        x_das[i].start()

    def norm_and_send(i):
        y_att.wait(i)
        by_rows(second_norm, CHUNKS[i])
        x_a2s[i].start()

    def back_and_send(i):
        y_backs[i].wait()
        by_rows(middle_back, CHUNKS[i])
        x_das[i].start()

    cross(0)
    ag("f0", "o0", "f4", "o4")
    by_rows(first_norm)
    x_a1.start()
    cross(1)
    cross(2)
    by_rows(gate)
    x_dm.start()
    ag("s0", "i0", "f1", "o1", "l0", "e0", "f2", "s1", "i1", "l1", "e1", "r0", "s2", "f3")
    x_a1.relay()
    ag("o2", "i2", "r1", "l2", "e2", "o3", "s3", "i3")
    x_dm.relay()
    ag("c0")
    x_a1.near()
    x_a1.far()
    ag("c1")
    forward(a1, mine, wa, 0, 3 * QKV, put(packed, mine))
    ag("l3", "e3")
    forward(a1, other, wa, 0, 3 * QKV, put(packed, other))
    ag("r2", "s4", "i4")
    heads(attend, 0, 1)
    ag("r3", "l4", "e4", "f5", "o5")
    heads(attend, 1, 3)
    ag("c2", "c3")
    share(y_att, att, 3 * QKV, QKV)
    x_dm.spread()
    ag("s5", "i5", "l5", "e5")
    x_dm.last()
    ag("r4")
    norm_and_send(0)
    ag("r5")
    norm_and_send(1)
    x_a2s[0].relay()
    y_att.drain()
    x_dm.own()
    x_dm.sides()
    x_dm.far()
    all_of(x_a2s, "own")
    ag("c4", "c5")
    pl.loop(0, 2)(backs)
    x_a2s[1].relay()
    hidden(me.x)
    all_of(x_a2s, "spread")
    pl.loop(2, 4)(backs)
    all_of(x_a2s, "sides")
    pl.loop(0, 2)(sides)
    all_of(x_a2s, "last")

    backward(du, me.chip_at(1), wf, 0, HALF, pf)
    y_back.give(1)
    all_of(x_a2s, "far")
    hidden(me.chip_at(2))
    backward(du, me.chip_at(2), wf, 0, HALF, pf)
    y_back.give(0)
    backward(du, me.chip_at(-1), wf, 0, HALF, pf)
    y_back.give(2)
    all_of(y_backs, "out")
    backward(du, me.chip_at(0), wf, 0, HALF, pf)
    y_back.give(3)
    all_of(y_backs, "rest")
    gradient(dm, act, gf, HALF, HALF)
    rsc("f0", "f1")
    all_of(y_backs, "relay")
    gradient(a2, du, gf, 0, HALF)
    rsc("r0", "r1", "f2", "f3")
    back_and_send(0)
    back_and_send(1)
    all_of(y_backs, "drain")
    all_of(x_a2s, "drain")
    backward(act, me.chip_at(2), wf, HALF, HALF, pf)
    y_ffn.give(0)
    backward(act, me.chip_at(1), wf, HALF, HALF, pf)
    y_ffn.give(1)
    rsc("d0", "g0", "d1", "g1")
    x_das[0].relay()
    backward(act, me.chip_at(-1), wf, HALF, HALF, pf)
    y_ffn.give(2)
    rsc("r2", "r3")
    backward(act, me.chip_at(0), wf, HALF, HALF, pf)
    y_ffn.give(3)
    x_das[1].relay()
    all_of(x_das, "near")
    forward(da, mine, wa, 3 * QKV, QKV, put(datt, mine))
    all_of(x_das, "far")
    forward(da, other, wa, 3 * QKV, QKV, put(datt, other))
    y_ffn.out()
    gradient(da, att, ga, 3 * QKV, QKV)
    rsc("F4", "F5", "N4", "N5")
    heads(attend_back, 0, 2)
    y_ffn.rest()
    rsc("d2", "g2", "d3", "g3", "s0", "s1")
    gradient(a1, packed.at[:, :, pl.ds(0, HALF)], ga, 0, HALF)
    rsc("F6", "F7", "N6", "N7", "R4", "R5")
    heads(attend_back, 2, 3)
    gradient(a1, packed.at[:, :, pl.ds(HALF, QKV)], ga, HALF, QKV)
    rsc("F8", "F9", "s2", "s3", "R6a", "R7a", "R6b", "R7b", "R6c", "R7c", "N8", "N9", "e0")
    y_ffn.relay()
    share(y_first, packed, 0, 3 * QKV)
    rsc("R8a", "R9a", "R8b", "R9b", "R8c", "R9c", "D4", "G4", "H4", "D5", "G5", "H5")
    rsc("D6a", "G6", "D7a", "G7", "D6b", "H6", "D7b", "H7", "D6c", "D7c", "e2")
    rsc("D8a", "G8", "D9a", "G9", "D8b", "H8", "D9b", "H9", "D8c", "D9c", "s4", "s5", "s6", "s7", "s8", "s9")
    rsc("e4", "e6", "e8")
    y_ffn.wait()
    by_rows(last_out)
    y_first.wait(0)
    y_first.wait(1)
    by_rows(first_back)
    rsc("e1", "e3")
    for group, out in enumerate((ob, oi)):
        arrive(xf.at[group], yr.at[group], me.across())
        out[:, pl.ds(other_f, HALF)] = wider(xf[group])
    rsc("e5", "e7", "e9")
    for piece in pieces:
        for half in piece:
            half.drain()
    for scatter in scatters:
        scatter.drain()
    all_of([x_a1, x_dm, y_first, y_ffn] + x_das, "drain")
    sends.close()


def copy_kernel(*refs):
    n = len(refs) // 2
    sem = refs[-1]
    copies = [pltpu.make_async_copy(refs[i], refs[n + i], sem.at[i]) for i in range(n)]
    for copy in copies:
        copy.start()
    for copy in copies:
        copy.wait()


def copy_out(arrays):
    return pl.pallas_call(
        copy_kernel,
        out_shape=[jax.ShapeDtypeStruct(a.shape, a.dtype) for a in arrays],
        in_specs=[VM] * len(arrays),
        out_specs=[ANY] * len(arrays),
        scratch_shapes=[DMA((len(arrays),))],
    )(*arrays)


def local(tokens, modulation, w_qkv, w_out, w_in, w_back, out_grad):
    grad_scale = 1.0 / math.sqrt(OWN * lax.axis_size("sp") * lax.axis_size("fsdp"))
    factor = TEMPER / math.sqrt(HEAD_DIM)

    def shape(dims, dtype=BF16):
        return jax.ShapeDtypeStruct(dims, dtype)

    def vm(*dims, dtype=BF16):
        return pltpu.VMEM(dims, dtype)

    seq, ring = (4, OWN, WIDTH), (8, OWN, WIDTH)
    results = pl.pallas_call(
        functools.partial(step_kernel, grad_scale, factor),
        out_shape=(
            shape((OWN, WIDTH)), shape((OWN, WIDTH), F32), shape((3, ROWS, QKV), F32),
            shape((ROWS, QKV), F32), shape((ROWS, GROUP), F32), shape((ROWS, GROUP), F32),
        ),
        in_specs=[VM, VM, ANY, ANY, ANY, ANY, VM],
        out_specs=(VM,) * 6,
        scratch_shapes=[
            vm(4, 4, 2, ROWS, GROUP), vm(4, 4, 2, ROWS, GROUP), vm(4, 4, 2, ROWS, GROUP), vm(4, 4, 2, ROWS, GROUP),
            vm(6, 2, 4, ROWS, QUART), vm(6, 2, 4, ROWS, HALF), vm(6, 2, ROWS, QUART), vm(6, 2, ROWS, HALF),
            vm(4, 2, 4, ROWS, 256), vm(4, 2, 4, ROWS, 384), vm(4, 2, ROWS, 256), vm(4, 2, ROWS, 384),
            vm(ROWS, GROUP), vm(ROWS, GROUP), vm(2, ROWS, HALF), vm(2, ROWS, HALF),
            vm(*seq), vm(*ring), vm(*ring), vm(*seq),
            vm(4, OWN, 3 * QKV), vm(4, OWN, QKV), vm(4, OWN, QKV),
            vm(8, OWN, HALF), vm(8, OWN, HALF, dtype=F32), vm(8, OWN, HALF),
            vm(*ring), vm(2, OWN, WIDTH), vm(OWN, WIDTH), vm(OWN, WIDTH),
            vm(2, 4, OWN, WIDTH), vm(2, 2, OWN, HALF), vm(2, 2, OWN, WIDTH), vm(OWN, WIDTH, dtype=F32),
            DMA((10, 2)), DMA((10, 6)), DMA((10, 6)), DMA((10, 12)),
            DMA((4,)), DMA((4,)), DMA((5,)), DMA((5,)), DMA((11, 2)), DMA((11, 7)), DMA((12,)),
        ],
        compiler_params=pltpu.CompilerParams(
            collective_id=0, has_side_effects=True, vmem_limit_bytes=67043328
        ),
    )(
        tokens[0], modulation.transpose(2, 0, 1, 3)[:, 0],
        w_qkv[0].transpose(1, 0, 2), w_out[0].T, w_in[0], w_back[0].T, out_grad[0],
    )
    final, grad, oq, oo, oi, ob = copy_out(results)
    return (
        final[None], grad[None], oq.transpose(1, 0, 2)[None], oo.T[None], oi[None], ob.T[None],
    )


def solution(mesh):
    weights = (
        P(None, "fsdp", None, "sp"),
        P(None, "sp", "fsdp"),
        P(None, "fsdp", "sp"),
        P(None, "sp", "fsdp"),
    )
    rows = P("fsdp", "sp", None)
    return jax.shard_map(
        local,
        mesh=mesh,
        in_specs=(rows, P("fsdp", None, None, None), *weights, rows),
        out_specs=(rows, rows, *weights),
        check_vma=False,
    )
```

```python
import functools
import math

import jax
import jax.numpy as jnp
from jax import lax
from jax.experimental import pallas as pl
from jax.experimental.pallas import tpu as pltpu
from jax.sharding import PartitionSpec as P

HEAD_DIM = 128
LN_EPS = 1e-06
TEMPER = 2.5
F32 = jnp.float32
BF16 = jnp.bfloat16
MESH = pl.DeviceIdType.MESH
GROUP = 1536
HALF = GROUP // 2
QUART = GROUP // 4
ROWS = 48


def rem(a, n):
    return lax.rem(a, n)


class Place:
    def __init__(self):
        f = lax.axis_index("fsdp")
        s = lax.axis_index("sp")
        self.z, self.y, self.xh = lax.div(f, 8), rem(lax.div(f, 2), 4), rem(f, 2)
        self.xl, self.c = lax.div(s, 2), rem(s, 2)
        self.s = s
        self.x = self.xh * 2 + self.xl
        self.n = self.x * 2 + self.c

    def dev(self, **kw):
        v = {k: kw.get(k, getattr(self, k)) for k in ("z", "y", "xh", "xl", "c")}
        return (v["z"] * 8 + v["y"] * 2 + v["xh"], v["xl"] * 2 + v["c"])

    def ring(self, axis, step):
        return rem(getattr(self, axis) + step + 4, 4)

    def near(self, axis, step):
        return self.dev(**{axis: self.ring(axis, step)})

    def along(self, step):
        x = rem(self.x + step + 4, 4)
        return self.dev(xh=lax.div(x, 2), xl=rem(x, 2))

    def chip_at(self, step):
        return rem(self.x + step + 4, 4)

    def across(self):
        return self.dev(xh=1 - self.xh)

    def chip(self):
        return self.dev(xl=1 - self.xl)

    def core(self):
        return self.dev(c=1 - self.c)


def greet(devices):
    barrier = pltpu.get_barrier_semaphore()
    for d in devices:
        pl.semaphore_signal(barrier, inc=1, device_id=d, device_id_type=MESH)
    pl.semaphore_wait(barrier, len(devices))


def torus_peers(me):
    return [me.near(a, s) for a in ("z", "y") for s in (1, -1)] + [me.across(), me.along(1), me.along(-1), me.core()]


class Sends:
    def __init__(self):
        self.open = []

    def start(self, src, dst, ssem, rsem, dev):
        copy = pltpu.make_async_remote_copy(
            src_ref=src, dst_ref=dst, send_sem=ssem, recv_sem=rsem, device_id=dev, device_id_type=MESH
        )
        copy.start()
        self.open.append(copy)

    def close(self):
        for copy in self.open:
            copy.wait_send()
        self.open = []


def launch(src, dst, ssem, rsem, dev):
    pltpu.make_async_remote_copy(
        src_ref=src, dst_ref=dst, send_sem=ssem, recv_sem=rsem, device_id=dev, device_id_type=MESH
    ).start()


def drained(ref, ssem, dev):
    pltpu.make_async_remote_copy(
        src_ref=ref, dst_ref=ref, send_sem=ssem, recv_sem=ssem, device_id=dev, device_id_type=MESH
    ).wait_send()


def arrive(ref, rsem, dev):
    pltpu.make_async_remote_copy(
        src_ref=ref, dst_ref=ref, send_sem=rsem, recv_sem=rsem, device_id=dev, device_id_type=MESH
    ).wait_recv()


def columns(start, low, high):
    return {"all": pl.ds(start, low + high), "lo": pl.ds(start, low), "hi": pl.ds(start + low, high)}


class Gather:
    def __init__(self, me, w, axes, span, xb, ssem, rsem, sends):
        self.me, self.w, self.axes, self.xb = me, w, axes, xb
        self.ssem, self.rsem, self.sends = ssem, rsem, sends
        self.cols = columns(*span)

    def part(self, p, q, which):
        first, second = self.axes
        at = {first: slice(None) if p is None else self.me.ring(first, p), second: self.me.ring(second, q)}
        return self.w.at[at["z"], at["y"], self.xb, :, self.cols[which]]

    def go(self, level, to, p, q, which, i):
        ref = self.part(p, q, which)
        launch(ref, ref, self.ssem.at[level], self.rsem.at[i], self.me.near(self.axes[level], to))

    def got(self, p, q, which, i):
        arrive(self.part(p, q, which), self.rsem.at[i], self.me.near(self.axes[0], 1))

    def first(self):
        self.go(0, 1, 0, 0, "all", 0)
        self.go(0, -1, 0, 0, "all", 1)

    def second(self):
        self.got(-1, 0, "all", 0)
        self.go(0, 1, -1, 0, "lo", 2)
        self.got(1, 0, "all", 1)
        self.go(0, -1, 1, 0, "hi", 2)

    def last(self):
        self.got(2, 0, "all", 2)

    def out(self, *ps):
        for p in ps:
            self.go(1, 1, p, 0, "all", 3)
            self.go(1, -1, p, 0, "all", 4)

    def own(self):
        self.out(0)

    def sides(self):
        self.out(-1, 1)

    def end(self):
        self.out(2)

    def relay(self):
        self.got(None, -1, "all", 3)
        self.go(1, 1, None, -1, "lo", 5)
        self.got(None, 1, "all", 4)
        self.go(1, -1, None, 1, "hi", 5)

    def close(self):
        self.got(None, 2, "all", 5)

    def drain(self):
        cols = self.cols["all"]
        drained(self.w.at[0, pl.ds(0, 3), 0, :, cols], self.ssem.at[0], self.me.near("z", 1))
        drained(self.w.at[pl.ds(0, 3), pl.ds(0, 4), 0, :, cols], self.ssem.at[1], self.me.near("z", 1))


def wider(ref_value):
    return ref_value.astype(F32)


def pack(total):
    return total.astype(BF16)


class Scatter:
    def __init__(self, me, g, axes, span, xb, bufs, ssem, rsem, sends):
        self.me, self.g, self.axes, self.xb = me, g, axes, xb
        self.bufs, self.ssem, self.rsem, self.sends = bufs, ssem, rsem, sends
        self.cols = columns(*span)
        self.inner = columns(0, *span[1:])

    def spot(self, level, step, which):
        axis = self.axes[level]
        at = {"z": self.me.z, "y": self.me.y}
        at[axis] = self.me.ring(axis, step)
        if level == 0:
            at[self.axes[1]] = slice(None)
        return (at["z"], at["y"], self.xb, slice(None), self.cols[which])

    def way(self, level, i, which):
        if level == 0:
            return self.bufs[0][0].at[i, :, :, columns(0, *self.sizes(which))["lo"]]
        return self.bufs[1][0].at[i, :, columns(0, *self.sizes(which))["lo"]]

    def sizes(self, which):
        return self.inner[which].size, 0

    def send(self, level, step, which, dst, i, to):
        launch(
            self.g.at[self.spot(level, step, which)], dst, self.ssem.at[level], self.rsem.at[level * 2 + i],
            self.me.near(self.axes[level], to),
        )

    def near(self, level, i, which):
        cols = self.inner[which]
        if level == 0:
            return self.bufs[level][1].at[i, :, :, cols]
        return self.bufs[level][1].at[i, :, cols]

    def far(self, level):
        for to, which, i in ((1, "lo", 0), (-1, "hi", 1)):
            self.send(level, 2, which, self.way(level, i, which), 0, to)

    def rest(self, level):
        for to, which, i in ((1, "hi", 0), (-1, "lo", 1)):
            self.send(level, to, which, self.near(level, i, which), 1, to)

    def both(self, level):
        self.far(level)
        self.rest(level)

    def relay(self, level):
        arrive(self.g.at[self.spot(level, 0, "all")], self.rsem.at[level * 2], self.me.near(self.axes[level], 1))
        for to, which, i in ((1, "lo", 0), (-1, "hi", 1)):
            buf = self.way(level, i, which)
            spot = self.spot(level, to, which)
            self.g[spot] = (wider(self.g[spot]) + wider(buf[...])).astype(BF16)
        for to, which, i in ((1, "lo", 0), (-1, "hi", 1)):
            self.send(level, to, which, self.near(level, i, which), 1, to)

    def total(self, level):
        near = self.bufs[level][1]
        arrive(near, self.rsem.at[level * 2 + 1], self.me.near(self.axes[level], 1))
        spot = self.spot(level, 0, "all")
        return spot, wider(self.g[spot]) + wider(near[0]) + wider(near[1])

    def drain_at(self, level):
        places = pl.ds(0, 3) if level == 0 else 0
        wide = pl.ds(0, 4) if level == 0 else pl.ds(0, 3)
        drained(self.g.at[places, wide, 0, :, self.cols["all"]], self.ssem.at[level], self.me.near("z", 1))

    def drain(self):
        self.drain_at(0)
        self.drain_at(1)

    def fold(self):
        spot, total = self.total(0)
        self.g[spot] = total.astype(BF16)


class FineScatter(Scatter):
    slots = {2: 0, 1: 1, -1: 2, 0: 3}

    def place(self, q, p, which):
        at = {self.axes[0]: self.me.ring(self.axes[0], q), self.axes[1]: self.me.ring(self.axes[1], p)}
        return (at["z"], at["y"], self.xb, slice(None), self.cols[which])

    def give(self, q, p, which, dst, i, to):
        slot = self.slots[p]
        launch(
            self.g.at[self.place(q, p, which)], dst, self.ssem.at[2 + slot], self.rsem.at[4 + slot * 2 + i],
            self.me.near(self.axes[0], to),
        )

    def take(self, ref, p, i):
        arrive(ref, self.rsem.at[4 + self.slots[p] * 2 + i], self.me.near(self.axes[0], 1))

    def side(self, i, p, which):
        return self.bufs[0][1].at[i, self.slots[p], :, self.inner[which]]

    def step(self, i, p, which):
        return self.bufs[0][0].at[i, self.slots[p], :, pl.ds(0, self.inner[which].size)]

    def far0(self, *ps):
        for p in ps:
            for to, which, i in ((1, "lo", 0), (-1, "hi", 1)):
                self.give(2, p, which, self.step(i, p, which), 0, to)

    def rest0(self, *ps):
        for p in ps:
            for to, which, i in ((1, "hi", 0), (-1, "lo", 1)):
                self.give(to, p, which, self.side(i, p, which), 1, to)

    def relay0(self, *ps):
        for p in ps:
            self.take(self.g.at[self.place(0, p, "all")], p, 0)
            for to, which, i in ((1, "lo", 0), (-1, "hi", 1)):
                spot = self.place(to, p, which)
                self.g[spot] = pack(wider(self.g[spot]) + wider(self.step(i, p, which)[...]))
            for to, which, i in ((1, "lo", 0), (-1, "hi", 1)):
                self.give(to, p, which, self.side(i, p, which), 1, to)

    def fold0(self, *ps):
        for p in ps:
            near = self.bufs[0][1]
            self.take(near.at[:, self.slots[p]], p, 1)
            spot = self.place(0, p, "all")
            total = wider(self.g[spot]) + wider(near[0, self.slots[p]]) + wider(near[1, self.slots[p]])
            self.g[spot] = pack(total)

    def drain(self):
        self.drain_at(1)
        for slot in range(4):
            ref = self.g.at[0, pl.ds(0, 3), 0, :, self.cols["all"]]
            drained(ref, self.ssem.at[2 + slot], self.me.near("z", 1))


DMA = pltpu.SemaphoreType.DMA
VM = pl.BlockSpec(memory_space=pltpu.VMEM)
ANY = pl.BlockSpec(memory_space=pl.ANY)
OWN = 128
WIDTH = 1536
HEADS = 3
QKV = HEADS * HEAD_DIM
GELU_A = math.sqrt(2.0 / math.pi)
GELU_B = 0.044715


CHUNKS = ((0, OWN // 2), (OWN // 2, OWN // 2))


class SeqGather:
    def __init__(self, me, buf, rows, ssem, rsem, sends):
        self.me, self.buf, self.rows, self.ssem, self.rsem, self.sends = me, buf, pl.ds(*rows), ssem, rsem, sends

    def push(self, block, i, dev):
        ref = self.buf.at[block, self.rows]
        launch(ref, ref, self.ssem.at[0], self.rsem.at[i], dev)

    def drain(self):
        drained(self.buf.at[pl.ds(0, 3), self.rows], self.ssem.at[0], self.me.core())

    def start(self):
        self.push(self.me.s, 0, self.me.chip())
        self.push(self.me.s, 1, self.me.core())

    def relay(self):
        other = (1 - self.me.xl) * 2 + self.me.c
        arrive(self.buf.at[other, self.rows], self.rsem.at[0], self.me.chip())
        self.push(other, 2, self.me.core())

    def near(self):
        arrive(self.buf.at[self.me.xl * 2 + 1 - self.me.c, self.rows], self.rsem.at[1], self.me.core())

    def far(self):
        arrive(self.buf.at[(1 - self.me.xl) * 2 + 1 - self.me.c, self.rows], self.rsem.at[2], self.me.core())


class SeqScatter:
    def __init__(self, me, part, swap, mine, theirs, ssem, rsem):
        self.me, self.part, self.swap, self.mine, self.theirs = me, part, swap, mine, theirs
        self.ssem, self.rsem = ssem, rsem

    def drain(self):
        drained(self.part.at[pl.ds(0, 3)], self.ssem.at[0], self.me.core())

    def give(self, i):
        xl = self.me.xl if i else 1 - self.me.xl
        launch(self.part.at[xl * 2 + 1 - self.me.c], self.swap.at[i], self.ssem.at[0], self.rsem.at[i], self.me.core())

    def cross(self):
        arrive(self.swap.at[0], self.rsem.at[0], self.me.core())

        def merge(r):
            self.mine[r] = pack(wider(self.part[(1 - self.me.xl) * 2 + self.me.c, r]) + wider(self.swap[0, r]))

        for i, rows in enumerate(CHUNKS):
            by_rows(merge, rows)
            r = pl.ds(*rows)
            launch(self.mine.at[r], self.theirs.at[r], self.ssem.at[0], self.rsem.at[2 + i], self.me.chip())

    def wait(self, i):
        if i == 0:
            arrive(self.swap.at[1], self.rsem.at[1], self.me.core())
        arrive(self.theirs.at[pl.ds(*CHUNKS[i])], self.rsem.at[2 + i], self.me.chip())

    def rows(self, r):
        return wider(self.part[self.me.s, r]) + wider(self.swap[1, r]) + wider(self.theirs[r])


LEFT, RIGHT = pl.ds(0, HALF), pl.ds(HALF, HALF)


class RingGather:
    def __init__(self, me, buf, rows, ssem, rsem, sends):
        self.me, self.buf, self.rows, self.ssem, self.rsem, self.sends = me, buf, pl.ds(*rows), ssem, rsem, sends

    def at(self, step, mine=True, cols=pl.ds(0, WIDTH)):
        return self.buf.at[self.me.chip_at(step) * 2 + (self.me.c if mine else 1 - self.me.c), self.rows, cols]

    def push(self, ref, i, dev):
        launch(ref, ref, self.ssem.at[0], self.rsem.at[i], dev)

    def drain(self):
        drained(self.buf.at[pl.ds(0, 7), self.rows], self.ssem.at[0], self.me.core())

    def start(self):
        for cols, step, i in ((LEFT, 1, 0), (RIGHT, -1, 1), (RIGHT, 1, 2), (LEFT, -1, 2)):
            self.push(self.at(0, cols=cols), i, self.me.along(step))
        self.push(self.at(0), 3, self.me.core())

    def relay(self):
        for step, cols, i in ((-1, LEFT, 0), (1, RIGHT, 1)):
            arrive(self.at(step, cols=cols), self.rsem.at[i], self.me.core())
            self.push(self.at(step, cols=cols), 4, self.me.along(-step))

    def spread(self):
        arrive(self.at(1), self.rsem.at[2], self.me.core())
        for step in (-1, 1):
            self.push(self.at(step), 5, self.me.core())

    def last(self):
        arrive(self.at(2), self.rsem.at[4], self.me.core())
        self.push(self.at(2), 6, self.me.core())

    def own(self):
        arrive(self.at(0, False), self.rsem.at[3], self.me.core())

    def sides(self):
        arrive(self.buf.at[pl.ds(0, 2), self.rows], self.rsem.at[5], self.me.core())

    def far(self):
        arrive(self.at(2, False), self.rsem.at[6], self.me.core())


class RingScatter:
    order = (2, 1, -1, 0)

    def __init__(self, me, part, swap, away, near, rows, ssem, rsem):
        self.me, self.part, self.swap, self.away, self.near = me, part, swap, away, near
        self.span, self.ssem, self.rsem = rows, ssem, rsem
        self.r = pl.ds(*rows)

    def block(self, step):
        return self.me.chip_at(step) * 2 + self.me.c

    def give(self, j):
        src = self.part.at[self.me.chip_at(self.order[j]) * 2 + 1 - self.me.c]
        launch(src, self.swap.at[j], self.ssem.at[0], self.rsem.at[j], self.me.core())

    def drain(self):
        if self.span[0] == 0:
            drained(self.part.at[pl.ds(0, 4)], self.ssem.at[0], self.me.core())
        drained(self.part.at[pl.ds(0, 3), self.r], self.ssem.at[1], self.me.core())

    def swapped(self, j):
        if self.span[0] == 0:
            arrive(self.swap.at[j], self.rsem.at[j], self.me.core())

    def push(self, step, cols, dst, i, to):
        launch(self.part.at[self.block(step), self.r, cols], dst, self.ssem.at[1], self.rsem.at[i], self.me.along(to))

    def out(self):
        self.swapped(0)
        block = self.block(2)

        def merge(r):
            self.part[block, r] = pack(wider(self.part[block, r]) + wider(self.swap[0, r]))

        by_rows(merge, self.span)
        self.push(2, LEFT, self.away.at[0, self.r], 4, 1)
        self.push(2, RIGHT, self.away.at[1, self.r], 4, -1)

    def rest(self):
        for step, j, i, cols in ((1, 1, 0, RIGHT), (-1, 2, 1, LEFT)):
            self.swapped(j)
            block = self.block(step)

            def merge(r):
                self.part[block, r, cols] = pack(wider(self.part[block, r, cols]) + wider(self.swap[j, r, cols]))

            by_rows(merge, self.span)
            self.push(step, cols, self.near.at[i, self.r, cols], 5, step)

    def relay(self):
        arrive(self.away.at[:, self.r], self.rsem.at[4], self.me.core())
        for step, j, i, cols in ((1, 1, 0, LEFT), (-1, 2, 1, RIGHT)):
            block = self.block(step)

            def merge(r):
                both = wider(self.part[block, r, cols]) + wider(self.swap[j, r, cols])
                self.part[block, r, cols] = pack(both + wider(self.away[i, r]))

            by_rows(merge, self.span)
            self.push(step, cols, self.near.at[i, self.r, cols], 5, step)

    def wait(self):
        self.swapped(3)
        arrive(self.near.at[:, self.r], self.rsem.at[5], self.me.core())

    def rows(self, r):
        own = wider(self.part[self.block(0), r]) + wider(self.swap[3, r])
        return own + (wider(self.near[0, r]) + wider(self.near[1, r]))


def normalize(stream):
    centred = stream - jnp.mean(stream, axis=-1, keepdims=True)
    rstd = lax.rsqrt(jnp.mean(centred * centred, axis=-1, keepdims=True) + LN_EPS)
    return (centred * rstd, rstd)


def norm_back(normed, rstd, incoming):
    first = jnp.mean(incoming, axis=-1, keepdims=True)
    second = jnp.mean(incoming * normed, axis=-1, keepdims=True)
    return rstd * (incoming - first - normed * second)


def contract(left, right, left_dim, right_dim):
    return lax.dot_general(
        left, right, (((left_dim,), (right_dim,)), ((), ())), preferred_element_type=F32
    )


def softmax_rows(queries, key_rows, factor):
    scores = contract(queries, key_rows, 1, 1) * factor
    scores = jnp.exp(scores - jnp.max(scores, axis=-1, keepdims=True))
    return scores * (1.0 / jnp.sum(scores, axis=-1, keepdims=True))


def by_rows(body, rows=(0, OWN)):
    @pl.loop(rows[0] // 32, (rows[0] + rows[1]) // 32)
    def _(i):
        body(pl.ds(pl.multiple_of(i * 32, 32), 32))


def step_kernel(
    grad_scale, factor,
    tok, mod, wq, wo, wi, wb, og,
    final, grad, oq, oo, oi, ob,
    wa, wf, ga, gf, r1, r2, p1, p2, r3, r4, p3, p4, xbuf, part, partf, xf, a1, a2, dm, da, packed, att, datt, act, dg, du,
    pf, swap, own_sum, theirs, swapf, away, near, middle,
    gs, gr, ss, rs, xs, xr, ys, yr, es, er, csem,
):
    me = Place()
    mine_f = pl.multiple_of(me.xh * HALF, HALF)
    other_f = pl.multiple_of((1 - me.xh) * HALF, HALF)
    home_a, home_f = wa.at[me.z, me.y, me.xh], wf.at[me.z, me.y, me.xh]
    parts = [
        (wq.at[j, :, pl.ds(h * HEAD_DIM, HEAD_DIM)], home_a.at[:, pl.ds(h * QKV + j * HEAD_DIM, HEAD_DIM)])
        for h in range(HEADS) for j in range(3)
    ] + [
        (wo, home_a.at[:, pl.ds(3 * QKV, QKV)]),
        (wi.at[:, pl.ds(mine_f, HALF)], home_f.at[:, LEFT]),
        (wb.at[:, pl.ds(mine_f, HALF)], home_f.at[:, RIGHT]),
    ]
    loads = [pltpu.make_async_copy(src, dst, csem.at[i // 10]) for i, (src, dst) in enumerate(parts)]
    for load in loads:
        load.start()
    greet(torus_peers(me))
    for i, home in enumerate((home_a, home_f)):
        pltpu.make_async_copy(home, home, csem.at[i]).wait()
    mine, other = me.xl, 1 - me.xl

    def m(i):
        return mod[i]

    sends = Sends()
    yz, zy = ("y", "z"), ("z", "y")
    plan = [
        (wa, 0, [(yz, (0, 384, 256)), (zy, (640, 256, 256))]), (wa, 1, [(zy, (0, 384, 256)), (yz, (640, 256, 256))]),
        (wa, 0, [(yz, (1152, 256, 128))]), (wa, 1, [(zy, (1152, 256, 128))]),
        (wf, 0, [(yz, (0, 384, 384)), (zy, (768, 384, 384))]), (wf, 1, [(yz, (0, 384, 384)), (zy, (768, 384, 384))]),
    ]
    pieces = []
    count = 0
    for ref, side, halves in plan:
        pieces.append([])
        for axes, span in halves:
            xb = 1 - me.xh if side else me.xh
            pieces[-1].append(Gather(me, ref, axes, span, xb, gs.at[count], gr.at[count], sends))
            count += 1

    def gather_event(k, what):
        if what == "first" and k % 2:
            for i, ref, cols in crossed[k]:
                arrive(ref.at[me.z, me.y, 1 - me.xh, :, cols], xr.at[i], me.across())
        for half in pieces[k]:
            getattr(half, what)()

    crossed = {1: [(0, wa, pl.ds(0, 3 * QKV))], 3: [(1, wa, pl.ds(3 * QKV, QKV))], 5: [(2, wf, LEFT), (3, wf, RIGHT)]}

    def cross(group):
        if group < 2:
            ref = home_a.at[:, crossed[2 * group + 1][0][2]]
            sends.start(ref, ref, xs.at[group], xr.at[group], me.across())
        else:
            for i, ref, cols in ((2, wi, LEFT), (3, wb, RIGHT)):
                sends.start(ref.at[:, pl.ds(other_f, HALF)], home_f.at[:, cols], xs.at[i], xr.at[i], me.across())

    def ag(*steps):
        names = {
            "f": "first", "s": "second", "l": "last", "o": "own", "i": "sides", "e": "end", "r": "relay", "c": "close"
        }
        for step in steps:
            gather_event(int(step[1]), names[step[0]])

    scatters = []
    for k in range(10):
        side = k % 2
        xb = me.xh if side else 1 - me.xh
        if k < 4:
            span, axes = ((HALF, 384, 384), (0, 384, 384))[k // 2], (yz, zy, zy, yz)[k]
        else:
            span, axes = ((3 * QKV, 256, 128), (0, 384, 384), (2 * QKV, 256, 128))[k // 2 - 2], (zy, yz, zy, yz, yz, zy)[k - 4]
        kind = Scatter if k < 4 else FineScatter
        if span[1] == 384:
            n = k if k < 4 else k - 2
            bufs = ((r1.at[n], r2.at[n]), (p1.at[n], p2.at[n]))
        else:
            n = k - 4 if k < 6 else k - 6
            bufs = ((r3.at[n], r4.at[n]), (p3.at[n], p4.at[n]))
        scatters.append(kind(me, gf if k < 4 else ga, axes, span, xb, bufs, ss.at[k], rs.at[k], sends))

    def finish(k):
        scatter = scatters[k]
        _, total = scatter.total(1)
        cols = scatter.cols["all"]
        group = k // 2
        if k < 4:
            out = (ob, oi)[group].at[:, pl.ds(mine_f, HALF)]
            if k % 2:
                out[...] = total
            else:
                partf[group] = pack(total)
                sends.start(partf.at[group], xf.at[group], ys.at[group], yr.at[group], me.across())
        elif k % 2 == 0:
            part[:, cols] = pack(total)
            sends.start(part.at[:, cols], xbuf.at[:, cols], ys.at[group], yr.at[group], me.across())
        else:
            arrive(xbuf.at[:, cols], yr.at[group], me.across())
            total = total + wider(xbuf[:, cols])
            for i in range(cols.size // QKV):
                value = total[:, i * QKV : (i + 1) * QKV]
                head = cols.start // QKV + i
                if head == HEADS:
                    oo[...] = value
                else:
                    for j in range(3):
                        oq[j, :, pl.ds(head * HEAD_DIM, HEAD_DIM)] = value[:, j * HEAD_DIM : (j + 1) * HEAD_DIM]

    def rsc(*steps):
        names = {
            "f": ("both", 0), "r": ("relay", 0), "d": ("fold",), "g": ("both", 1), "s": ("relay", 1),
            "F": ("far0",), "N": ("rest0",), "R": ("relay0",), "D": ("fold0",), "G": ("far", 1), "H": ("rest", 1),
        }
        spots = {"": (2, 1, -1, 0), "a": (2,), "b": (1, -1), "c": (0,), "ab": (2, 1, -1), "bc": (1, -1, 0)}
        for step in steps:
            scatter_event(step, int(step[1]), names, spots)

    def scatter_event(step, k, names, spots):
        if step[0] == "e":
            finish(k)
        else:
            name, *args = names[step[0]]
            if step[0] in "FNRD":
                args = spots[step[2:]]
            getattr(scatters[k], name)(*args)

    def rows_of(ref, side, cols=slice(None)):
        value = ref[pl.ds(side * 2, 2), :, cols]
        return value.reshape(2 * OWN, value.shape[-1])

    def forward(src, side, w, col, width, emit):
        weight = w[:, :, :, :, pl.ds(col, width)].reshape(WIDTH, width)
        emit(contract(rows_of(src, side), weight, 1, 0).reshape(2, OWN, width))

    def backward(src, side, w, col, width, out):
        @pl.loop(0, 2)
        def _(j):
            weight = w[pl.ds(j * 2, 2), :, :, :, pl.ds(col, width)].reshape(HALF, width)
            at = pl.multiple_of(j * HALF, 128)
            value = contract(rows_of(src, side), weight, 1, 1)
            out[pl.ds(side * 2, 2), :, pl.ds(at, HALF)] = pack(value).reshape(2, OWN, HALF)

    def gradient(left, right, g, col, width):
        count = left.shape[0] * OWN

        @pl.loop(0, 4)
        def _(j):
            rows = left[:, :, pl.ds(pl.multiple_of(j * 384, 128), 384)].reshape(count, 384)
            value = contract(rows, right[...].reshape(count, width), 0, 0) * grad_scale
            g[j, :, :, :, pl.ds(col, width)] = pack(value).reshape(4, 2, ROWS, width)

    every = (0, OWN)
    x_a1 = SeqGather(me, a1, every, es.at[0], er.at[0], sends)
    x_das = [SeqGather(me, da, rows, es.at[1 + i], er.at[1 + i], sends) for i, rows in enumerate(CHUNKS)]
    a2_sends = Sends()
    x_a2s = [RingGather(me, a2, rows, es.at[3 + i], er.at[3 + i], a2_sends) for i, rows in enumerate(CHUNKS)]
    x_dm = RingGather(me, dm, every, es.at[5], er.at[5], sends)
    y_att = SeqScatter(me, pf.at[pl.ds(0, 4)], swap, own_sum, theirs, es.at[6], er.at[6])
    y_first = SeqScatter(me, a2.at[pl.ds(0, 4)], swap, own_sum, theirs, es.at[7], er.at[7])
    y_backs = [
        RingScatter(me, pf, swapf.at[0], away.at[0], near.at[0], rows, es.at[8 + i], er.at[8 + i])
        for i, rows in enumerate(CHUNKS)
    ]
    y_back = y_backs[0]
    y_ffn = RingScatter(me, pf, swapf.at[1], away.at[1], near.at[1], every, es.at[10], er.at[10])

    def all_of(objects, *names):
        for name in names:
            for item in objects:
                getattr(item, name)()

    def share(y, src, col, width):
        backward(src, other, wa, col, width, y.part)
        y.give(0)
        backward(src, mine, wa, col, width, y.part)
        y.give(1)
        y.cross()

    def first_norm(r):
        n1, _ = normalize(wider(tok[r]))
        a1[me.s, r] = pack(n1 * (1.0 + m(1)) + m(0))

    def gate(r):
        dm[me.n, r] = pack(m(5) * wider(og[r]))

    def put(dst, side):
        def emit(value):
            dst[pl.ds(side * 2, 2)] = pack(value)
        return emit

    def head_cols(place, head):
        return pl.ds(pl.multiple_of(head * QKV + place * HEAD_DIM, HEAD_DIM), HEAD_DIM)

    def own_cols(head):
        return pl.ds(pl.multiple_of(head * HEAD_DIM, HEAD_DIM), HEAD_DIM)

    def head_rows(ref, cols):
        return ref[:, :, cols].reshape(4 * OWN, HEAD_DIM)

    def attend(head):
        q, k, v = (head_rows(packed, head_cols(i, head)) for i in range(3))
        probs = softmax_rows(q, k, factor)
        att[:, :, own_cols(head)] = pack(contract(pack(probs), v, 1, 0)).reshape(4, OWN, HEAD_DIM)

    def attend_back(head):
        q, k, v = (head_rows(packed, head_cols(i, head)) for i in range(3))
        up = head_rows(datt, own_cols(head))
        probs = softmax_rows(q, k, factor)
        dprobs = contract(up, v, 1, 1)
        dscores = pack(probs * (dprobs - jnp.sum(probs * dprobs, axis=-1, keepdims=True)) * factor)
        parts = (contract(dscores, k, 1, 0), contract(dscores, q, 0, 0), contract(pack(probs), up, 0, 0))
        for i, value in enumerate(parts):
            packed[:, :, head_cols(i, head)] = pack(value).reshape(4, OWN, HEAD_DIM)

    def heads(body, low=0, high=HEADS):
        pl.loop(low, high)(body)

    def second_norm(r):
        mid = wider(tok[r]) + m(2) * y_att.rows(r)
        middle[r] = mid
        n2, _ = normalize(mid)
        a2[me.n, r] = pack(n2 * (1.0 + m(4)) + m(3))

    def hidden(chip):
        def emit(u):
            t = jnp.tanh(GELU_A * (u + GELU_B * (u * u * u)))
            at = pl.ds(chip * 2, 2)
            act[at] = pack(0.5 * u * (1.0 + t))
            slope = 0.5 * (1.0 + t) + (0.5 * GELU_A) * u * (1.0 - t * t) * (1.0 + (3.0 * GELU_B) * (u * u))
            du[at] = pack(slope * dg[at])
        forward(a2, chip, wf, 0, HALF, emit)

    def hidden_back(chip):
        def emit(value):
            dg[pl.ds(chip * 2, 2)] = value
        forward(dm, chip, wf, HALF, HALF, emit)

    def middle_back(r):
        n2, rstd = normalize(middle[r])
        up = wider(og[r]) + norm_back(n2, rstd, y_back.rows(r) * (1.0 + m(4)))
        grad[r] = up
        da[me.s, r] = pack(m(2) * up)

    def last_out(r):
        final[r] = pack(middle[r] + m(5) * y_ffn.rows(r))

    def first_back(r):
        n1, rstd = normalize(wider(tok[r]))
        grad[r] = grad[r] + norm_back(n1, rstd, y_first.rows(r) * (1.0 + m(1)))

    def sides(i):
        hidden(me.chip_at(2 * i - 1))

    def backs(i):
        hidden_back(me.chip_at(i))

    def norm_and_send(i):
        y_att.wait(i)
        by_rows(second_norm, CHUNKS[i])
        x_a2s[i].start()

    def back_and_send(i):
        y_backs[i].wait()
        by_rows(middle_back, CHUNKS[i])
        x_das[i].start()

    def norm_and_send(i):
        y_att.wait(i)
        by_rows(second_norm, CHUNKS[i])
        x_a2s[i].start()

    def back_and_send(i):
        y_backs[i].wait()
        by_rows(middle_back, CHUNKS[i])
        x_das[i].start()

    cross(0)
    ag("f0", "o0", "f4", "o4")
    by_rows(first_norm)
    x_a1.start()
    cross(1)
    cross(2)
    by_rows(gate)
    x_dm.start()
    ag("s0", "i0", "f1", "o1", "l0", "e0", "f2", "s1", "i1", "l1", "e1", "r0", "s2", "f3")
    x_a1.relay()
    ag("o2", "i2", "r1", "l2", "e2", "o3", "s3", "i3")
    x_dm.relay()
    ag("c0")
    x_a1.near()
    x_a1.far()
    ag("c1")
    forward(a1, mine, wa, 0, 3 * QKV, put(packed, mine))
    ag("l3", "e3")
    forward(a1, other, wa, 0, 3 * QKV, put(packed, other))
    ag("r2", "s4", "i4")
    heads(attend, 0, 1)
    ag("r3", "l4", "e4", "f5", "o5")
    heads(attend, 1, 3)
    ag("c2", "c3")
    share(y_att, att, 3 * QKV, QKV)
    x_dm.spread()
    ag("s5", "i5", "l5", "e5")
    x_dm.last()
    ag("r4")
    norm_and_send(0)
    ag("r5")
    norm_and_send(1)
    x_a2s[0].relay()
    y_att.drain()
    x_dm.own()
    x_dm.sides()
    x_dm.far()
    all_of(x_a2s, "own")
    ag("c4", "c5")
    pl.loop(0, 2)(backs)
    x_a2s[1].relay()
    hidden(me.x)
    all_of(x_a2s, "spread")
    pl.loop(2, 4)(backs)
    all_of(x_a2s, "sides")
    pl.loop(0, 2)(sides)
    all_of(x_a2s, "last")

    backward(du, me.chip_at(1), wf, 0, HALF, pf)
    y_back.give(1)
    all_of(x_a2s, "far")
    hidden(me.chip_at(2))
    backward(du, me.chip_at(2), wf, 0, HALF, pf)
    y_back.give(0)
    backward(du, me.chip_at(-1), wf, 0, HALF, pf)
    y_back.give(2)
    all_of(y_backs, "out")
    backward(du, me.chip_at(0), wf, 0, HALF, pf)
    y_back.give(3)
    all_of(y_backs, "rest")
    gradient(dm, act, gf, HALF, HALF)
    rsc("f0", "f1")
    all_of(y_backs, "relay")
    gradient(a2, du, gf, 0, HALF)
    rsc("r0", "r1", "f2", "f3")
    back_and_send(0)
    back_and_send(1)
    all_of(y_backs, "drain")
    all_of(x_a2s, "drain")
    backward(act, me.chip_at(2), wf, HALF, HALF, pf)
    y_ffn.give(0)
    backward(act, me.chip_at(1), wf, HALF, HALF, pf)
    y_ffn.give(1)
    rsc("d0", "g0", "d1", "g1")
    x_das[0].relay()
    backward(act, me.chip_at(-1), wf, HALF, HALF, pf)
    y_ffn.give(2)
    rsc("r2", "r3")
    backward(act, me.chip_at(0), wf, HALF, HALF, pf)
    y_ffn.give(3)
    x_das[1].relay()
    all_of(x_das, "near")
    forward(da, mine, wa, 3 * QKV, QKV, put(datt, mine))
    all_of(x_das, "far")
    forward(da, other, wa, 3 * QKV, QKV, put(datt, other))
    y_ffn.out()
    gradient(da, att, ga, 3 * QKV, QKV)
    rsc("F4", "F5", "N4", "N5")
    heads(attend_back, 0, 2)
    y_ffn.rest()
    rsc("d2", "g2", "d3", "g3", "s0", "s1")
    gradient(a1, packed.at[:, :, pl.ds(0, HALF)], ga, 0, HALF)
    rsc("F6", "F7", "N6", "N7", "R4", "R5")
    heads(attend_back, 2, 3)
    gradient(a1, packed.at[:, :, pl.ds(HALF, QKV)], ga, HALF, QKV)
    rsc("F8", "F9", "s2", "s3", "R6a", "R7a", "R6b", "R7b", "R6c", "R7c", "N8", "N9", "e0")
    y_ffn.relay()
    share(y_first, packed, 0, 3 * QKV)
    rsc("R8a", "R9a", "R8b", "R9b", "R8c", "R9c", "D4", "G4", "H4", "D5", "G5", "H5")
    rsc("D6a", "G6", "D7a", "G7", "D6b", "H6", "D7b", "H7", "D6c", "D7c", "e2")
    rsc("D8a", "G8", "D9a", "G9", "D8b", "H8", "D9b", "H9", "D8c", "D9c", "s4", "s5", "s6", "s7", "s8", "s9")
    rsc("e4", "e6", "e8")
    y_ffn.wait()
    by_rows(last_out)
    y_first.wait(0)
    y_first.wait(1)
    by_rows(first_back)
    rsc("e1", "e3")
    for group, out in enumerate((ob, oi)):
        arrive(xf.at[group], yr.at[group], me.across())
        out[:, pl.ds(other_f, HALF)] = wider(xf[group])
    rsc("e5", "e7", "e9")
    for piece in pieces:
        for half in piece:
            half.drain()
    for scatter in scatters:
        scatter.drain()
    all_of([x_a1, x_dm, y_first, y_ffn] + x_das, "drain")
    sends.close()


def copy_kernel(*refs):
    n = len(refs) // 2
    sem = refs[-1]
    copies = [pltpu.make_async_copy(refs[i], refs[n + i], sem.at[i]) for i in range(n)]
    for copy in copies:
        copy.start()
    for copy in copies:
        copy.wait()


def copy_out(arrays):
    return pl.pallas_call(
        copy_kernel,
        out_shape=[jax.ShapeDtypeStruct(a.shape, a.dtype) for a in arrays],
        in_specs=[VM] * len(arrays),
        out_specs=[ANY] * len(arrays),
        scratch_shapes=[DMA((len(arrays),))],
    )(*arrays)


def local(tokens, modulation, w_qkv, w_out, w_in, w_back, out_grad):
    grad_scale = 1.0 / math.sqrt(OWN * lax.axis_size("sp") * lax.axis_size("fsdp"))
    factor = TEMPER / math.sqrt(HEAD_DIM)

    def shape(dims, dtype=BF16):
        return jax.ShapeDtypeStruct(dims, dtype)

    def vm(*dims, dtype=BF16):
        return pltpu.VMEM(dims, dtype)

    seq, ring = (4, OWN, WIDTH), (8, OWN, WIDTH)
    results = pl.pallas_call(
        functools.partial(step_kernel, grad_scale, factor),
        out_shape=(
            shape((OWN, WIDTH)), shape((OWN, WIDTH), F32), shape((3, ROWS, QKV), F32),
            shape((ROWS, QKV), F32), shape((ROWS, GROUP), F32), shape((ROWS, GROUP), F32),
        ),
        in_specs=[VM, VM, ANY, ANY, ANY, ANY, VM],
        out_specs=(VM,) * 6,
        scratch_shapes=[
            vm(4, 4, 2, ROWS, GROUP), vm(4, 4, 2, ROWS, GROUP), vm(4, 4, 2, ROWS, GROUP), vm(4, 4, 2, ROWS, GROUP),
            vm(6, 2, 4, ROWS, QUART), vm(6, 2, 4, ROWS, HALF), vm(6, 2, ROWS, QUART), vm(6, 2, ROWS, HALF),
            vm(4, 2, 4, ROWS, 256), vm(4, 2, 4, ROWS, 384), vm(4, 2, ROWS, 256), vm(4, 2, ROWS, 384),
            vm(ROWS, GROUP), vm(ROWS, GROUP), vm(2, ROWS, HALF), vm(2, ROWS, HALF),
            vm(*seq), vm(*ring), vm(*ring), vm(*seq),
            vm(4, OWN, 3 * QKV), vm(4, OWN, QKV), vm(4, OWN, QKV),
            vm(8, OWN, HALF), vm(8, OWN, HALF, dtype=F32), vm(8, OWN, HALF),
            vm(*ring), vm(2, OWN, WIDTH), vm(OWN, WIDTH), vm(OWN, WIDTH),
            vm(2, 4, OWN, WIDTH), vm(2, 2, OWN, HALF), vm(2, 2, OWN, WIDTH), vm(OWN, WIDTH, dtype=F32),
            DMA((10, 2)), DMA((10, 6)), DMA((10, 6)), DMA((10, 12)),
            DMA((4,)), DMA((4,)), DMA((5,)), DMA((5,)), DMA((11, 2)), DMA((11, 7)), DMA((2,)),
        ],
        compiler_params=pltpu.CompilerParams(
            collective_id=0, has_side_effects=True, vmem_limit_bytes=67043328
        ),
    )(
        tokens[0], modulation.transpose(2, 0, 1, 3)[:, 0],
        w_qkv[0].transpose(1, 0, 2), w_out[0].T, w_in[0], w_back[0].T, out_grad[0],
    )
    final, grad, oq, oo, oi, ob = copy_out(results)
    return (
        final[None], grad[None], oq.transpose(1, 0, 2)[None], oo.T[None], oi[None], ob.T[None],
    )


def solution(mesh):
    weights = (
        P(None, "fsdp", None, "sp"),
        P(None, "sp", "fsdp"),
        P(None, "fsdp", "sp"),
        P(None, "sp", "fsdp"),
    )
    rows = P("fsdp", "sp", None)
    return jax.shard_map(
        local,
        mesh=mesh,
        in_specs=(rows, P("fsdp", None, None, None), *weights, rows),
        out_specs=(rows, rows, *weights),
        check_vma=False,
    )
```
